32 devices in a mesh: members: 2 (over y), comp: 4 (over z), lat: 2 (over x), sub: 2 (over core).
Axes of the slice: x: 2, y: 2, z: 4, core: 2. Of those that a mesh axis runs over, the one named last changes fastest.
Arguments:
- spectrum: float32 [1920, 4096], P('comp', ('members', 'lat', 'sub')), parts along dimension 1, may hold values from 0.05 to 2
- sea_mask: int32 [4096], P(('members', 'lat', 'sub')), parts along dimension 0, may hold values 0 or 1
- neighbours: int32 [4, 4096], P(None, ('members', 'lat', 'sub')), parts along dimension 1, may hold values from 0 to 2047, as said below
- substeps: int32 [30], replicated, may hold values from 1 to 6, as said below
- courant: float32 [30], replicated, may hold values from 0.2 to 0.7
- source_operator: bfloat16 [1920, 1920], P('sub'), may hold values from -0.125 to 0.125
Outputs:
- new_spectrum: float32 [1920, 4096], P('comp', ('members', 'lat', 'sub')), parts along dimension 1
The draws below stay inside these ranges and needn't reach their ends.
There are 2 independent parts, one for each index of `members`. The reference program is written for one: setup_inputs(seed, part) draws one part's arguments, and reference() takes and returns one part's arrays. A program takes and returns all parts, laid end to end along the dimension named above; an argument that names none is the same for every part. Nothing has to cross between parts.
Inputs may be any that keep to these rules, and one draw needn't show every extreme that they name: Non-increasing with the band; the first band takes 6 substeps and the last band one. Points are numbered row by row, 256 to a row. The west and east neighbours lie in the same row, one or two columns away, wrapping around the row. The south neighbour lies in the row before and the north neighbour in the row after, within one column (wrapping); on the first and last row of the member's grid that neighbour is the point itself.
All inputs are finite; a program needn't handle non-finite values. No bound on the sum of `sea_mask` on one device may be relied on, other than what follows from the above.
Results may differ from the reference program's by a relative error of at most 0.0015.
Values may be sent and summed in bfloat16 or wider, within the bound.
A program may use at most 64 MiB of HBM per device.

```python
import math
import jax
import jax.numpy as jnp

NF = 30
ND = 64
NBINS = 1920
NLON = 256
MAXSTEPS = 6
SRC_STEPS = 4
P_SIZE = 2048


def draw_neighbours(key, part):
    rows_all = P_SIZE // NLON
    position = jnp.arange(P_SIZE, dtype=jnp.int32)
    row_number = position // NLON
    column = position % NLON
    key_list = jax.random.split(key, 4)
    west_step = jax.random.randint(key_list[0], (P_SIZE,), 1, 3).astype(jnp.int32)
    east_step = jax.random.randint(key_list[1], (P_SIZE,), 1, 3).astype(jnp.int32)
    south_step = jax.random.randint(key_list[2], (P_SIZE,), -1, 2).astype(jnp.int32)
    north_step = jax.random.randint(key_list[3], (P_SIZE,), -1, 2).astype(jnp.int32)
    west_index = row_number * NLON + (column - west_step) % NLON
    east_index = row_number * NLON + (column + east_step) % NLON
    south_index = jnp.where(row_number > 0, (row_number - 1) * NLON + (column + south_step) % NLON, position)
    north_index = jnp.where(row_number < rows_all - 1, (row_number + 1) * NLON + (column + north_step) % NLON, position)
    return jnp.stack([west_index, east_index, south_index, north_index]).astype(jnp.int32)


def draw_substeps(key, part):
    raw_counts = jax.random.randint(key, (NF,), 1, MAXSTEPS + 1).astype(jnp.int32)
    raw_counts = raw_counts.at[0].set(MAXSTEPS).at[NF - 1].set(1)
    return (-jnp.sort(-raw_counts)).astype(jnp.int32)


def set_ends(entries, stream_key, low, largest):
    extent = entries.shape
    place = [jax.random.randint(jax.random.fold_in(stream_key, axis), (), 0, extent[axis]) for axis in range(len(extent))]
    entries = entries.at[tuple(place)].set(low)
    longest = extent.index(max(extent))
    place[longest] = (place[longest] + 1) % extent[longest]
    return entries.at[tuple(place)].set(largest)


def shard_levels(own_key, extent, shards, low, largest):
    gain, own = 1.0, jax.random.fold_in(own_key, 6)
    for dim, shards_of in shards:
        heights = jnp.exp(jax.random.uniform(jax.random.fold_in(own, dim), (shards_of,), jnp.float32, low / len(shards), largest / len(shards)))
        gain = gain * jnp.repeat(heights, extent[dim] // shards_of).reshape([-1 if axis == dim else 1 for axis in range(len(extent))])
    return gain


def normal_values(own_key, extent, spread, reach, pieces=(), kind=jnp.bfloat16):
    drawn = jax.random.normal(own_key, extent, jnp.float32) * spread
    if len(pieces) > 0:
        drawn = shard_levels(own_key, extent, pieces, -0.22, 0.18) * drawn
    return jnp.clip(drawn, min=-reach, max=reach).astype(kind)


def setup_inputs(seed: int = 0, part: int = 0) -> dict:
    arg_keys = jax.random.split(jax.random.key(seed), 7)
    own_keys = jax.random.split(jax.random.fold_in(arg_keys[6], part), 7)
    return {
        "spectrum": jnp.clip(jnp.exp(math.log(2.0) - 3.6888794 * jax.random.uniform(own_keys[0], (NBINS, P_SIZE), jnp.float32) ** shard_levels(own_keys[0], (NBINS, P_SIZE), ((0, 4), (1, 4)), -0.2, 0.2)), 0.05, 2.0),
        "sea_mask": set_ends((jax.random.randint(own_keys[1], (P_SIZE,), 0, 5) < 4).astype(jnp.int32), jax.random.fold_in(own_keys[1], 1), 0, 1),
        "neighbours": draw_neighbours(jax.random.fold_in(jax.random.fold_in(arg_keys[6], part), 71), part),
        "substeps": draw_substeps(jax.random.fold_in(arg_keys[6], 71), part),
        "courant": jnp.clip(jax.random.uniform(arg_keys[4], (NF,), jnp.float32, 0.2, 0.7), 0.2, 0.7),
        "source_operator": normal_values(arg_keys[5], (NBINS, NBINS), NBINS ** -0.5, 0.125, ((0, 2),)),
    }


STEP_SIZE = 0.1


def reference(spectrum, sea_mask, neighbours, substeps, courant, source_operator):
    bin_index = jnp.arange(NF * ND, dtype=jnp.int32)
    frequency = bin_index // ND
    direction = bin_index % ND
    angles = (direction.astype(jnp.float32) + 0.5) * (2.0 * math.pi / ND)
    cosine = jnp.cos(angles)
    sine_dir = jnp.sin(angles)
    bin_speed = courant[frequency]
    weight_x = bin_speed * jnp.abs(cosine)
    weight_y = bin_speed * jnp.abs(sine_dir)
    bin_steps = substeps[frequency]
    sea_float = sea_mask.astype(jnp.float32)
    field_now = sea_float[None, :] * spectrum
    for substep in range(MAXSTEPS):
        west_vals = field_now[:, neighbours[0]]
        east_vals = field_now[:, neighbours[1]]
        south_vals = field_now[:, neighbours[2]]
        north_vals = field_now[:, neighbours[3]]
        upwind_lon = jnp.where((cosine > 0)[:, None], west_vals, east_vals)
        upwind_lat = jnp.where((sine_dir > 0)[:, None], south_vals, north_vals)
        advanced = sea_float[None, :] * (field_now - weight_x[:, None] * (field_now - upwind_lon)
                                         - weight_y[:, None] * (field_now - upwind_lat))
        field_now = jnp.where((substep < bin_steps)[:, None], advanced, field_now)
    propagated = field_now
    start_spec = propagated.astype(jnp.bfloat16)
    state_now = start_spec.astype(jnp.float32)
    for source_step in range(SRC_STEPS):
        driving = jnp.dot(source_operator, state_now.astype(jnp.bfloat16), preferred_element_type=jnp.float32)
        state_now = state_now + STEP_SIZE * state_now * driving
    increment = (state_now - start_spec.astype(jnp.float32)).astype(jnp.bfloat16)
    return sea_float[None, :] * (propagated + increment.astype(jnp.float32))
```

```python
import functools
import math

import jax
import jax.numpy as jnp
import numpy as np
from jax import lax
from jax.experimental import pallas as pl
from jax.experimental.pallas import tpu as pltpu
from jax.sharding import PartitionSpec as P

NF = 30
ND = 64
NLON = 256
MAXSTEPS = 6
SRC_STEPS = 4
STEP_SIZE = 0.1
MESH = pl.DeviceIdType.MESH
HALF = ND // 2
TILES = 4
SLOTS = 8
NEAR = 4
FAR = 2
F32 = jnp.float32
BF16 = jnp.bfloat16


def kernel(
    nlat, ncomp, group, spec_ref, mask_ref, nb_ref, steps_ref, cour_ref, cos_ref, sin_ref, op_ref,
    out_ref, w_ref, own_ref, halo_ref, code_ref, prop_ref, away_ref, got_ref, start_ref, state_ref,
    low_ref, inc_ref, home_ref,
    h_send, h_recv, w_send, w_recv, w_local, a_send, a_recv, b_send, b_recv,
):
    lat = lax.axis_index("lat")
    sub = lax.axis_index("sub")
    me = lax.axis_index("comp")
    bins, points = spec_ref.shape
    chunks, size = prop_ref.shape[0], prop_ref.shape[1]
    planes = size // 8
    share = points // ncomp
    total = bins * ncomp
    half_rows = total // 2
    first = me * bins
    last_lat = nlat - 1
    partner = {"sub": 1 - sub}

    barrier = pltpu.get_barrier_semaphore()
    peers = [partner]
    if nlat == 2:
        peers.append({"lat": 1 - lat})
    else:
        for move in (1, -1):
            peers.append({"lat": lax.rem(lat + move + nlat, nlat)})
            peers.append({"lat": lax.rem(lat + 2 * move + nlat, nlat), "sub": 1 - sub})
    for j in range(1, ncomp):
        peers.append({"comp": lax.rem(me + j, ncomp)})
    for peer in peers:
        pl.semaphore_signal(barrier, inc=1, device_id=peer, device_id_type=MESH)

    own_half = pl.ds(pl.multiple_of(sub * half_rows, 16), half_rows)
    load_w = pltpu.make_async_copy(op_ref, w_ref.at[own_half], w_local)
    load_w.start()

    lane = lax.broadcasted_iota(jnp.int32, (1, points), 1)
    column = lane & (NLON - 1)
    position = (lat * 2 + sub) * points + lane
    sea = mask_ref[...].astype(F32)
    west = (column - nb_ref[0:1, :]) & (NLON - 1)
    east = (nb_ref[1:2, :] - column) & (NLON - 1)

    def vertical(index_row):
        moved = ((index_row - column + 1) & (NLON - 1)) - 1
        return jnp.where(index_row == position, 2, moved)

    rows = lax.broadcasted_iota(jnp.int32, (size, points), 0)
    codes = jnp.zeros((size, points), F32)
    entries = [west, east, vertical(nb_ref[2:3, :]), vertical(nb_ref[3:4, :])]
    for k, entry in enumerate([e.astype(F32) for e in entries] + [sea]):
        codes = jnp.where(rows == k, jnp.broadcast_to(entry, (size, points)), codes)
    own_ref[0] = codes.astype(BF16)
    own_ref[1] = codes.astype(BF16)

    pl.semaphore_wait(barrier, len(peers))

    def kind(q):
        return lax.rem(lax.div(first + (q - 2) * size, HALF), 2)

    def has_from(ty, far):
        return jnp.where(ty == 0, lat >= far, lat <= last_lat - far)

    def has_to(ty, far):
        return jnp.where(ty == 0, lat <= last_lat - far, lat >= far)

    def pair_copy(q):
        return pltpu.make_async_remote_copy(
            src_ref=own_ref.at[q], dst_ref=halo_ref.at[0, q], send_sem=h_send.at[0, q],
            recv_sem=h_recv.at[0, q], device_id=partner, device_id_type=MESH)

    def side_copy(q, ty):
        to = jnp.clip(lat + 1 - 2 * ty, 0, last_lat)
        return pltpu.make_async_remote_copy(
            src_ref=own_ref.at[q], dst_ref=halo_ref.at[1, q], send_sem=h_send.at[1, q],
            recv_sem=h_recv.at[1, q], device_id={"lat": to}, device_id_type=MESH)

    def hand_copy(q, ty):
        slot = jnp.where(sub == ty, 2, 0)
        return pltpu.make_async_remote_copy(
            src_ref=halo_ref.at[1, q], dst_ref=halo_ref.at[slot, q], send_sem=h_send.at[2, q],
            recv_sem=h_recv.at[2, q], device_id=partner, device_id_type=MESH)

    def far_copy(q, ty):
        to = jnp.clip(lat + 2 - 4 * ty, 0, last_lat)
        return pltpu.make_async_remote_copy(
            src_ref=own_ref.at[q], dst_ref=halo_ref.at[2, q], send_sem=h_send.at[3, q],
            recv_sem=h_recv.at[3, q], device_id={"lat": to, "sub": 1 - sub}, device_id_type=MESH)

    def send_own(q, ty):
        @pl.when(has_to(ty, 1))
        def _():
            side_copy(q, ty).start()

        @pl.when(sub == ty)
        def _():
            pair_copy(q).start()

        if nlat > 2:
            @pl.when((sub != ty) & has_to(ty, 2))
            def _():
                far_copy(q, ty).start()

    def hand_on(q, ty):
        @pl.when(has_from(ty, 1))
        def _():
            side_copy(q, ty).wait_recv()
            hand_copy(q, ty).start()

    def arrive(q, ty):
        @pl.when(has_from(ty, 1))
        def _():
            hand_copy(q, ty).wait_recv()

        @pl.when(sub != ty)
        def _():
            pair_copy(q).wait_recv()

        if nlat > 2:
            @pl.when((sub == ty) & has_from(ty, 2))
            def _():
                far_copy(q, ty).wait_recv()

    def sent(q, ty):
        @pl.when(has_to(ty, 1))
        def _():
            side_copy(q, ty).wait_send()

        @pl.when(sub == ty)
        def _():
            pair_copy(q).wait_send()

        if nlat > 2:
            @pl.when((sub != ty) & has_to(ty, 2))
            def _():
                far_copy(q, ty).wait_send()

        @pl.when(has_from(ty, 1))
        def _():
            hand_copy(q, ty).wait_send()

    send_own(0, 0)
    send_own(1, 1)

    def prepare(i, carry):
        chunk = sea * spec_ref[pl.ds(pl.multiple_of(i * size, size), size), :]
        own_ref[i + 2] = chunk.astype(BF16)
        send_own(i + 2, kind(i + 2))
        return carry

    lax.fori_loop(0, chunks, prepare, 0)

    give_w = pltpu.make_async_remote_copy(
        src_ref=op_ref, dst_ref=w_ref.at[own_half], send_sem=w_send, recv_sem=w_recv,
        device_id=partner, device_id_type=MESH)
    give_w.start()

    for q in (0, 1):
        hand_on(q, q)
    ahead = min(6, chunks)
    for q in range(2, 2 + ahead):
        hand_on(q, kind(q))

    for ty in (0, 1):
        arrive(ty, ty)
        for slot in range(SLOTS):
            row = slot % 2 if ty == 0 else 1 - slot % 2
            cols = slice(row * NLON, (row + 1) * NLON)
            if slot < 6:
                part = halo_ref[2 - slot // 2, ty, :, cols].astype(F32)
            else:
                part = own_ref[ty, :, cols].astype(F32)
            for k, source in enumerate((0, 1, 2 + ty, 4)):
                code_ref[ty, slot, k] = jnp.broadcast_to(part[source:source + 1, :], (8, NLON))

    def propagate(i):
        q = i + 2
        ty = kind(q)

        @pl.when(i + ahead < chunks)
        def _():
            hand_on(q + ahead, kind(q + ahead))

        arrive(q, ty)
        bin0 = first + i * size
        freq = lax.div(bin0, ND)
        direction = lax.rem(bin0, ND)
        to_east = jnp.where((direction < ND // 4) | (direction >= 3 * ND // 4), 1, 0)
        steps = steps_ref[freq]
        speed = cour_ref[freq]
        sign = jnp.where(to_east == 1, 1.0, -1.0)
        shift1 = jnp.where(to_east == 1, 1, NLON - 1)
        shift2 = jnp.where(to_east == 1, 2, NLON - 2)
        back1 = NLON - shift1
        d8 = lax.div(direction, 8)
        abs_cos = cos_ref[pl.ds(d8, planes)]
        abs_sin = sin_ref[pl.ds(d8, planes)]

        def lanes(slot):
            row = jnp.where(ty == 0, slot % 2, 1 - slot % 2)
            return pl.ds(pl.multiple_of(row * NLON, NLON), NLON)

        values = []
        for slot in range(SLOTS):
            if slot < 6:
                part = halo_ref[2 - slot // 2, q, :, lanes(slot)].astype(F32)
            else:
                part = spec_ref[pl.ds(pl.multiple_of(i * size, size), size), lanes(slot)]
            part = part.reshape(planes, 8, NLON)
            if slot >= 6:
                part = part * code_ref[ty, slot, 3][None]
            values.append(part)
        for t in range(MAXSTEPS):
            live = jnp.where(t < steps, speed, 0.0)
            wx = live * abs_cos
            wy = live * abs_sin
            keep = 1.0 - wx - wy
            fresh = list(values)
            for slot in range(t + 1, SLOTS):
                x = values[slot]
                below = values[slot - 1]
                near = code_ref[ty, slot, 1 - to_east][None] == 1.0
                vert = code_ref[ty, slot, 2][None] * sign
                lon = jnp.where(near, pltpu.roll(x, shift1, 2), pltpu.roll(x, shift2, 2))
                up = jnp.where(vert == -1.0, pltpu.roll(below, shift1, 2),
                               jnp.where(vert == 1.0, pltpu.roll(below, back1, 2), below))
                up = jnp.where(jnp.abs(vert) == 2.0, x, up)
                fresh[slot] = code_ref[ty, slot, 3][None] * (keep * x + wx * lon + wy * up)
            values = fresh
        for slot in (6, 7):
            prop_ref[i, :, lanes(slot)] = values[slot].reshape(size, NLON)
        whole = prop_ref[i]
        for c in range(ncomp):
            away_ref[c, i] = whole[:, c * share:(c + 1) * share].astype(BF16)

    groups = chunks // group

    def out_copy(j, g):
        to = lax.rem(me + j, ncomp)
        span = pl.ds(g * group, group)
        return pltpu.make_async_remote_copy(
            src_ref=away_ref.at[to, span], dst_ref=got_ref.at[me, span],
            send_sem=a_send.at[j], recv_sem=a_recv.at[j],
            device_id={"comp": to}, device_id_type=MESH)

    def whole_copy(j):
        to = lax.rem(me + j, ncomp)
        return pltpu.make_async_remote_copy(
            src_ref=away_ref.at[to], dst_ref=got_ref.at[me],
            send_sem=a_send.at[j], recv_sem=a_recv.at[j],
            device_id={"comp": to}, device_id_type=MESH)

    def run_group(g, carry):
        def one(i, inner):
            propagate(g * group + i)
            return inner

        lax.fori_loop(0, group, one, 0)
        for j in range(1, ncomp):
            out_copy(j, g).start()
        return carry

    lax.fori_loop(0, groups, run_group, 0)

    for q in (0, 1):
        sent(q, q)

    def drain(q, carry):
        sent(q, kind(q))
        return carry

    lax.fori_loop(2, chunks + 2, drain, 0)
    got_ref[me] = away_ref[me]
    load_w.wait()
    give_w.wait()

    for j in range(1, ncomp):
        whole_copy(j).wait()
    for c in range(ncomp):
        start_ref[c * bins:(c + 1) * bins, :] = got_ref[c].astype(F32).reshape(bins, share)
    tile = total // TILES
    per_tile = bins // tile if bins >= tile else tile // bins
    for m in range(TILES):
        span = slice(m * tile, (m + 1) * tile)
        low_ref[0, span, :] = start_ref[span, :].astype(BF16)

    def tile_rows(m):
        return pl.ds(pl.multiple_of(m * tile, 16), tile)

    def advance(step, m):
        span = tile_rows(m)
        driving = jnp.dot(w_ref[span, :], low_ref[step % 2], preferred_element_type=F32)
        now = start_ref[span, :] if step == 0 else state_ref[span, :]
        return span, now + STEP_SIZE * now * driving

    for step in range(SRC_STEPS - 1):
        def one_tile(m, carry, step=step):
            span, now = advance(step, m)
            state_ref[span, :] = now
            low_ref[(step + 1) % 2, span, :] = now.astype(BF16)
            return carry

        lax.fori_loop(0, TILES, one_tile, 0)

    def home_copy(j, to):
        return pltpu.make_async_remote_copy(
            src_ref=inc_ref.at[to], dst_ref=home_ref.at[me],
            send_sem=b_send.at[j], recv_sem=b_recv.at[j],
            device_id={"comp": to}, device_id_type=MESH)

    mine = lax.div(me * TILES, ncomp)

    def last_tile(i, carry):
        m = lax.rem(mine + 1 + i, TILES)
        span, now = advance(SRC_STEPS - 1, m)
        gain = now - start_ref[span, :]
        for k in range(per_tile):
            to = m * per_tile + k
            inc_ref[to] = gain[k * bins:(k + 1) * bins, :].astype(BF16)
            j = lax.rem(to - me + ncomp, ncomp)

            @pl.when(to != me)
            def _():
                home_copy(j, to).start()

        return carry

    lax.fori_loop(0, TILES, last_tile, 0)
    home_ref[me] = inc_ref[me]
    for c in range(ncomp):
        j = lax.rem(me - c + ncomp, ncomp)

        @pl.when(me != c)
        def _():
            home_copy(j, lax.rem(me + j, ncomp)).wait()

        cols = slice(c * share, (c + 1) * share)
        before = prop_ref[:, :, cols].reshape(bins, share)
        out_ref[:, cols] = sea[:, cols] * (before + home_ref[c].astype(F32))


def fast_kernel(
    ncomp, spec_ref, mask_ref, nb_ref, steps_ref, cour_ref, op_ref,
    out_ref, w_ref, full_ref, oth_ref, hsend_ref, halo_ref, raw_ref, code_ref, ang_ref, perm_ref,
    pout_ref, pin_ref, away_ref, x_ref, state_ref, inc_ref, home_ref,
    l_sem, w_sem, c_send, c_recv, r_send, r_recv, h_send, h_recv, a_send, a_recv, o_sem,
    f_send, f_recv, p_send, p_recv, e_send, e_recv, b_send, b_recv,
):
    lat = lax.axis_index("lat")
    sub = lax.axis_index("sub")
    me = lax.axis_index("comp")
    groups = spec_ref.shape[0]
    bins = groups * 2 * 16
    kmax = halo_ref.shape[0]
    lanes = NLON // 2
    total = bins * ncomp
    tiles = ncomp // 2
    partner = {"sub": 1 - sub}
    others = [partner, {"lat": 1 - lat}, {"lat": 1 - lat, "sub": 1 - sub}]

    loads = []
    for r in range(2):
        cols = slice(r * NLON, (r + 1) * NLON)
        loads.append(pltpu.make_async_copy(
            spec_ref.at[:, 1 - sub, :, cols], oth_ref.at[pl.ds(0, groups), r], l_sem.at[r]))
        loads.append(pltpu.make_async_copy(
            spec_ref.at[:, sub, :, cols], full_ref.at[pl.ds(0, groups), 2 * sub + r], l_sem.at[2 + r]))
    for load in (loads[0], loads[2], loads[1], loads[3]):
        load.start()
    load_w = pltpu.make_async_copy(op_ref, w_ref, w_sem)

    barrier = pltpu.get_barrier_semaphore()
    peers = list(others)
    for d in range(1, ncomp):
        z = lax.rem(me + d, ncomp)
        peers += [{"comp": z}, {"comp": z, "sub": 1 - sub}]
    for peer in peers:
        pl.semaphore_signal(barrier, inc=1, device_id=peer, device_id_type=MESH)
    load_w.start()

    points = mask_ref.shape[1]
    lane = lax.broadcasted_iota(jnp.int32, (1, points), 1)
    column = lane & (NLON - 1)
    sea = mask_ref[...].astype(F32)
    west = (column - nb_ref[0:1, :]) & (NLON - 1)
    east = (nb_ref[1:2, :] - column) & (NLON - 1)
    moves = [((nb_ref[k:k + 1, :] - column + 1) & (NLON - 1)) - 1 for k in (2, 3)]
    index = lax.broadcasted_iota(jnp.int32, (8, points), 0)
    codes = jnp.zeros((8, points), F32)
    for k, entry in enumerate([e.astype(F32) for e in (west, east, *moves)] + [sea]):
        codes = jnp.where(index == k, jnp.broadcast_to(entry, (8, points)), codes)
    raw_ref[lat, sub] = codes

    a = lax.broadcasted_iota(jnp.int32, (NLON, NLON), 0)
    b = lax.broadcasted_iota(jnp.int32, (NLON, NLON), 1)
    split = lambda c: jnp.where(c < lanes, 2 * c, 2 * (c - lanes) + 1)
    perm_ref[0] = (a == split(b)).astype(F32).astype(BF16)
    perm_ref[1] = (b == split(a)).astype(F32).astype(BF16)

    near_ty = lat
    far_ty = 1 - lat
    n0 = lax.rem(lat + me * groups, 2)
    f0 = 1 - n0
    for q, ty in enumerate((near_ty, far_ty)):
        d = lax.broadcasted_iota(jnp.int32, (16, lanes), 0) + 16 * (2 * ty + sub)
        angle = (d.astype(F32) + 0.5) * np.float32(2.0 * math.pi / ND)
        ang_ref[q, 0] = jnp.abs(jnp.cos(angle))
        ang_ref[q, 1] = jnp.abs(jnp.sin(angle))

    for load in loads:
        load.wait()
    sea_rows = [jnp.broadcast_to(sea[:, r * NLON:(r + 1) * NLON], (16, NLON)) for r in range(2)]

    def convert(k, carry):
        j = n0 + 2 * k
        for r in range(2):
            mine = full_ref[j, 2 * sub + r] * sea_rows[r]
            other = oth_ref[j, r] * sea_rows[r]
            hsend_ref[k, sub, r] = mine.astype(BF16)
            hsend_ref[k, 1 - sub, r] = other.astype(BF16)
        return carry

    lax.fori_loop(0, kmax, convert, 0)
    pl.semaphore_wait(barrier, len(peers))

    def code_copy(n):
        return pltpu.make_async_remote_copy(
            src_ref=raw_ref.at[lat, sub], dst_ref=raw_ref.at[lat, sub], send_sem=c_send.at[n],
            recv_sem=c_recv.at[n], device_id=others[n], device_id_type=MESH)

    def raw_copy():
        return pltpu.make_async_remote_copy(
            src_ref=oth_ref.at[pl.ds(0, groups)],
            dst_ref=full_ref.at[pl.ds(0, groups), pl.ds(2 * sub, 2)],
            send_sem=r_send, recv_sem=r_recv, device_id=partner, device_id_type=MESH)

    def halo_copy(k, p):
        return pltpu.make_async_remote_copy(
            src_ref=hsend_ref.at[k, p], dst_ref=halo_ref.at[k, pl.ds(2 * sub, 2)],
            send_sem=h_send.at[k, p], recv_sem=h_recv.at[k, sub],
            device_id={"lat": 1 - lat, "sub": p}, device_id_type=MESH)

    def halo_wait(k, s):
        pltpu.make_async_remote_copy(
            src_ref=hsend_ref.at[k, s], dst_ref=halo_ref.at[k, pl.ds(2 * s, 2)],
            send_sem=h_send.at[k, s], recv_sem=h_recv.at[k, s],
            device_id={"lat": 1 - lat, "sub": s}, device_id_type=MESH).wait_recv()

    code_copy(0).start()
    raw_copy().start()
    code_copy(1).start()
    code_copy(2).start()

    def send_halo(k, carry):
        @pl.when(n0 + 2 * k < groups)
        def _():
            for p in range(2):
                halo_copy(k, p).start()
        return carry

    lax.fori_loop(0, kmax, send_halo, 0)

    def decode(chip):
        for s in range(2):
            for r in range(2):
                part = raw_ref[chip, s, :, r * NLON:(r + 1) * NLON].astype(BF16)
                both = jnp.dot(part, perm_ref[0], preferred_element_type=F32)
                for k in range(5):
                    code_ref[chip, 2 * s + r, k] = jnp.broadcast_to(both[k:k + 1, :], (8, NLON))

    def chunk_copy(h, j, d):
        to = lax.rem(me + d, ncomp)
        return pltpu.make_async_remote_copy(
            src_ref=away_ref.at[h, to, j], dst_ref=x_ref.at[h, 0, me * groups + j, sub],
            send_sem=a_send.at[h, d], recv_sem=a_recv.at[h, me],
            device_id={"comp": to}, device_id_type=MESH)

    def whole_copy(h, d):
        to = lax.rem(me + d, ncomp)
        return pltpu.make_async_remote_copy(
            src_ref=away_ref.at[h, to, pl.ds(0, groups)],
            dst_ref=x_ref.at[h, 0, pl.ds(me * groups, groups), sub],
            send_sem=a_send.at[h, d], recv_sem=a_recv.at[h, me],
            device_id={"comp": to}, device_id_type=MESH)

    def whole_wait(h, z):
        pltpu.make_async_remote_copy(
            src_ref=away_ref.at[h, z, pl.ds(0, groups)],
            dst_ref=x_ref.at[h, 0, pl.ds(z * groups, groups), sub],
            send_sem=a_send.at[h, 0], recv_sem=a_recv.at[h, z],
            device_id={"comp": z}, device_id_type=MESH).wait_recv()

    def pick(ty, i):
        return ty * 3 + (1 - 2 * ty) * i

    def separate(x):
        high = x.astype(BF16)
        low = (x - high.astype(F32)).astype(BF16)
        return high, low

    def propagate(ks, far, to_east):
        ty = far_ty if far else near_ty
        js = [(f0 if far else n0) + 2 * k for k in ks]
        vert = 2 + ty
        lowest = 0 if far else 4

        def code(q, k, half):
            chip = lat if q >= 4 else 1 - lat
            part = code_ref[chip, pick(ty, q % 4), k, :, half * lanes:(half + 1) * lanes]
            return jnp.concatenate([part, part], axis=0)

        raw = jnp.concatenate([full_ref[j, pick(ty, i)] for j in js for i in range(4)], axis=0)
        high, low = separate(raw)
        mixed = (jnp.dot(high, perm_ref[0], preferred_element_type=F32)
                 + jnp.dot(low, perm_ref[0], preferred_element_type=F32))
        if far:
            edge = jnp.concatenate([halo_ref[k, pick(ty, i)] for k in ks for i in range(4)], axis=0)
            edge = jnp.dot(edge, perm_ref[0], preferred_element_type=F32)
        cells = []
        weights = []
        for n, j in enumerate(js):
            values = [None] * 8
            for i in range(4):
                rows = slice((n * 4 + i) * 16, (n * 4 + i + 1) * 16)
                values[4 + i] = tuple(
                    mixed[rows, half * lanes:(half + 1) * lanes] * code(4 + i, 4, half)
                    for half in range(2))
                if far:
                    values[i] = tuple(edge[rows, half * lanes:(half + 1) * lanes] for half in range(2))
            cells.append(values)
            freq = jnp.minimum(lax.div(me * bins + j * 32, ND), steps_ref.shape[0] - 1)
            weights.append((steps_ref[freq], cour_ref[freq]))
        abs_cos, abs_sin = ang_ref[int(far), 0], ang_ref[int(far), 1]
        ahead, behind = (1, lanes - 1)
        for t in range(MAXSTEPS):
            slots = [q for q in range(7, lowest - 1, -1) if q >= 4 or t <= q + 1]
            for n, (steps, speed) in enumerate(weights):
                live = jnp.where(t < steps, speed, 0.0)
                wx = live * abs_cos
                wy = live * abs_sin
                keep = 1.0 - wx - wy
                values = cells[n]
                fresh = list(values)
                turned = {}

                def turn(q, half, shift):
                    key = (q, half, shift)
                    if key not in turned:
                        turned[key] = pltpu.roll(values[q][half], shift, 1)
                    return turned[key]

                def left(q):
                    return turn(q, 1, ahead), values[q][0]

                def right(q):
                    return values[q][1], turn(q, 0, behind)

                for q in slots:
                    shift = ahead if to_east else behind
                    one = left(q) if to_east else right(q)
                    lon_code = 0 if to_east else 1
                    new = []
                    for half in range(2):
                        x = values[q][half]
                        lon = jnp.where(code(q, lon_code, half) == 1.0, one[half], turn(q, half, shift))
                        if q == lowest:
                            up = x
                        else:
                            move = code(q, vert, half)
                            up = jnp.where(move == -1.0, left(q - 1)[half],
                                           jnp.where(move == 1.0, right(q - 1)[half], values[q - 1][half]))
                        new.append(code(q, 4, half) * (keep * x + wx * lon + wy * up))
                    fresh[q] = tuple(new)
                cells[n] = fresh
        for n, j in enumerate(js):
            for i in range(4):
                r = pick(ty, i)
                for half in range(2):
                    value = cells[n][4 + i][half]
                    pout_ref[j, r, :, half * lanes:(half + 1) * lanes] = value
                    away_ref[lax.div(r, 2), 2 * lax.rem(r, 2) + half, j] = value.astype(BF16)
        for n, j in enumerate(js):
            @pl.when(j < groups)
            def _():
                for d in range(1, ncomp):
                    chunk_copy(0, j, d).start()

    straight = sub == lat
    code_copy(0).wait_recv()
    decode(lat)
    raw_copy().wait_recv()

    def near_body(g, carry):
        ks = [g * NEAR + n for n in range(NEAR)]

        @pl.when(straight)
        def _():
            propagate(ks, False, True)

        @pl.when(jnp.logical_not(straight))
        def _():
            propagate(ks, False, False)
        return carry

    lax.fori_loop(0, kmax // NEAR, near_body, 0)
    code_copy(1).wait_recv()
    code_copy(2).wait_recv()
    decode(1 - lat)

    def far_body(g, carry):
        ks = [g * FAR + n for n in range(FAR)]
        for k in ks:
            @pl.when(f0 + 2 * k < groups)
            def _():
                for s in range(2):
                    halo_wait(k, s)

        @pl.when(straight)
        def _():
            propagate(ks, True, False)

        @pl.when(jnp.logical_not(straight))
        def _():
            propagate(ks, True, True)
        return carry

    lax.fori_loop(0, kmax // FAR, far_body, 0)

    def own_copy(h):
        return pltpu.make_async_copy(
            away_ref.at[h, me, pl.ds(0, groups)],
            x_ref.at[h, 0, pl.ds(me * groups, groups), sub], o_sem.at[h])

    def own_forward(h):
        return pltpu.make_async_remote_copy(
            src_ref=away_ref.at[h, me, pl.ds(0, groups)],
            dst_ref=x_ref.at[h, 0, pl.ds(me * groups, groups), sub],
            send_sem=f_send.at[h, 0], recv_sem=f_recv.at[h, 0],
            device_id=partner, device_id_type=MESH)

    def forward(h, d):
        z = lax.rem(me + d, ncomp)
        span = x_ref.at[h, 0, pl.ds(z * groups, groups), sub]
        return pltpu.make_async_remote_copy(
            src_ref=span, dst_ref=span, send_sem=f_send.at[h, d], recv_sem=f_recv.at[h, d],
            device_id=partner, device_id_type=MESH)

    def forward_wait(h, d):
        z = lax.rem(me + d, ncomp)
        span = x_ref.at[h, 0, pl.ds(z * groups, groups), 1 - sub]
        pltpu.make_async_remote_copy(
            src_ref=span, dst_ref=span, send_sem=f_send.at[h, d], recv_sem=f_recv.at[h, d],
            device_id=partner, device_id_type=MESH).wait_recv()

    def prop_copy():
        return pltpu.make_async_remote_copy(
            src_ref=pout_ref.at[pl.ds(0, groups), pl.ds(2 * (1 - sub), 2)],
            dst_ref=pin_ref, send_sem=p_send, recv_sem=p_recv,
            device_id=partner, device_id_type=MESH)

    for d in range(1, ncomp):
        whole_copy(1, d).start()
    for h in range(2):
        own_copy(h).start()
        own_forward(h).start()
    prop_copy().start()
    load_w.wait()

    def collect(h):
        for d in range(1, ncomp):
            whole_wait(h, lax.rem(me + d, ncomp))
            forward(h, d).start()

    def complete(h):
        own_copy(h).wait()
        for d in range(ncomp):
            forward_wait(h, d)

    first = sub * tiles * groups

    def state_copy(h, step, m):
        span = x_ref.at[h, step + 1, pl.ds(first + m * groups, groups)]
        return pltpu.make_async_remote_copy(
            src_ref=span, dst_ref=span, send_sem=e_send.at[h, step, m], recv_sem=e_recv.at[h, step, m],
            device_id=partner, device_id_type=MESH)

    def state_wait(h, step, m):
        span = x_ref.at[h, step + 1, pl.ds((1 - sub) * tiles * groups + m * groups, groups)]
        pltpu.make_async_remote_copy(
            src_ref=span, dst_ref=span, send_sem=e_send.at[h, step, m], recv_sem=e_recv.at[h, step, m],
            device_id=partner, device_id_type=MESH).wait_recv()

    def home_copy(h, m):
        to = sub * tiles + m
        return to, pltpu.make_async_remote_copy(
            src_ref=inc_ref.at[h, m], dst_ref=home_ref.at[me],
            send_sem=b_send.at[h, m], recv_sem=b_recv.at[me],
            device_id={"comp": to, "sub": h}, device_id_type=MESH)

    def advance(h, step):
        def one(i, carry):
            m = lax.rem(i + 1 + me, tiles)
            rows = pl.ds(pl.multiple_of(m * bins, 16), bins)
            field = x_ref[h, step].reshape(total, lanes)
            driving = jnp.dot(w_ref[rows, :], field, preferred_element_type=F32)
            if step == 0:
                now = x_ref[h, 0, pl.ds(first + m * groups, groups)].reshape(bins, lanes).astype(F32)
            else:
                now = state_ref[h, rows, :]
            now = now + STEP_SIZE * now * driving
            if step < SRC_STEPS - 1:
                state_ref[h, rows, :] = now
                x_ref[h, step + 1, pl.ds(first + m * groups, groups)] = now.astype(BF16).reshape(
                    groups, 2, 16, lanes)
                state_copy(h, step, m).start()
            else:
                start = x_ref[h, 0, pl.ds(first + m * groups, groups)].reshape(bins, lanes).astype(F32)
                gain = (now - start).astype(BF16)
                inc_ref[h, m] = gain
                to, copy = home_copy(h, m)
                local = (to == me) & (sub == h)

                @pl.when(jnp.logical_not(local))
                def _():
                    copy.start()

                @pl.when(local)
                def _():
                    home_ref[me] = inc_ref[h, m]
            return carry

        if step > 0:
            for m in range(tiles):
                state_wait(h, step - 1, m)
        lax.fori_loop(0, tiles, one, 0)

    collect(0)
    complete(0)
    advance(0, 0)
    advance(0, 1)
    advance(0, 2)
    collect(1)
    advance(0, 3)
    complete(1)
    for step in range(SRC_STEPS):
        advance(1, step)

    sea_wide = [jnp.broadcast_to(sea[:, r * NLON:(r + 1) * NLON], (16, NLON)) for r in range(2)]
    prop_copy().wait_recv()

    def restore(j, carry):
        parts = [pout_ref[j, 2 * sub], pout_ref[j, 2 * sub + 1], pin_ref[j, 0], pin_ref[j, 1]]
        high, low = separate(jnp.concatenate(parts, axis=0))
        plain = (jnp.dot(high, perm_ref[1], preferred_element_type=F32)
                 + jnp.dot(low, perm_ref[1], preferred_element_type=F32))
        for n in range(4):
            p = sub if n < 2 else 1 - sub
            rows = pl.ds(pl.multiple_of((2 * j + p) * 16, 16), 16)
            r = n % 2
            out_ref[rows, r * NLON:(r + 1) * NLON] = sea_wide[r] * plain[n * 16:(n + 1) * 16, :]
        return carry

    lax.fori_loop(0, groups, restore, 0)

    mine_local = lax.div(me, tiles) == sub
    for d in (0, 1, 3, 2):
        z = lax.rem(me + d, ncomp)

        def land():
            pltpu.make_async_remote_copy(
                src_ref=inc_ref.at[0, 0], dst_ref=home_ref.at[z],
                send_sem=b_send.at[0, 0], recv_sem=b_recv.at[z],
                device_id={"comp": z}, device_id_type=MESH).wait_recv()

        if d == 0:
            pl.when(jnp.logical_not(mine_local))(land)
        else:
            land()
        r = lax.div(z, 2)
        half = lax.rem(z, 2)
        cols = pl.ds(pl.multiple_of(r * NLON, NLON), NLON)
        spread = perm_ref[1, pl.ds(pl.multiple_of(half * lanes, lanes), lanes), :]
        sea_row = jnp.where(r == 0, sea_wide[0][0:8], sea_wide[1][0:8])
        back = jnp.dot(home_ref[z], spread, preferred_element_type=F32)
        back = back.reshape(bins // 8, 8, NLON) * sea_row[None]
        out_ref[:, cols] = out_ref[:, cols] + back.reshape(bins, NLON)

    for n in range(3):
        code_copy(n).wait_send()
    raw_copy().wait_send()

    def halo_left(k, carry):
        @pl.when(n0 + 2 * k < groups)
        def _():
            for p in range(2):
                halo_copy(k, p).wait_send()
        return carry

    lax.fori_loop(0, kmax, halo_left, 0)
    prop_copy().wait_send()
    for h in range(2):
        own_forward(h).wait_send()
        for d in range(1, ncomp):
            whole_copy(h, d).wait_send()
            forward(h, d).wait_send()
        for m in range(tiles):
            for step in range(SRC_STEPS - 1):
                state_copy(h, step, m).wait_send()
            to, copy = home_copy(h, m)

            @pl.when(jnp.logical_not((to == me) & (sub == h)))
            def _():
                copy.wait_send()


def write_kernel(src_ref, dst_ref, sems):
    pieces = sems.shape[0]
    rows = src_ref.shape[0] // pieces
    copies = [pltpu.make_async_copy(
        src_ref.at[pl.ds(i * rows, rows)], dst_ref.at[pl.ds(i * rows, rows)], sems.at[i])
        for i in range(pieces)]
    for copy in copies:
        copy.start()
    for copy in copies:
        copy.wait()


def fast_device(ncomp, spectrum, sea_mask, neighbours, substeps, courant, source_operator):
    bins, points = spectrum.shape
    groups = bins // 32
    kmax = (groups + 1) // 2
    lanes = NLON // 2
    total = bins * ncomp
    tiles = ncomp // 2
    vmem = pl.BlockSpec(memory_space=pltpu.VMEM)
    smem = pl.BlockSpec(memory_space=pltpu.SMEM)
    hbm = pl.BlockSpec(memory_space=pl.ANY)
    dma = pltpu.SemaphoreType.DMA
    result = pl.pallas_call(
        functools.partial(fast_kernel, ncomp),
        out_shape=pltpu.VMEM((bins, points), F32),
        in_specs=[hbm, vmem, vmem, smem, smem, hbm],
        out_specs=vmem,
        scratch_shapes=[
            pltpu.VMEM((total // 2, total), BF16),
            pltpu.VMEM((2 * kmax, 4, 16, NLON), F32),
            pltpu.VMEM((2 * kmax, 2, 16, NLON), F32),
            pltpu.VMEM((kmax, 2, 2, 16, NLON), BF16),
            pltpu.VMEM((kmax, 4, 16, NLON), BF16),
            pltpu.VMEM((2, 2, 8, points), F32),
            pltpu.VMEM((2, 4, 5, 8, NLON), F32),
            pltpu.VMEM((2, 2, 16, lanes), F32),
            pltpu.VMEM((2, NLON, NLON), BF16),
            pltpu.VMEM((2 * kmax, 4, 16, NLON), F32),
            pltpu.VMEM((groups, 2, 16, NLON), F32),
            pltpu.VMEM((2, ncomp, 2 * kmax, 16, lanes), BF16),
            pltpu.VMEM((2, SRC_STEPS, ncomp * groups, 2, 16, lanes), BF16),
            pltpu.VMEM((2, total // 2, lanes), F32),
            pltpu.VMEM((2, tiles, bins, lanes), BF16),
            pltpu.VMEM((ncomp, bins, lanes), BF16),
            dma((4,)), dma, dma((3,)), dma((3,)), dma, dma,
            dma((kmax, 2)), dma((kmax, 2)), dma((2, ncomp)), dma((2, ncomp)), dma((2,)),
            dma((2, ncomp)), dma((2, ncomp)), dma, dma,
            dma((2, SRC_STEPS - 1, tiles)), dma((2, SRC_STEPS - 1, tiles)),
            dma((2, tiles)), dma((ncomp,)),
        ],
        compiler_params=pltpu.CompilerParams(
            collective_id=1, has_side_effects=True, vmem_limit_bytes=48 * 1024 * 1024),
    )(spectrum.reshape(groups, 2, 16, points), sea_mask.reshape(1, points), neighbours, substeps, courant,
      source_operator)
    return pl.pallas_call(
        write_kernel,
        out_shape=jax.ShapeDtypeStruct((bins, points), F32),
        in_specs=[vmem],
        out_specs=hbm,
        scratch_shapes=[dma((4,))],
        compiler_params=pltpu.CompilerParams(vmem_limit_bytes=4 * 1024 * 1024),
    )(result)


def solution(mesh):
    nlat, ncomp = mesh.shape["lat"], mesh.shape["comp"]

    def per_device(spectrum, sea_mask, neighbours, substeps, courant, source_operator):
        bins, points = spectrum.shape
        even = bins % 32 == 0 and (bins // 32 + 1) // 2 % NEAR == 0
        if nlat == 2 and ncomp == 4 and points == 2 * NLON and even:
            return fast_device(ncomp, spectrum, sea_mask, neighbours, substeps, courant, source_operator)
        size = 16 if bins % 16 == 0 else 8
        chunks = bins // size
        group = 5 if chunks % 5 == 0 else 1
        share = points // ncomp
        total = bins * ncomp
        angles = (np.arange(ND, dtype=np.float32) + np.float32(0.5)) * np.float32(2.0 * math.pi / ND)
        spread = lambda v: jnp.asarray(
            np.broadcast_to(np.abs(v).astype(np.float32)[:, None], (ND, NLON)).reshape(ND // 8, 8, NLON))
        vmem = pl.BlockSpec(memory_space=pltpu.VMEM)
        smem = pl.BlockSpec(memory_space=pltpu.SMEM)
        kinds = 3 if nlat == 2 else 4
        return pl.pallas_call(
            functools.partial(kernel, nlat, ncomp, group),
            out_shape=jax.ShapeDtypeStruct((bins, points), F32),
            in_specs=[vmem, vmem, vmem, smem, smem, vmem, vmem, pl.BlockSpec(memory_space=pl.ANY)],
            out_specs=vmem,
            scratch_shapes=[
                pltpu.VMEM((total, total), BF16),
                pltpu.VMEM((chunks + 2, size, points), BF16),
                pltpu.VMEM((3, chunks + 2, size, points), BF16),
                pltpu.VMEM((2, SLOTS, 4, 8, NLON), F32),
                pltpu.VMEM((chunks, size, points), F32),
                pltpu.VMEM((ncomp, chunks, size, share), BF16),
                pltpu.VMEM((ncomp, chunks, size, share), BF16),
                pltpu.VMEM((total, share), F32),
                pltpu.VMEM((total, share), F32),
                pltpu.VMEM((2, total, share), BF16),
                pltpu.VMEM((ncomp, bins, share), BF16),
                pltpu.VMEM((ncomp, bins, share), BF16),
                pltpu.SemaphoreType.DMA((kinds, chunks + 2)),
                pltpu.SemaphoreType.DMA((kinds, chunks + 2)),
                pltpu.SemaphoreType.DMA,
                pltpu.SemaphoreType.DMA,
                pltpu.SemaphoreType.DMA,
                pltpu.SemaphoreType.DMA((ncomp,)),
                pltpu.SemaphoreType.DMA((ncomp,)),
                pltpu.SemaphoreType.DMA((ncomp,)),
                pltpu.SemaphoreType.DMA((ncomp,)),
            ],
            compiler_params=pltpu.CompilerParams(
                collective_id=0, has_side_effects=True, vmem_limit_bytes=56 * 1024 * 1024),
        )(spectrum, sea_mask.reshape(1, points), neighbours, substeps, courant,
          spread(np.cos(angles)), spread(np.sin(angles)), source_operator)

    placed = (
        P("comp", ("members", "lat", "sub")),
        P(("members", "lat", "sub")),
        P(None, ("members", "lat", "sub")),
        P(),
        P(),
        P("sub", None),
    )
    return jax.shard_map(
        per_device,
        mesh=mesh,
        in_specs=placed,
        out_specs=P("comp", ("members", "lat", "sub")),
        check_vma=False,
    )
```

```python
import functools
import math

import jax
import jax.numpy as jnp
import numpy as np
from jax import lax
from jax.experimental import pallas as pl
from jax.experimental.pallas import tpu as pltpu
from jax.sharding import PartitionSpec as P

NF = 30
ND = 64
NLON = 256
MAXSTEPS = 6
SRC_STEPS = 4
STEP_SIZE = 0.1
MESH = pl.DeviceIdType.MESH
HALF = ND // 2
TILES = 4
SLOTS = 8
NEAR = 4
FAR = 2
BACK = 5
F32 = jnp.float32
BF16 = jnp.bfloat16


def kernel(
    nlat, ncomp, group, spec_ref, mask_ref, nb_ref, steps_ref, cour_ref, cos_ref, sin_ref, op_ref,
    out_ref, w_ref, own_ref, halo_ref, code_ref, prop_ref, away_ref, got_ref, start_ref, state_ref,
    low_ref, inc_ref, home_ref,
    h_send, h_recv, w_send, w_recv, w_local, a_send, a_recv, b_send, b_recv,
):
    lat = lax.axis_index("lat")
    sub = lax.axis_index("sub")
    me = lax.axis_index("comp")
    bins, points = spec_ref.shape
    chunks, size = prop_ref.shape[0], prop_ref.shape[1]
    planes = size // 8
    share = points // ncomp
    total = bins * ncomp
    half_rows = total // 2
    first = me * bins
    last_lat = nlat - 1
    partner = {"sub": 1 - sub}

    barrier = pltpu.get_barrier_semaphore()
    peers = [partner]
    if nlat == 2:
        peers.append({"lat": 1 - lat})
    else:
        for move in (1, -1):
            peers.append({"lat": lax.rem(lat + move + nlat, nlat)})
            peers.append({"lat": lax.rem(lat + 2 * move + nlat, nlat), "sub": 1 - sub})
    for j in range(1, ncomp):
        peers.append({"comp": lax.rem(me + j, ncomp)})
    for peer in peers:
        pl.semaphore_signal(barrier, inc=1, device_id=peer, device_id_type=MESH)

    own_half = pl.ds(pl.multiple_of(sub * half_rows, 16), half_rows)
    load_w = pltpu.make_async_copy(op_ref, w_ref.at[own_half], w_local)
    load_w.start()

    lane = lax.broadcasted_iota(jnp.int32, (1, points), 1)
    column = lane & (NLON - 1)
    position = (lat * 2 + sub) * points + lane
    sea = mask_ref[...].astype(F32)
    west = (column - nb_ref[0:1, :]) & (NLON - 1)
    east = (nb_ref[1:2, :] - column) & (NLON - 1)

    def vertical(index_row):
        moved = ((index_row - column + 1) & (NLON - 1)) - 1
        return jnp.where(index_row == position, 2, moved)

    rows = lax.broadcasted_iota(jnp.int32, (size, points), 0)
    codes = jnp.zeros((size, points), F32)
    entries = [west, east, vertical(nb_ref[2:3, :]), vertical(nb_ref[3:4, :])]
    for k, entry in enumerate([e.astype(F32) for e in entries] + [sea]):
        codes = jnp.where(rows == k, jnp.broadcast_to(entry, (size, points)), codes)
    own_ref[0] = codes.astype(BF16)
    own_ref[1] = codes.astype(BF16)

    pl.semaphore_wait(barrier, len(peers))

    def kind(q):
        return lax.rem(lax.div(first + (q - 2) * size, HALF), 2)

    def has_from(ty, far):
        return jnp.where(ty == 0, lat >= far, lat <= last_lat - far)

    def has_to(ty, far):
        return jnp.where(ty == 0, lat <= last_lat - far, lat >= far)

    def pair_copy(q):
        return pltpu.make_async_remote_copy(
            src_ref=own_ref.at[q], dst_ref=halo_ref.at[0, q], send_sem=h_send.at[0, q],
            recv_sem=h_recv.at[0, q], device_id=partner, device_id_type=MESH)

    def side_copy(q, ty):
        to = jnp.clip(lat + 1 - 2 * ty, 0, last_lat)
        return pltpu.make_async_remote_copy(
            src_ref=own_ref.at[q], dst_ref=halo_ref.at[1, q], send_sem=h_send.at[1, q],
            recv_sem=h_recv.at[1, q], device_id={"lat": to}, device_id_type=MESH)

    def hand_copy(q, ty):
        slot = jnp.where(sub == ty, 2, 0)
        return pltpu.make_async_remote_copy(
            src_ref=halo_ref.at[1, q], dst_ref=halo_ref.at[slot, q], send_sem=h_send.at[2, q],
            recv_sem=h_recv.at[2, q], device_id=partner, device_id_type=MESH)

    def far_copy(q, ty):
        to = jnp.clip(lat + 2 - 4 * ty, 0, last_lat)
        return pltpu.make_async_remote_copy(
            src_ref=own_ref.at[q], dst_ref=halo_ref.at[2, q], send_sem=h_send.at[3, q],
            recv_sem=h_recv.at[3, q], device_id={"lat": to, "sub": 1 - sub}, device_id_type=MESH)

    def send_own(q, ty):
        @pl.when(has_to(ty, 1))
        def _():
            side_copy(q, ty).start()

        @pl.when(sub == ty)
        def _():
            pair_copy(q).start()

        if nlat > 2:
            @pl.when((sub != ty) & has_to(ty, 2))
            def _():
                far_copy(q, ty).start()

    def hand_on(q, ty):
        @pl.when(has_from(ty, 1))
        def _():
            side_copy(q, ty).wait_recv()
            hand_copy(q, ty).start()

    def arrive(q, ty):
        @pl.when(has_from(ty, 1))
        def _():
            hand_copy(q, ty).wait_recv()

        @pl.when(sub != ty)
        def _():
            pair_copy(q).wait_recv()

        if nlat > 2:
            @pl.when((sub == ty) & has_from(ty, 2))
            def _():
                far_copy(q, ty).wait_recv()

    def sent(q, ty):
        @pl.when(has_to(ty, 1))
        def _():
            side_copy(q, ty).wait_send()

        @pl.when(sub == ty)
        def _():
            pair_copy(q).wait_send()

        if nlat > 2:
            @pl.when((sub != ty) & has_to(ty, 2))
            def _():
                far_copy(q, ty).wait_send()

        @pl.when(has_from(ty, 1))
        def _():
            hand_copy(q, ty).wait_send()

    send_own(0, 0)
    send_own(1, 1)

    def prepare(i, carry):
        chunk = sea * spec_ref[pl.ds(pl.multiple_of(i * size, size), size), :]
        own_ref[i + 2] = chunk.astype(BF16)
        send_own(i + 2, kind(i + 2))
        return carry

    lax.fori_loop(0, chunks, prepare, 0)

    give_w = pltpu.make_async_remote_copy(
        src_ref=op_ref, dst_ref=w_ref.at[own_half], send_sem=w_send, recv_sem=w_recv,
        device_id=partner, device_id_type=MESH)
    give_w.start()

    for q in (0, 1):
        hand_on(q, q)
    ahead = min(6, chunks)
    for q in range(2, 2 + ahead):
        hand_on(q, kind(q))

    for ty in (0, 1):
        arrive(ty, ty)
        for slot in range(SLOTS):
            row = slot % 2 if ty == 0 else 1 - slot % 2
            cols = slice(row * NLON, (row + 1) * NLON)
            if slot < 6:
                part = halo_ref[2 - slot // 2, ty, :, cols].astype(F32)
            else:
                part = own_ref[ty, :, cols].astype(F32)
            for k, source in enumerate((0, 1, 2 + ty, 4)):
                code_ref[ty, slot, k] = jnp.broadcast_to(part[source:source + 1, :], (8, NLON))

    def propagate(i):
        q = i + 2
        ty = kind(q)

        @pl.when(i + ahead < chunks)
        def _():
            hand_on(q + ahead, kind(q + ahead))

        arrive(q, ty)
        bin0 = first + i * size
        freq = lax.div(bin0, ND)
        direction = lax.rem(bin0, ND)
        to_east = jnp.where((direction < ND // 4) | (direction >= 3 * ND // 4), 1, 0)
        steps = steps_ref[freq]
        speed = cour_ref[freq]
        sign = jnp.where(to_east == 1, 1.0, -1.0)
        shift1 = jnp.where(to_east == 1, 1, NLON - 1)
        shift2 = jnp.where(to_east == 1, 2, NLON - 2)
        back1 = NLON - shift1
        d8 = lax.div(direction, 8)
        abs_cos = cos_ref[pl.ds(d8, planes)]
        abs_sin = sin_ref[pl.ds(d8, planes)]

        def lanes(slot):
            row = jnp.where(ty == 0, slot % 2, 1 - slot % 2)
            return pl.ds(pl.multiple_of(row * NLON, NLON), NLON)

        values = []
        for slot in range(SLOTS):
            if slot < 6:
                part = halo_ref[2 - slot // 2, q, :, lanes(slot)].astype(F32)
            else:
                part = spec_ref[pl.ds(pl.multiple_of(i * size, size), size), lanes(slot)]
            part = part.reshape(planes, 8, NLON)
            if slot >= 6:
                part = part * code_ref[ty, slot, 3][None]
            values.append(part)
        for t in range(MAXSTEPS):
            live = jnp.where(t < steps, speed, 0.0)
            wx = live * abs_cos
            wy = live * abs_sin
            keep = 1.0 - wx - wy
            fresh = list(values)
            for slot in range(t + 1, SLOTS):
                x = values[slot]
                below = values[slot - 1]
                near = code_ref[ty, slot, 1 - to_east][None] == 1.0
                vert = code_ref[ty, slot, 2][None] * sign
                lon = jnp.where(near, pltpu.roll(x, shift1, 2), pltpu.roll(x, shift2, 2))
                up = jnp.where(vert == -1.0, pltpu.roll(below, shift1, 2),
                               jnp.where(vert == 1.0, pltpu.roll(below, back1, 2), below))
                up = jnp.where(jnp.abs(vert) == 2.0, x, up)
                fresh[slot] = code_ref[ty, slot, 3][None] * (keep * x + wx * lon + wy * up)
            values = fresh
        for slot in (6, 7):
            prop_ref[i, :, lanes(slot)] = values[slot].reshape(size, NLON)
        whole = prop_ref[i]
        for c in range(ncomp):
            away_ref[c, i] = whole[:, c * share:(c + 1) * share].astype(BF16)

    groups = chunks // group

    def out_copy(j, g):
        to = lax.rem(me + j, ncomp)
        span = pl.ds(g * group, group)
        return pltpu.make_async_remote_copy(
            src_ref=away_ref.at[to, span], dst_ref=got_ref.at[me, span],
            send_sem=a_send.at[j], recv_sem=a_recv.at[j],
            device_id={"comp": to}, device_id_type=MESH)

    def whole_copy(j):
        to = lax.rem(me + j, ncomp)
        return pltpu.make_async_remote_copy(
            src_ref=away_ref.at[to], dst_ref=got_ref.at[me],
            send_sem=a_send.at[j], recv_sem=a_recv.at[j],
            device_id={"comp": to}, device_id_type=MESH)

    def run_group(g, carry):
        def one(i, inner):
            propagate(g * group + i)
            return inner

        lax.fori_loop(0, group, one, 0)
        for j in range(1, ncomp):
            out_copy(j, g).start()
        return carry

    lax.fori_loop(0, groups, run_group, 0)

    for q in (0, 1):
        sent(q, q)

    def drain(q, carry):
        sent(q, kind(q))
        return carry

    lax.fori_loop(2, chunks + 2, drain, 0)
    got_ref[me] = away_ref[me]
    load_w.wait()
    give_w.wait()

    for j in range(1, ncomp):
        whole_copy(j).wait()
    for c in range(ncomp):
        start_ref[c * bins:(c + 1) * bins, :] = got_ref[c].astype(F32).reshape(bins, share)
    tile = total // TILES
    per_tile = bins // tile if bins >= tile else tile // bins
    for m in range(TILES):
        span = slice(m * tile, (m + 1) * tile)
        low_ref[0, span, :] = start_ref[span, :].astype(BF16)

    def tile_rows(m):
        return pl.ds(pl.multiple_of(m * tile, 16), tile)

    def advance(step, m):
        span = tile_rows(m)
        driving = jnp.dot(w_ref[span, :], low_ref[step % 2], preferred_element_type=F32)
        now = start_ref[span, :] if step == 0 else state_ref[span, :]
        return span, now + STEP_SIZE * now * driving

    for step in range(SRC_STEPS - 1):
        def one_tile(m, carry, step=step):
            span, now = advance(step, m)
            state_ref[span, :] = now
            low_ref[(step + 1) % 2, span, :] = now.astype(BF16)
            return carry

        lax.fori_loop(0, TILES, one_tile, 0)

    def home_copy(j, to):
        return pltpu.make_async_remote_copy(
            src_ref=inc_ref.at[to], dst_ref=home_ref.at[me],
            send_sem=b_send.at[j], recv_sem=b_recv.at[j],
            device_id={"comp": to}, device_id_type=MESH)

    mine = lax.div(me * TILES, ncomp)

    def last_tile(i, carry):
        m = lax.rem(mine + 1 + i, TILES)
        span, now = advance(SRC_STEPS - 1, m)
        gain = now - start_ref[span, :]
        for k in range(per_tile):
            to = m * per_tile + k
            inc_ref[to] = gain[k * bins:(k + 1) * bins, :].astype(BF16)
            j = lax.rem(to - me + ncomp, ncomp)

            @pl.when(to != me)
            def _():
                home_copy(j, to).start()

        return carry

    lax.fori_loop(0, TILES, last_tile, 0)
    home_ref[me] = inc_ref[me]
    for c in range(ncomp):
        j = lax.rem(me - c + ncomp, ncomp)

        @pl.when(me != c)
        def _():
            home_copy(j, lax.rem(me + j, ncomp)).wait()

        cols = slice(c * share, (c + 1) * share)
        before = prop_ref[:, :, cols].reshape(bins, share)
        out_ref[:, cols] = sea[:, cols] * (before + home_ref[c].astype(F32))


def fast_kernel(
    ncomp, spec_ref, mask_hbm, nb_hbm, steps_hbm, cour_hbm, op_ref,
    out_ref, mask_ref, nb_ref, steps_ref, cour_ref, w_ref, full_ref, oth_ref, hsend_ref, halo_ref, raw_ref, code_ref, ang_ref, perm_ref,
    pout_ref, pin_ref, away_ref, x_ref, start_ref, state_ref, inc_ref, home_ref,
    l_sem, i_sem, w_sem, c_send, c_recv, r_send, r_recv, g_send, g_recv, h_send, h_recv,
    a_send, a_recv, o_sem, p_send, p_recv, b_send, b_recv,
):
    lat = lax.axis_index("lat")
    sub = lax.axis_index("sub")
    me = lax.axis_index("comp")
    groups = spec_ref.shape[0]
    bins = groups * 2 * 16
    kmax = halo_ref.shape[0]
    lanes = NLON // 2
    total = bins * ncomp
    partner = {"sub": 1 - sub}
    others = [partner, {"lat": 1 - lat}, {"lat": 1 - lat, "sub": 1 - sub}]

    small = [pltpu.make_async_copy(src, dst, i_sem.at[n]) for n, (src, dst) in enumerate((
        (mask_hbm, mask_ref), (nb_hbm, nb_ref), (steps_hbm, steps_ref), (cour_hbm, cour_ref)))]
    for load in small:
        load.start()
    loads = []
    for r in range(2):
        cols = slice(r * NLON, (r + 1) * NLON)
        loads.append(pltpu.make_async_copy(
            spec_ref.at[:, 1 - sub, :, cols], oth_ref.at[pl.ds(0, groups), r], l_sem.at[r]))
        loads.append(pltpu.make_async_copy(
            spec_ref.at[:, sub, :, cols], full_ref.at[pl.ds(0, groups), 2 * sub + r], l_sem.at[2 + r]))
    for load in (loads[0], loads[2], loads[1], loads[3]):
        load.start()
    own_half = pl.ds(pl.multiple_of(sub * (total // 2), 16), total // 2)
    load_w = pltpu.make_async_copy(op_ref, w_ref.at[own_half], w_sem)

    barrier = pltpu.get_barrier_semaphore()
    peers = list(others)
    for d in range(1, ncomp):
        z = lax.rem(me + d, ncomp)
        peers += [{"comp": z}, {"comp": z, "sub": 1 - sub}]
    for peer in peers:
        pl.semaphore_signal(barrier, inc=1, device_id=peer, device_id_type=MESH)
    load_w.start()
    for load in small:
        load.wait()

    points = mask_ref.shape[1]
    lane = lax.broadcasted_iota(jnp.int32, (1, points), 1)
    column = lane & (NLON - 1)
    sea = mask_ref[...].astype(F32)
    west = (column - nb_ref[0:1, :]) & (NLON - 1)
    east = (nb_ref[1:2, :] - column) & (NLON - 1)
    moves = [((nb_ref[k:k + 1, :] - column + 1) & (NLON - 1)) - 1 for k in (2, 3)]
    index = lax.broadcasted_iota(jnp.int32, (8, points), 0)
    codes = jnp.zeros((8, points), F32)
    for k, entry in enumerate([e.astype(F32) for e in (west, east, *moves)] + [sea]):
        codes = jnp.where(index == k, jnp.broadcast_to(entry, (8, points)), codes)
    raw_ref[lat, sub] = codes

    a = lax.broadcasted_iota(jnp.int32, (NLON, NLON), 0)
    b = lax.broadcasted_iota(jnp.int32, (NLON, NLON), 1)
    split = lambda c: jnp.where(c < lanes, 2 * c, 2 * (c - lanes) + 1)
    perm_ref[0] = (a == split(b)).astype(F32).astype(BF16)
    perm_ref[1] = (b == split(a)).astype(F32).astype(BF16)

    near_ty = lat
    far_ty = 1 - lat
    n0 = lax.rem(lat + me * groups, 2)
    f0 = 1 - n0
    for q, ty in enumerate((near_ty, far_ty)):
        d = lax.broadcasted_iota(jnp.int32, (16, lanes), 0) + 16 * (2 * ty + sub)
        angle = (d.astype(F32) + 0.5) * np.float32(2.0 * math.pi / ND)
        ang_ref[q, 0] = jnp.abs(jnp.cos(angle))
        ang_ref[q, 1] = jnp.abs(jnp.sin(angle))

    for load in loads:
        load.wait()
    sea_rows = [jnp.broadcast_to(sea[:, r * NLON:(r + 1) * NLON], (16, NLON)) for r in range(2)]

    def convert(k, carry):
        j = n0 + 2 * k
        for r in range(2):
            mine = full_ref[j, 2 * sub + r] * sea_rows[r]
            other = oth_ref[j, r] * sea_rows[r]
            hsend_ref[k, sub, r] = mine.astype(BF16)
            hsend_ref[k, 1 - sub, r] = other.astype(BF16)
        return carry

    lax.fori_loop(0, kmax, convert, 0)
    pl.semaphore_wait(barrier, len(peers))

    def code_copy(n):
        return pltpu.make_async_remote_copy(
            src_ref=raw_ref.at[lat, sub], dst_ref=raw_ref.at[lat, sub], send_sem=c_send.at[n],
            recv_sem=c_recv.at[n], device_id=others[n], device_id_type=MESH)

    def raw_copy():
        return pltpu.make_async_remote_copy(
            src_ref=oth_ref.at[pl.ds(0, groups)],
            dst_ref=full_ref.at[pl.ds(0, groups), pl.ds(2 * sub, 2)],
            send_sem=r_send, recv_sem=r_recv, device_id=partner, device_id_type=MESH)

    def halo_copy(k, p):
        return pltpu.make_async_remote_copy(
            src_ref=hsend_ref.at[k, p], dst_ref=halo_ref.at[k, pl.ds(2 * sub, 2)],
            send_sem=h_send.at[k, p], recv_sem=h_recv.at[k, sub],
            device_id={"lat": 1 - lat, "sub": p}, device_id_type=MESH)

    def halo_wait(k, s):
        pltpu.make_async_remote_copy(
            src_ref=hsend_ref.at[k, s], dst_ref=halo_ref.at[k, pl.ds(2 * s, 2)],
            send_sem=h_send.at[k, s], recv_sem=h_recv.at[k, s],
            device_id={"lat": 1 - lat, "sub": s}, device_id_type=MESH).wait_recv()

    code_copy(0).start()
    raw_copy().start()
    code_copy(1).start()
    code_copy(2).start()

    def give_w():
        return pltpu.make_async_remote_copy(
            src_ref=op_ref, dst_ref=w_ref.at[own_half], send_sem=g_send, recv_sem=g_recv,
            device_id=partner, device_id_type=MESH)

    def take_w():
        other_half = pl.ds(pl.multiple_of((1 - sub) * (total // 2), 16), total // 2)
        return pltpu.make_async_remote_copy(
            src_ref=op_ref, dst_ref=w_ref.at[other_half], send_sem=g_send, recv_sem=g_recv,
            device_id=partner, device_id_type=MESH)

    def send_halo(k, carry):
        @pl.when(n0 + 2 * k < groups)
        def _():
            for p in range(2):
                halo_copy(k, p).start()
        return carry

    lax.fori_loop(0, kmax, send_halo, 0)
    give_w().start()

    def decode(chip):
        for s in range(2):
            for r in range(2):
                part = raw_ref[chip, s, :, r * NLON:(r + 1) * NLON].astype(BF16)
                both = jnp.dot(part, perm_ref[0], preferred_element_type=F32)
                for k in range(5):
                    code_ref[chip, 2 * s + r, k] = jnp.broadcast_to(both[k:k + 1, :], (8, NLON))

    side = lax.div(me, 2)

    def target(i):
        near = me + 1 - 2 * lax.rem(me, 2)
        return jnp.where(i == 0, 3 - 3 * side, jnp.where(i == 1, 2 - side, jnp.where(i == 2, near, me)))

    def chunk_copy(h, j, i):
        to = target(i)
        return pltpu.make_async_remote_copy(
            src_ref=away_ref.at[h, to, j], dst_ref=x_ref.at[0, me * groups + j, sub],
            send_sem=a_send.at[h, i], recv_sem=a_recv.at[me, sub],
            device_id={"comp": to, "sub": h}, device_id_type=MESH)

    def whole_copy(h, i):
        to = target(i)
        return pltpu.make_async_remote_copy(
            src_ref=away_ref.at[h, to, pl.ds(0, groups)],
            dst_ref=x_ref.at[0, pl.ds(me * groups, groups), sub],
            send_sem=a_send.at[h, i], recv_sem=a_recv.at[me, sub],
            device_id={"comp": to, "sub": h}, device_id_type=MESH)

    def whole_wait(z, s):
        pltpu.make_async_remote_copy(
            src_ref=away_ref.at[0, z, pl.ds(0, groups)],
            dst_ref=x_ref.at[0, pl.ds(z * groups, groups), s],
            send_sem=a_send.at[0, 0], recv_sem=a_recv.at[z, s],
            device_id={"comp": z, "sub": s}, device_id_type=MESH).wait_recv()

    def pick(ty, i):
        return ty * 3 + (1 - 2 * ty) * i

    def separate(x):
        high = x.astype(BF16)
        low = (x - high.astype(F32)).astype(BF16)
        return high, low

    def propagate(ks, far, to_east):
        ty = far_ty if far else near_ty
        js = [(f0 if far else n0) + 2 * k for k in ks]
        vert = 2 + ty
        lowest = 0 if far else 4

        def code(q, k, half):
            chip = lat if q >= 4 else 1 - lat
            part = code_ref[chip, pick(ty, q % 4), k, :, half * lanes:(half + 1) * lanes]
            return jnp.concatenate([part, part], axis=0)

        raw = jnp.concatenate([full_ref[j, pick(ty, i)] for j in js for i in range(4)], axis=0)
        high, low = separate(raw)
        mixed = (jnp.dot(high, perm_ref[0], preferred_element_type=F32)
                 + jnp.dot(low, perm_ref[0], preferred_element_type=F32))
        if far:
            edge = jnp.concatenate([halo_ref[k, pick(ty, i)] for k in ks for i in range(4)], axis=0)
            edge = jnp.dot(edge, perm_ref[0], preferred_element_type=F32)
        cells = []
        weights = []
        for n, j in enumerate(js):
            values = [None] * 8
            for i in range(4):
                rows = slice((n * 4 + i) * 16, (n * 4 + i + 1) * 16)
                values[4 + i] = tuple(
                    mixed[rows, half * lanes:(half + 1) * lanes] * code(4 + i, 4, half)
                    for half in range(2))
                if far:
                    values[i] = tuple(edge[rows, half * lanes:(half + 1) * lanes] for half in range(2))
            cells.append(values)
            freq = jnp.minimum(lax.div(me * bins + j * 32, ND), steps_ref.shape[0] - 1)
            weights.append((steps_ref[freq], cour_ref[freq]))
        abs_cos, abs_sin = ang_ref[int(far), 0], ang_ref[int(far), 1]
        ahead, behind = (1, lanes - 1)
        for t in range(MAXSTEPS):
            slots = [q for q in range(7, lowest - 1, -1) if q >= 4 or t <= q + 1]
            for n, (steps, speed) in enumerate(weights):
                live = jnp.where(t < steps, speed, 0.0)
                wx = live * abs_cos
                wy = live * abs_sin
                keep = 1.0 - wx - wy
                values = cells[n]
                fresh = list(values)
                turned = {}

                def turn(q, half, shift):
                    key = (q, half, shift)
                    if key not in turned:
                        turned[key] = pltpu.roll(values[q][half], shift, 1)
                    return turned[key]

                def left(q):
                    return turn(q, 1, ahead), values[q][0]

                def right(q):
                    return values[q][1], turn(q, 0, behind)

                for q in slots:
                    shift = ahead if to_east else behind
                    one = left(q) if to_east else right(q)
                    lon_code = 0 if to_east else 1
                    new = []
                    for half in range(2):
                        x = values[q][half]
                        lon = jnp.where(code(q, lon_code, half) == 1.0, one[half], turn(q, half, shift))
                        if q == lowest:
                            up = x
                        else:
                            move = code(q, vert, half)
                            up = jnp.where(move == -1.0, left(q - 1)[half],
                                           jnp.where(move == 1.0, right(q - 1)[half], values[q - 1][half]))
                        new.append(code(q, 4, half) * (keep * x + wx * lon + wy * up))
                    fresh[q] = tuple(new)
                cells[n] = fresh
        for n, j in enumerate(js):
            for i in range(4):
                r = pick(ty, i)
                for half in range(2):
                    value = cells[n][4 + i][half]
                    pout_ref[j, r, :, half * lanes:(half + 1) * lanes] = value
                    away_ref[lax.div(r, 2), 2 * lax.rem(r, 2) + half, j] = value.astype(BF16)
        for n, j in enumerate(js):
            @pl.when(j < groups)
            def _():
                for i in range(ncomp - 1):
                    chunk_copy(0, j, i).start()

    straight = sub == lat
    code_copy(0).wait_recv()
    decode(lat)
    raw_copy().wait_recv()

    def near_body(g, carry):
        ks = [g * NEAR + n for n in range(NEAR)]

        @pl.when(straight)
        def _():
            propagate(ks, False, True)

        @pl.when(jnp.logical_not(straight))
        def _():
            propagate(ks, False, False)
        return carry

    lax.fori_loop(0, kmax // NEAR, near_body, 0)
    code_copy(1).wait_recv()
    code_copy(2).wait_recv()
    decode(1 - lat)

    def far_body(g, carry):
        ks = [g * FAR + n for n in range(FAR)]
        for k in ks:
            @pl.when(f0 + 2 * k < groups)
            def _():
                for s in range(2):
                    halo_wait(k, s)

        @pl.when(straight)
        def _():
            propagate(ks, True, False)

        @pl.when(jnp.logical_not(straight))
        def _():
            propagate(ks, True, True)
        return carry

    lax.fori_loop(0, kmax // FAR, far_body, 0)

    own_copy = pltpu.make_async_copy(
        away_ref.at[sub, me, pl.ds(0, groups)], x_ref.at[0, pl.ds(me * groups, groups), sub], o_sem)

    def cross_copy():
        return pltpu.make_async_remote_copy(
            src_ref=away_ref.at[1 - sub, me, pl.ds(0, groups)],
            dst_ref=x_ref.at[0, pl.ds(me * groups, groups), sub],
            send_sem=a_send.at[0, ncomp - 1], recv_sem=a_recv.at[me, sub],
            device_id=partner, device_id_type=MESH)

    def prop_copy():
        return pltpu.make_async_remote_copy(
            src_ref=pout_ref.at[pl.ds(0, groups), pl.ds(2 * (1 - sub), 2)],
            dst_ref=pin_ref, send_sem=p_send, recv_sem=p_recv,
            device_id=partner, device_id_type=MESH)

    own_copy.start()
    cross_copy().start()
    for i in range(ncomp - 1):
        whole_copy(1, i).start()
    prop_copy().start()

    def home_copy(m):
        return pltpu.make_async_remote_copy(
            src_ref=inc_ref.at[m], dst_ref=home_ref.at[me],
            send_sem=b_send.at[m], recv_sem=b_recv.at[me],
            device_id={"comp": m}, device_id_type=MESH)

    def advance(step):
        def one(i, carry):
            m = target(i)
            rows = pl.ds(pl.multiple_of(m * bins, 16), bins)
            units = pl.ds(m * groups, groups)
            field = x_ref[step % 2].reshape(total, lanes)
            driving = jnp.dot(w_ref[rows, :], field, preferred_element_type=F32)
            if step == 0:
                now = x_ref[0, units].reshape(bins, lanes).astype(F32)
                start_ref[rows, :] = now
            else:
                now = state_ref[rows, :]
            now = now + STEP_SIZE * now * driving
            if step < SRC_STEPS - 1:
                state_ref[rows, :] = now
                x_ref[(step + 1) % 2, units] = now.astype(BF16).reshape(groups, 2, 16, lanes)
            else:
                inc_ref[m] = (now - start_ref[rows, :]).astype(BF16)

                @pl.when(m != me)
                def _():
                    home_copy(m).start()
            return carry

        lax.fori_loop(0, ncomp, one, 0)

    sea_wide = [jnp.broadcast_to(sea[:, r * NLON:(r + 1) * NLON], (16, NLON)) for r in range(2)]

    def restore(g, carry):
        js = [g * BACK + n for n in range(BACK)]
        parts = [ref for j in js for ref in (
            pout_ref[j, 2 * sub], pout_ref[j, 2 * sub + 1], pin_ref[j, 0], pin_ref[j, 1])]
        high, low = separate(jnp.concatenate(parts, axis=0))
        plain = (jnp.dot(high, perm_ref[1], preferred_element_type=F32)
                 + jnp.dot(low, perm_ref[1], preferred_element_type=F32))
        for n in range(4 * BACK):
            p = sub if n % 4 < 2 else 1 - sub
            rows = pl.ds(pl.multiple_of((2 * js[n // 4] + p) * 16, 16), 16)
            r = n % 2
            out_ref[rows, r * NLON:(r + 1) * NLON] = sea_wide[r] * plain[n * 16:(n + 1) * 16, :]
        return carry

    def restore_all():
        prop_copy().wait_recv()
        lax.fori_loop(0, groups // BACK, restore, 0)

    pl.when(sub == 1)(restore_all)
    load_w.wait()
    take_w().wait_recv()
    own_copy.wait()
    for z in range(ncomp):
        for s in range(2):
            @pl.when((z != me) | (s != sub))
            def _():
                whole_wait(z, s)

    for step in range(SRC_STEPS):
        advance(step)

    pl.when(sub == 0)(restore_all)
    for i in (3, 2, 1, 0):
        z = target(i)

        def land():
            pltpu.make_async_remote_copy(
                src_ref=inc_ref.at[z], dst_ref=home_ref.at[z],
                send_sem=b_send.at[z], recv_sem=b_recv.at[z],
                device_id={"comp": z}, device_id_type=MESH).wait_recv()

        if i < 3:
            land()
        r = lax.div(z, 2)
        half = lax.rem(z, 2)
        cols = pl.ds(pl.multiple_of(r * NLON, NLON), NLON)
        spread = perm_ref[1, pl.ds(pl.multiple_of(half * lanes, lanes), lanes), :]
        sea_row = jnp.where(r == 0, sea_wide[0][0:8], sea_wide[1][0:8])
        arrived = inc_ref[z] if i == 3 else home_ref[z]
        back = jnp.dot(arrived, spread, preferred_element_type=F32)
        back = back.reshape(bins // 8, 8, NLON) * sea_row[None]
        out_ref[:, cols] = out_ref[:, cols] + back.reshape(bins, NLON)

    for n in range(3):
        code_copy(n).wait_send()
    raw_copy().wait_send()

    def halo_left(k, carry):
        @pl.when(n0 + 2 * k < groups)
        def _():
            for p in range(2):
                halo_copy(k, p).wait_send()
        return carry

    lax.fori_loop(0, kmax, halo_left, 0)
    prop_copy().wait_send()
    cross_copy().wait_send()
    give_w().wait_send()
    for i in range(ncomp - 1):
        for h in range(2):
            whole_copy(h, i).wait_send()
        home_copy(target(i)).wait_send()


def write_kernel(src_ref, dst_ref, sems):
    pieces = sems.shape[0]
    rows = src_ref.shape[0] // pieces
    copies = [pltpu.make_async_copy(
        src_ref.at[pl.ds(i * rows, rows)], dst_ref.at[pl.ds(i * rows, rows)], sems.at[i])
        for i in range(pieces)]
    for copy in copies:
        copy.start()
    for copy in copies:
        copy.wait()


def fast_device(ncomp, spectrum, sea_mask, neighbours, substeps, courant, source_operator):
    bins, points = spectrum.shape
    groups = bins // 32
    kmax = (groups + 1) // 2
    lanes = NLON // 2
    total = bins * ncomp
    vmem = pl.BlockSpec(memory_space=pltpu.VMEM)
    hbm = pl.BlockSpec(memory_space=pltpu.HBM)
    dma = pltpu.SemaphoreType.DMA
    result = pl.pallas_call(
        functools.partial(fast_kernel, ncomp),
        out_shape=pltpu.VMEM((bins, points), F32),
        in_specs=[hbm] * 6,
        out_specs=vmem,
        scratch_shapes=[
            pltpu.VMEM((1, points), jnp.int32),
            pltpu.VMEM((4, points), jnp.int32),
            pltpu.SMEM(substeps.shape, jnp.int32),
            pltpu.SMEM(courant.shape, F32),
            pltpu.VMEM((total, total), BF16),
            pltpu.VMEM((2 * kmax, 4, 16, NLON), F32),
            pltpu.VMEM((2 * kmax, 2, 16, NLON), F32),
            pltpu.VMEM((kmax, 2, 2, 16, NLON), BF16),
            pltpu.VMEM((kmax, 4, 16, NLON), BF16),
            pltpu.VMEM((2, 2, 8, points), F32),
            pltpu.VMEM((2, 4, 5, 8, NLON), F32),
            pltpu.VMEM((2, 2, 16, lanes), F32),
            pltpu.VMEM((2, NLON, NLON), BF16),
            pltpu.VMEM((2 * kmax, 4, 16, NLON), F32),
            pltpu.VMEM((groups, 2, 16, NLON), F32),
            pltpu.VMEM((2, ncomp, 2 * kmax, 16, lanes), BF16),
            pltpu.VMEM((2, ncomp * groups, 2, 16, lanes), BF16),
            pltpu.VMEM((total, lanes), F32),
            pltpu.VMEM((total, lanes), F32),
            pltpu.VMEM((ncomp, bins, lanes), BF16),
            pltpu.VMEM((ncomp, bins, lanes), BF16),
            dma((4,)), dma((4,)), dma, dma((3,)), dma((3,)), dma, dma, dma, dma,
            dma((kmax, 2)), dma((kmax, 2)), dma((2, ncomp)), dma((ncomp, 2)), dma, dma, dma,
            dma((ncomp,)), dma((ncomp,)),
        ],
        compiler_params=pltpu.CompilerParams(
            collective_id=1, has_side_effects=True, vmem_limit_bytes=60 * 1024 * 1024),
    )(spectrum.reshape(groups, 2, 16, points), sea_mask.reshape(1, points), neighbours, substeps, courant,
      source_operator)
    return pl.pallas_call(
        write_kernel,
        out_shape=jax.ShapeDtypeStruct((bins, points), F32),
        in_specs=[vmem],
        out_specs=hbm,
        scratch_shapes=[dma((4,))],
        compiler_params=pltpu.CompilerParams(vmem_limit_bytes=4 * 1024 * 1024),
    )(result)


def solution(mesh):
    nlat, ncomp = mesh.shape["lat"], mesh.shape["comp"]

    def per_device(spectrum, sea_mask, neighbours, substeps, courant, source_operator):
        bins, points = spectrum.shape
        even = bins % 32 == 0 and (bins // 32 + 1) // 2 % NEAR == 0 and bins // 32 % BACK == 0
        if nlat == 2 and ncomp == 4 and points == 2 * NLON and even:
            return fast_device(ncomp, spectrum, sea_mask, neighbours, substeps, courant, source_operator)
        size = 16 if bins % 16 == 0 else 8
        chunks = bins // size
        group = 5 if chunks % 5 == 0 else 1
        share = points // ncomp
        total = bins * ncomp
        angles = (np.arange(ND, dtype=np.float32) + np.float32(0.5)) * np.float32(2.0 * math.pi / ND)
        spread = lambda v: jnp.asarray(
            np.broadcast_to(np.abs(v).astype(np.float32)[:, None], (ND, NLON)).reshape(ND // 8, 8, NLON))
        vmem = pl.BlockSpec(memory_space=pltpu.VMEM)
        smem = pl.BlockSpec(memory_space=pltpu.SMEM)
        kinds = 3 if nlat == 2 else 4
        return pl.pallas_call(
            functools.partial(kernel, nlat, ncomp, group),
            out_shape=jax.ShapeDtypeStruct((bins, points), F32),
            in_specs=[vmem, vmem, vmem, smem, smem, vmem, vmem, pl.BlockSpec(memory_space=pl.ANY)],
            out_specs=vmem,
            scratch_shapes=[
                pltpu.VMEM((total, total), BF16),
                pltpu.VMEM((chunks + 2, size, points), BF16),
                pltpu.VMEM((3, chunks + 2, size, points), BF16),
                pltpu.VMEM((2, SLOTS, 4, 8, NLON), F32),
                pltpu.VMEM((chunks, size, points), F32),
                pltpu.VMEM((ncomp, chunks, size, share), BF16),
                pltpu.VMEM((ncomp, chunks, size, share), BF16),
                pltpu.VMEM((total, share), F32),
                pltpu.VMEM((total, share), F32),
                pltpu.VMEM((2, total, share), BF16),
                pltpu.VMEM((ncomp, bins, share), BF16),
                pltpu.VMEM((ncomp, bins, share), BF16),
                pltpu.SemaphoreType.DMA((kinds, chunks + 2)),
                pltpu.SemaphoreType.DMA((kinds, chunks + 2)),
                pltpu.SemaphoreType.DMA,
                pltpu.SemaphoreType.DMA,
                pltpu.SemaphoreType.DMA,
                pltpu.SemaphoreType.DMA((ncomp,)),
                pltpu.SemaphoreType.DMA((ncomp,)),
                pltpu.SemaphoreType.DMA((ncomp,)),
                pltpu.SemaphoreType.DMA((ncomp,)),
            ],
            compiler_params=pltpu.CompilerParams(
                collective_id=0, has_side_effects=True, vmem_limit_bytes=56 * 1024 * 1024),
        )(spectrum, sea_mask.reshape(1, points), neighbours, substeps, courant,
          spread(np.cos(angles)), spread(np.sin(angles)), source_operator)

    placed = (
        P("comp", ("members", "lat", "sub")),
        P(("members", "lat", "sub")),
        P(None, ("members", "lat", "sub")),
        P(),
        P(),
        P("sub", None),
    )
    return jax.shard_map(
        per_device,
        mesh=mesh,
        in_specs=placed,
        out_specs=P("comp", ("members", "lat", "sub")),
        check_vma=False,
    )
```

```python
import functools
import math

import jax
import jax.numpy as jnp
import numpy as np
from jax import lax
from jax.experimental import pallas as pl
from jax.experimental.pallas import tpu as pltpu
from jax.sharding import PartitionSpec as P

NF = 30
ND = 64
NLON = 256
MAXSTEPS = 6
SRC_STEPS = 4
STEP_SIZE = 0.1
MESH = pl.DeviceIdType.MESH
HALF = ND // 2
TILES = 4
SLOTS = 8
NEAR = 4
FAR = 2
BACK = 5
F32 = jnp.float32
BF16 = jnp.bfloat16


def kernel(
    nlat, ncomp, group, spec_ref, mask_ref, nb_ref, steps_ref, cour_ref, cos_ref, sin_ref, op_ref,
    out_ref, w_ref, own_ref, halo_ref, code_ref, prop_ref, away_ref, got_ref, start_ref, state_ref,
    low_ref, inc_ref, home_ref,
    h_send, h_recv, w_send, w_recv, w_local, a_send, a_recv, b_send, b_recv,
):
    lat = lax.axis_index("lat")
    sub = lax.axis_index("sub")
    me = lax.axis_index("comp")
    bins, points = spec_ref.shape
    chunks, size = prop_ref.shape[0], prop_ref.shape[1]
    planes = size // 8
    share = points // ncomp
    total = bins * ncomp
    half_rows = total // 2
    first = me * bins
    last_lat = nlat - 1
    partner = {"sub": 1 - sub}

    barrier = pltpu.get_barrier_semaphore()
    peers = [partner]
    if nlat == 2:
        peers.append({"lat": 1 - lat})
    else:
        for move in (1, -1):
            peers.append({"lat": lax.rem(lat + move + nlat, nlat)})
            peers.append({"lat": lax.rem(lat + 2 * move + nlat, nlat), "sub": 1 - sub})
    for j in range(1, ncomp):
        peers.append({"comp": lax.rem(me + j, ncomp)})
    for peer in peers:
        pl.semaphore_signal(barrier, inc=1, device_id=peer, device_id_type=MESH)

    own_half = pl.ds(pl.multiple_of(sub * half_rows, 16), half_rows)
    load_w = pltpu.make_async_copy(op_ref, w_ref.at[own_half], w_local)
    load_w.start()

    lane = lax.broadcasted_iota(jnp.int32, (1, points), 1)
    column = lane & (NLON - 1)
    position = (lat * 2 + sub) * points + lane
    sea = mask_ref[...].astype(F32)
    west = (column - nb_ref[0:1, :]) & (NLON - 1)
    east = (nb_ref[1:2, :] - column) & (NLON - 1)

    def vertical(index_row):
        moved = ((index_row - column + 1) & (NLON - 1)) - 1
        return jnp.where(index_row == position, 2, moved)

    rows = lax.broadcasted_iota(jnp.int32, (size, points), 0)
    codes = jnp.zeros((size, points), F32)
    entries = [west, east, vertical(nb_ref[2:3, :]), vertical(nb_ref[3:4, :])]
    for k, entry in enumerate([e.astype(F32) for e in entries] + [sea]):
        codes = jnp.where(rows == k, jnp.broadcast_to(entry, (size, points)), codes)
    own_ref[0] = codes.astype(BF16)
    own_ref[1] = codes.astype(BF16)

    pl.semaphore_wait(barrier, len(peers))

    def kind(q):
        return lax.rem(lax.div(first + (q - 2) * size, HALF), 2)

    def has_from(ty, far):
        return jnp.where(ty == 0, lat >= far, lat <= last_lat - far)

    def has_to(ty, far):
        return jnp.where(ty == 0, lat <= last_lat - far, lat >= far)

    def pair_copy(q):
        return pltpu.make_async_remote_copy(
            src_ref=own_ref.at[q], dst_ref=halo_ref.at[0, q], send_sem=h_send.at[0, q],
            recv_sem=h_recv.at[0, q], device_id=partner, device_id_type=MESH)

    def side_copy(q, ty):
        to = jnp.clip(lat + 1 - 2 * ty, 0, last_lat)
        return pltpu.make_async_remote_copy(
            src_ref=own_ref.at[q], dst_ref=halo_ref.at[1, q], send_sem=h_send.at[1, q],
            recv_sem=h_recv.at[1, q], device_id={"lat": to}, device_id_type=MESH)

    def hand_copy(q, ty):
        slot = jnp.where(sub == ty, 2, 0)
        return pltpu.make_async_remote_copy(
            src_ref=halo_ref.at[1, q], dst_ref=halo_ref.at[slot, q], send_sem=h_send.at[2, q],
            recv_sem=h_recv.at[2, q], device_id=partner, device_id_type=MESH)

    def far_copy(q, ty):
        to = jnp.clip(lat + 2 - 4 * ty, 0, last_lat)
        return pltpu.make_async_remote_copy(
            src_ref=own_ref.at[q], dst_ref=halo_ref.at[2, q], send_sem=h_send.at[3, q],
            recv_sem=h_recv.at[3, q], device_id={"lat": to, "sub": 1 - sub}, device_id_type=MESH)

    def send_own(q, ty):
        @pl.when(has_to(ty, 1))
        def _():
            side_copy(q, ty).start()

        @pl.when(sub == ty)
        def _():
            pair_copy(q).start()

        if nlat > 2:
            @pl.when((sub != ty) & has_to(ty, 2))
            def _():
                far_copy(q, ty).start()

    def hand_on(q, ty):
        @pl.when(has_from(ty, 1))
        def _():
            side_copy(q, ty).wait_recv()
            hand_copy(q, ty).start()

    def arrive(q, ty):
        @pl.when(has_from(ty, 1))
        def _():
            hand_copy(q, ty).wait_recv()

        @pl.when(sub != ty)
        def _():
            pair_copy(q).wait_recv()

        if nlat > 2:
            @pl.when((sub == ty) & has_from(ty, 2))
            def _():
                far_copy(q, ty).wait_recv()

    def sent(q, ty):
        @pl.when(has_to(ty, 1))
        def _():
            side_copy(q, ty).wait_send()

        @pl.when(sub == ty)
        def _():
            pair_copy(q).wait_send()

        if nlat > 2:
            @pl.when((sub != ty) & has_to(ty, 2))
            def _():
                far_copy(q, ty).wait_send()

        @pl.when(has_from(ty, 1))
        def _():
            hand_copy(q, ty).wait_send()

    send_own(0, 0)
    send_own(1, 1)

    def prepare(i, carry):
        chunk = sea * spec_ref[pl.ds(pl.multiple_of(i * size, size), size), :]
        own_ref[i + 2] = chunk.astype(BF16)
        send_own(i + 2, kind(i + 2))
        return carry

    lax.fori_loop(0, chunks, prepare, 0)

    give_w = pltpu.make_async_remote_copy(
        src_ref=op_ref, dst_ref=w_ref.at[own_half], send_sem=w_send, recv_sem=w_recv,
        device_id=partner, device_id_type=MESH)
    give_w.start()

    for q in (0, 1):
        hand_on(q, q)
    ahead = min(6, chunks)
    for q in range(2, 2 + ahead):
        hand_on(q, kind(q))

    for ty in (0, 1):
        arrive(ty, ty)
        for slot in range(SLOTS):
            row = slot % 2 if ty == 0 else 1 - slot % 2
            cols = slice(row * NLON, (row + 1) * NLON)
            if slot < 6:
                part = halo_ref[2 - slot // 2, ty, :, cols].astype(F32)
            else:
                part = own_ref[ty, :, cols].astype(F32)
            for k, source in enumerate((0, 1, 2 + ty, 4)):
                code_ref[ty, slot, k] = jnp.broadcast_to(part[source:source + 1, :], (8, NLON))

    def propagate(i):
        q = i + 2
        ty = kind(q)

        @pl.when(i + ahead < chunks)
        def _():
            hand_on(q + ahead, kind(q + ahead))

        arrive(q, ty)
        bin0 = first + i * size
        freq = lax.div(bin0, ND)
        direction = lax.rem(bin0, ND)
        to_east = jnp.where((direction < ND // 4) | (direction >= 3 * ND // 4), 1, 0)
        steps = steps_ref[freq]
        speed = cour_ref[freq]
        sign = jnp.where(to_east == 1, 1.0, -1.0)
        shift1 = jnp.where(to_east == 1, 1, NLON - 1)
        shift2 = jnp.where(to_east == 1, 2, NLON - 2)
        back1 = NLON - shift1
        d8 = lax.div(direction, 8)
        abs_cos = cos_ref[pl.ds(d8, planes)]
        abs_sin = sin_ref[pl.ds(d8, planes)]

        def lanes(slot):
            row = jnp.where(ty == 0, slot % 2, 1 - slot % 2)
            return pl.ds(pl.multiple_of(row * NLON, NLON), NLON)

        values = []
        for slot in range(SLOTS):
            if slot < 6:
                part = halo_ref[2 - slot // 2, q, :, lanes(slot)].astype(F32)
            else:
                part = spec_ref[pl.ds(pl.multiple_of(i * size, size), size), lanes(slot)]
            part = part.reshape(planes, 8, NLON)
            if slot >= 6:
                part = part * code_ref[ty, slot, 3][None]
            values.append(part)
        for t in range(MAXSTEPS):
            live = jnp.where(t < steps, speed, 0.0)
            wx = live * abs_cos
            wy = live * abs_sin
            keep = 1.0 - wx - wy
            fresh = list(values)
            for slot in range(t + 1, SLOTS):
                x = values[slot]
                below = values[slot - 1]
                near = code_ref[ty, slot, 1 - to_east][None] == 1.0
                vert = code_ref[ty, slot, 2][None] * sign
                lon = jnp.where(near, pltpu.roll(x, shift1, 2), pltpu.roll(x, shift2, 2))
                up = jnp.where(vert == -1.0, pltpu.roll(below, shift1, 2),
                               jnp.where(vert == 1.0, pltpu.roll(below, back1, 2), below))
                up = jnp.where(jnp.abs(vert) == 2.0, x, up)
                fresh[slot] = code_ref[ty, slot, 3][None] * (keep * x + wx * lon + wy * up)
            values = fresh
        for slot in (6, 7):
            prop_ref[i, :, lanes(slot)] = values[slot].reshape(size, NLON)
        whole = prop_ref[i]
        for c in range(ncomp):
            away_ref[c, i] = whole[:, c * share:(c + 1) * share].astype(BF16)

    groups = chunks // group

    def out_copy(j, g):
        to = lax.rem(me + j, ncomp)
        span = pl.ds(g * group, group)
        return pltpu.make_async_remote_copy(
            src_ref=away_ref.at[to, span], dst_ref=got_ref.at[me, span],
            send_sem=a_send.at[j], recv_sem=a_recv.at[j],
            device_id={"comp": to}, device_id_type=MESH)

    def whole_copy(j):
        to = lax.rem(me + j, ncomp)
        return pltpu.make_async_remote_copy(
            src_ref=away_ref.at[to], dst_ref=got_ref.at[me],
            send_sem=a_send.at[j], recv_sem=a_recv.at[j],
            device_id={"comp": to}, device_id_type=MESH)

    def run_group(g, carry):
        def one(i, inner):
            propagate(g * group + i)
            return inner

        lax.fori_loop(0, group, one, 0)
        for j in range(1, ncomp):
            out_copy(j, g).start()
        return carry

    lax.fori_loop(0, groups, run_group, 0)

    for q in (0, 1):
        sent(q, q)

    def drain(q, carry):
        sent(q, kind(q))
        return carry

    lax.fori_loop(2, chunks + 2, drain, 0)
    got_ref[me] = away_ref[me]
    load_w.wait()
    give_w.wait()

    for j in range(1, ncomp):
        whole_copy(j).wait()
    for c in range(ncomp):
        start_ref[c * bins:(c + 1) * bins, :] = got_ref[c].astype(F32).reshape(bins, share)
    tile = total // TILES
    per_tile = bins // tile if bins >= tile else tile // bins
    for m in range(TILES):
        span = slice(m * tile, (m + 1) * tile)
        low_ref[0, span, :] = start_ref[span, :].astype(BF16)

    def tile_rows(m):
        return pl.ds(pl.multiple_of(m * tile, 16), tile)

    def advance(step, m):
        span = tile_rows(m)
        driving = jnp.dot(w_ref[span, :], low_ref[step % 2], preferred_element_type=F32)
        now = start_ref[span, :] if step == 0 else state_ref[span, :]
        return span, now + STEP_SIZE * now * driving

    for step in range(SRC_STEPS - 1):
        def one_tile(m, carry, step=step):
            span, now = advance(step, m)
            state_ref[span, :] = now
            low_ref[(step + 1) % 2, span, :] = now.astype(BF16)
            return carry

        lax.fori_loop(0, TILES, one_tile, 0)

    def home_copy(j, to):
        return pltpu.make_async_remote_copy(
            src_ref=inc_ref.at[to], dst_ref=home_ref.at[me],
            send_sem=b_send.at[j], recv_sem=b_recv.at[j],
            device_id={"comp": to}, device_id_type=MESH)

    mine = lax.div(me * TILES, ncomp)

    def last_tile(i, carry):
        m = lax.rem(mine + 1 + i, TILES)
        span, now = advance(SRC_STEPS - 1, m)
        gain = now - start_ref[span, :]
        for k in range(per_tile):
            to = m * per_tile + k
            inc_ref[to] = gain[k * bins:(k + 1) * bins, :].astype(BF16)
            j = lax.rem(to - me + ncomp, ncomp)

            @pl.when(to != me)
            def _():
                home_copy(j, to).start()

        return carry

    lax.fori_loop(0, TILES, last_tile, 0)
    home_ref[me] = inc_ref[me]
    for c in range(ncomp):
        j = lax.rem(me - c + ncomp, ncomp)

        @pl.when(me != c)
        def _():
            home_copy(j, lax.rem(me + j, ncomp)).wait()

        cols = slice(c * share, (c + 1) * share)
        before = prop_ref[:, :, cols].reshape(bins, share)
        out_ref[:, cols] = sea[:, cols] * (before + home_ref[c].astype(F32))


def fast_kernel(
    ncomp, spec_ref, mask_hbm, nb_hbm, steps_hbm, cour_hbm, op_ref,
    out_ref, mask_ref, nb_ref, steps_ref, cour_ref, w_ref, full_ref, oth_ref, hsend_ref, halo_ref, code_ref, ang_ref, perm_ref,
    pout_ref, pin_ref, away_ref, x_ref, start_ref, state_ref, inc_ref, home_ref,
    l_sem, i_sem, w_sem, c_send, c_recv, r_send, r_recv, g_send, g_recv, h_send, h_recv,
    a_send, a_recv, o_sem, p_send, p_recv, b_send, b_recv,
):
    lat = lax.axis_index("lat")
    sub = lax.axis_index("sub")
    me = lax.axis_index("comp")
    groups = spec_ref.shape[0]
    bins = groups * 2 * 16
    kmax = halo_ref.shape[0]
    lanes = NLON // 2
    total = bins * ncomp
    partner = {"sub": 1 - sub}
    others = [partner, {"lat": 1 - lat}, {"lat": 1 - lat, "sub": 1 - sub}]

    small = [pltpu.make_async_copy(src, dst, i_sem.at[n]) for n, (src, dst) in enumerate((
        (mask_hbm, mask_ref.at[lat, sub]), (nb_hbm, nb_ref.at[lat, sub]),
        (steps_hbm, steps_ref), (cour_hbm, cour_ref)))]
    loads = []
    for r in range(2):
        cols = slice(r * NLON, (r + 1) * NLON)
        loads.append(pltpu.make_async_copy(
            spec_ref.at[:, 1 - sub, :, cols], oth_ref.at[pl.ds(0, groups), r], l_sem.at[r]))
        loads.append(pltpu.make_async_copy(
            spec_ref.at[:, sub, :, cols], full_ref.at[pl.ds(0, groups), 2 * sub + r], l_sem.at[2 + r]))
    for load in (small[0], *loads, *small[1:]):
        load.start()
    own_half = pl.ds(pl.multiple_of(sub * (total // 2), 16), total // 2)
    load_w = pltpu.make_async_copy(op_ref, w_ref.at[own_half], w_sem)

    barrier = pltpu.get_barrier_semaphore()
    peers = list(others)
    for d in range(1, ncomp):
        z = lax.rem(me + d, ncomp)
        peers += [{"comp": z}, {"comp": z, "sub": 1 - sub}]
    for peer in peers:
        pl.semaphore_signal(barrier, inc=1, device_id=peer, device_id_type=MESH)

    a = lax.broadcasted_iota(jnp.int32, (NLON, NLON), 0)
    b = lax.broadcasted_iota(jnp.int32, (NLON, NLON), 1)
    split = lambda c: jnp.where(c < lanes, 2 * c, 2 * (c - lanes) + 1)
    perm_ref[0] = (a == split(b)).astype(F32).astype(BF16)
    perm_ref[1] = (b == split(a)).astype(F32).astype(BF16)

    near_ty = lat
    far_ty = 1 - lat
    n0 = lax.rem(lat + me * groups, 2)
    f0 = 1 - n0
    for q, ty in enumerate((near_ty, far_ty)):
        d = lax.broadcasted_iota(jnp.int32, (16, lanes), 0) + 16 * (2 * ty + sub)
        angle = (d.astype(F32) + 0.5) * np.float32(2.0 * math.pi / ND)
        ang_ref[q, 0] = jnp.abs(jnp.cos(angle))
        ang_ref[q, 1] = jnp.abs(jnp.sin(angle))

    def point_copies(n):
        return [pltpu.make_async_remote_copy(
            src_ref=ref.at[lat, sub], dst_ref=ref.at[lat, sub], send_sem=c_send.at[n, m],
            recv_sem=c_recv.at[n, m], device_id=others[n], device_id_type=MESH)
            for m, ref in enumerate((mask_ref, nb_ref))]

    def raw_copies():
        return [pltpu.make_async_remote_copy(
            src_ref=spec_ref.at[:, 1 - sub, :, r * NLON:(r + 1) * NLON],
            dst_ref=full_ref.at[pl.ds(0, groups), 2 * sub + r],
            send_sem=r_send.at[r], recv_sem=r_recv.at[r], device_id=partner, device_id_type=MESH)
            for r in range(2)]

    def raw_waits():
        for r in range(2):
            pltpu.make_async_remote_copy(
                src_ref=spec_ref.at[:, 1 - sub, :, r * NLON:(r + 1) * NLON],
                dst_ref=full_ref.at[pl.ds(0, groups), 2 * (1 - sub) + r],
                send_sem=r_send.at[r], recv_sem=r_recv.at[r],
                device_id=partner, device_id_type=MESH).wait_recv()

    small[0].wait()
    small[1].wait()
    sea = mask_ref[lat, sub].astype(F32)
    for load in loads:
        load.wait()
    sea_rows = [jnp.broadcast_to(sea[:, r * NLON:(r + 1) * NLON], (16, NLON)) for r in range(2)]

    def convert(k, carry):
        j = n0 + 2 * k
        for r in range(2):
            mine = full_ref[j, 2 * sub + r] * sea_rows[r]
            other = oth_ref[j, r] * sea_rows[r]
            hsend_ref[k, sub, r] = mine.astype(BF16)
            hsend_ref[k, 1 - sub, r] = other.astype(BF16)
        return carry

    lax.fori_loop(0, kmax, convert, 0)
    pl.semaphore_wait(barrier, len(peers))
    def halo_copy(k, p):
        return pltpu.make_async_remote_copy(
            src_ref=hsend_ref.at[k, p], dst_ref=halo_ref.at[k, pl.ds(2 * sub, 2)],
            send_sem=h_send.at[k, p], recv_sem=h_recv.at[k, sub],
            device_id={"lat": 1 - lat, "sub": p}, device_id_type=MESH)

    def halo_wait(k, s):
        pltpu.make_async_remote_copy(
            src_ref=hsend_ref.at[k, s], dst_ref=halo_ref.at[k, pl.ds(2 * s, 2)],
            send_sem=h_send.at[k, s], recv_sem=h_recv.at[k, s],
            device_id={"lat": 1 - lat, "sub": s}, device_id_type=MESH).wait_recv()

    def give_w():
        return pltpu.make_async_remote_copy(
            src_ref=op_ref, dst_ref=w_ref.at[own_half], send_sem=g_send, recv_sem=g_recv,
            device_id=partner, device_id_type=MESH)

    def take_w():
        other_half = pl.ds(pl.multiple_of((1 - sub) * (total // 2), 16), total // 2)
        return pltpu.make_async_remote_copy(
            src_ref=op_ref, dst_ref=w_ref.at[other_half], send_sem=g_send, recv_sem=g_recv,
            device_id=partner, device_id_type=MESH)

    def send_halo(k, carry):
        @pl.when(n0 + 2 * k < groups)
        def _():
            for p in range(2):
                halo_copy(k, p).start()
        return carry

    for copy in point_copies(0):
        copy.start()
    lax.fori_loop(0, FAR, send_halo, 0)
    for copy in (*raw_copies(), *point_copies(1), *point_copies(2)):
        copy.start()
    lax.fori_loop(FAR, kmax, send_halo, 0)
    load_w.start()
    give_w().start()
    for load in small[2:]:
        load.wait()

    points = mask_ref.shape[-1]
    lane = lax.broadcasted_iota(jnp.int32, (1, points), 1)
    column = lane & (NLON - 1)
    index = lax.broadcasted_iota(jnp.int32, (8, points), 0)

    def decode(chip):
        for s in range(2):
            nb = nb_ref[chip, s]
            west = (column - nb[0:1, :]) & (NLON - 1)
            east = (nb[1:2, :] - column) & (NLON - 1)
            moves = [((nb[k:k + 1, :] - column + 1) & (NLON - 1)) - 1 for k in (2, 3)]
            codes = jnp.zeros((8, points), F32)
            for k, entry in enumerate((west, east, *moves, mask_ref[chip, s])):
                codes = jnp.where(index == k, jnp.broadcast_to(entry.astype(F32), (8, points)), codes)
            for r in range(2):
                part = codes[:, r * NLON:(r + 1) * NLON].astype(BF16)
                both = jnp.dot(part, perm_ref[0], preferred_element_type=F32)
                for k in range(5):
                    code_ref[chip, 2 * s + r, k] = jnp.broadcast_to(both[k:k + 1, :], (8, NLON))

    side = lax.div(me, 2)

    def target(i):
        near = me + 1 - 2 * lax.rem(me, 2)
        return jnp.where(i == 0, 3 - 3 * side, jnp.where(i == 1, 2 - side, jnp.where(i == 2, near, me)))

    def chunk_copy(h, j, i):
        to = target(i)
        return pltpu.make_async_remote_copy(
            src_ref=away_ref.at[h, to, j], dst_ref=x_ref.at[0, me * groups + j, sub],
            send_sem=a_send.at[h, i], recv_sem=a_recv.at[me, sub],
            device_id={"comp": to, "sub": h}, device_id_type=MESH)

    def whole_copy(h, i):
        to = target(i)
        return pltpu.make_async_remote_copy(
            src_ref=away_ref.at[h, to, pl.ds(0, groups)],
            dst_ref=x_ref.at[0, pl.ds(me * groups, groups), sub],
            send_sem=a_send.at[h, i], recv_sem=a_recv.at[me, sub],
            device_id={"comp": to, "sub": h}, device_id_type=MESH)

    def whole_wait(z, s):
        pltpu.make_async_remote_copy(
            src_ref=away_ref.at[0, z, pl.ds(0, groups)],
            dst_ref=x_ref.at[0, pl.ds(z * groups, groups), s],
            send_sem=a_send.at[0, 0], recv_sem=a_recv.at[z, s],
            device_id={"comp": z, "sub": s}, device_id_type=MESH).wait_recv()

    def pick(ty, i):
        return ty * 3 + (1 - 2 * ty) * i

    def separate(x):
        high = x.astype(BF16)
        low = (x - high.astype(F32)).astype(BF16)
        return high, low

    def propagate(ks, far, to_east):
        ty = far_ty if far else near_ty
        js = [(f0 if far else n0) + 2 * k for k in ks]
        vert = 2 + ty
        lowest = 0 if far else 4

        def code(q, k, half):
            chip = lat if q >= 4 else 1 - lat
            part = code_ref[chip, pick(ty, q % 4), k, :, half * lanes:(half + 1) * lanes]
            return jnp.concatenate([part, part], axis=0)

        raw = jnp.concatenate([full_ref[j, pick(ty, i)] for j in js for i in range(4)], axis=0)
        high, low = separate(raw)
        mixed = (jnp.dot(high, perm_ref[0], preferred_element_type=F32)
                 + jnp.dot(low, perm_ref[0], preferred_element_type=F32))
        if far:
            edge = jnp.concatenate([halo_ref[k, pick(ty, i)] for k in ks for i in range(4)], axis=0)
            edge = jnp.dot(edge, perm_ref[0], preferred_element_type=F32)
        cells = []
        weights = []
        for n, j in enumerate(js):
            values = [None] * 8
            for i in range(4):
                rows = slice((n * 4 + i) * 16, (n * 4 + i + 1) * 16)
                values[4 + i] = tuple(
                    mixed[rows, half * lanes:(half + 1) * lanes] * code(4 + i, 4, half)
                    for half in range(2))
                if far:
                    values[i] = tuple(edge[rows, half * lanes:(half + 1) * lanes] for half in range(2))
            cells.append(values)
            freq = jnp.minimum(lax.div(me * bins + j * 32, ND), steps_ref.shape[0] - 1)
            weights.append((steps_ref[freq], cour_ref[freq]))
        abs_cos, abs_sin = ang_ref[int(far), 0], ang_ref[int(far), 1]
        ahead, behind = (1, lanes - 1)
        for t in range(MAXSTEPS):
            slots = [q for q in range(7, lowest - 1, -1) if q >= 4 or t <= q + 1]
            for n, (steps, speed) in enumerate(weights):
                live = jnp.where(t < steps, speed, 0.0)
                wx = live * abs_cos
                wy = live * abs_sin
                keep = 1.0 - wx - wy
                values = cells[n]
                fresh = list(values)
                turned = {}

                def turn(q, half, shift):
                    key = (q, half, shift)
                    if key not in turned:
                        turned[key] = pltpu.roll(values[q][half], shift, 1)
                    return turned[key]

                def left(q):
                    return turn(q, 1, ahead), values[q][0]

                def right(q):
                    return values[q][1], turn(q, 0, behind)

                for q in slots:
                    shift = ahead if to_east else behind
                    one = left(q) if to_east else right(q)
                    lon_code = 0 if to_east else 1
                    new = []
                    for half in range(2):
                        x = values[q][half]
                        lon = jnp.where(code(q, lon_code, half) == 1.0, one[half], turn(q, half, shift))
                        if q == lowest:
                            up = x
                        else:
                            move = code(q, vert, half)
                            up = jnp.where(move == -1.0, left(q - 1)[half],
                                           jnp.where(move == 1.0, right(q - 1)[half], values[q - 1][half]))
                        new.append(code(q, 4, half) * (keep * x + wx * lon + wy * up))
                    fresh[q] = tuple(new)
                cells[n] = fresh
        for n, j in enumerate(js):
            for i in range(4):
                r = pick(ty, i)
                for half in range(2):
                    value = cells[n][4 + i][half]
                    pout_ref[j, r, :, half * lanes:(half + 1) * lanes] = value
                    away_ref[lax.div(r, 2), 2 * lax.rem(r, 2) + half, j] = value.astype(BF16)
        for n, j in enumerate(js):
            @pl.when(j < groups)
            def _():
                for i in range(ncomp - 1):
                    chunk_copy(0, j, i).start()

    straight = sub == lat
    for copy in point_copies(0):
        copy.wait_recv()
    decode(lat)
    raw_waits()

    def near_body(g, carry):
        ks = [g * NEAR + n for n in range(NEAR)]

        @pl.when(straight)
        def _():
            propagate(ks, False, True)

        @pl.when(jnp.logical_not(straight))
        def _():
            propagate(ks, False, False)
        return carry

    lax.fori_loop(0, kmax // NEAR, near_body, 0)
    for n in (1, 2):
        for copy in point_copies(n):
            copy.wait_recv()
    decode(1 - lat)

    def far_body(g, carry):
        ks = [g * FAR + n for n in range(FAR)]
        for k in ks:
            @pl.when(f0 + 2 * k < groups)
            def _():
                for s in range(2):
                    halo_wait(k, s)

        @pl.when(straight)
        def _():
            propagate(ks, True, False)

        @pl.when(jnp.logical_not(straight))
        def _():
            propagate(ks, True, True)

        for k in ks:
            @pl.when(n0 + 2 * k < groups)
            def _():
                for i in range(ncomp - 1):
                    chunk_copy(1, n0 + 2 * k, i).start()
        return carry

    lax.fori_loop(0, kmax // FAR, far_body, 0)

    own_copy = pltpu.make_async_copy(
        away_ref.at[sub, me, pl.ds(0, groups)], x_ref.at[0, pl.ds(me * groups, groups), sub], o_sem)

    def cross_copy():
        return pltpu.make_async_remote_copy(
            src_ref=away_ref.at[1 - sub, me, pl.ds(0, groups)],
            dst_ref=x_ref.at[0, pl.ds(me * groups, groups), sub],
            send_sem=a_send.at[0, ncomp - 1], recv_sem=a_recv.at[me, sub],
            device_id=partner, device_id_type=MESH)

    def prop_copy():
        return pltpu.make_async_remote_copy(
            src_ref=pout_ref.at[pl.ds(0, groups), pl.ds(2 * (1 - sub), 2)],
            dst_ref=pin_ref, send_sem=p_send, recv_sem=p_recv,
            device_id=partner, device_id_type=MESH)

    own_copy.start()
    cross_copy().start()

    def send_rest(k, carry):
        @pl.when(f0 + 2 * k < groups)
        def _():
            for i in range(ncomp - 1):
                chunk_copy(1, f0 + 2 * k, i).start()
        return carry

    lax.fori_loop(0, kmax, send_rest, 0)
    prop_copy().start()

    def home_copy(m):
        return pltpu.make_async_remote_copy(
            src_ref=inc_ref.at[m], dst_ref=home_ref.at[me],
            send_sem=b_send.at[m], recv_sem=b_recv.at[me],
            device_id={"comp": m}, device_id_type=MESH)

    early = (2 * bins) // 128 * 128
    late = total - early

    once = 1 + lax.div(me, ncomp)

    def partial(start, span, use):
        def one(i, carry):
            rows = pl.ds(pl.multiple_of(i * total, 16), total)
            field = x_ref[0, pl.ds(lax.div(start, 32), span // 32)].reshape(span, lanes)
            cols = pl.ds(pl.multiple_of(start, 128), span)
            use(rows, jnp.dot(w_ref[rows, cols], field, preferred_element_type=F32))
            return carry

        lax.fori_loop(0, once, one, 0)

    def begin():
        def use(rows, driving):
            state_ref[rows, :] = driving

        partial(side * late, early, use)

    def first_step():
        def use(rows, driving):
            start = x_ref[0].reshape(total, lanes).astype(F32)
            now = start + STEP_SIZE * start * (state_ref[rows, :] + driving)
            start_ref[rows, :] = start
            state_ref[rows, :] = now
            x_ref[1] = now.astype(BF16).reshape(ncomp * groups, 2, 16, lanes)

        partial((1 - side) * early, late, use)

    def advance(step, carry):
        field = x_ref[lax.rem(step, 2)].reshape(total, lanes)
        driving = jnp.dot(w_ref[...], field, preferred_element_type=F32)
        now = state_ref[...]
        now = now + STEP_SIZE * now * driving
        state_ref[...] = now
        x_ref[lax.rem(step + 1, 2)] = now.astype(BF16).reshape(ncomp * groups, 2, 16, lanes)
        return carry

    def finish():
        def one(i, carry):
            m = target(i)
            rows = pl.ds(pl.multiple_of(m * bins, 16), bins)
            field = x_ref[(SRC_STEPS - 1) % 2].reshape(total, lanes)
            driving = jnp.dot(w_ref[rows, :], field, preferred_element_type=F32)
            now = state_ref[rows, :]
            now = now + STEP_SIZE * now * driving
            inc_ref[m] = (now - start_ref[rows, :]).astype(BF16)

            @pl.when(m != me)
            def _():
                home_copy(m).start()
            return carry

        lax.fori_loop(0, ncomp, one, 0)

    sea_wide = [jnp.broadcast_to(sea[:, r * NLON:(r + 1) * NLON], (16, NLON)) for r in range(2)]

    def restore(g, carry):
        js = [g * BACK + n for n in range(BACK)]
        parts = [ref for j in js for ref in (
            pout_ref[j, 2 * sub], pout_ref[j, 2 * sub + 1], pin_ref[j, 0], pin_ref[j, 1])]
        high, low = separate(jnp.concatenate(parts, axis=0))
        plain = (jnp.dot(high, perm_ref[1], preferred_element_type=F32)
                 + jnp.dot(low, perm_ref[1], preferred_element_type=F32))
        for n in range(4 * BACK):
            p = sub if n % 4 < 2 else 1 - sub
            rows = pl.ds(pl.multiple_of((2 * js[n // 4] + p) * 16, 16), 16)
            r = n % 2
            out_ref[rows, r * NLON:(r + 1) * NLON] = sea_wide[r] * plain[n * 16:(n + 1) * 16, :]
        return carry

    def restore_all():
        prop_copy().wait_recv()
        lax.fori_loop(0, groups // BACK, restore, 0)

    pl.when(sub == 1)(restore_all)
    load_w.wait()
    take_w().wait_recv()
    own_copy.wait()
    whole_wait(me, 1 - sub)
    for s in range(2):
        whole_wait(target(2), s)
    begin()
    for i in (1, 0):
        for s in range(2):
            whole_wait(target(i), s)
    first_step()
    lax.fori_loop(1, SRC_STEPS - 1, advance, 0)
    finish()

    pl.when(sub == 0)(restore_all)
    for i in (3, 2, 1, 0):
        z = target(i)

        def land():
            pltpu.make_async_remote_copy(
                src_ref=inc_ref.at[z], dst_ref=home_ref.at[z],
                send_sem=b_send.at[z], recv_sem=b_recv.at[z],
                device_id={"comp": z}, device_id_type=MESH).wait_recv()

        if i < 3:
            land()
        r = lax.div(z, 2)
        half = lax.rem(z, 2)
        cols = pl.ds(pl.multiple_of(r * NLON, NLON), NLON)
        spread = perm_ref[1, pl.ds(pl.multiple_of(half * lanes, lanes), lanes), :]
        sea_row = jnp.where(r == 0, sea_wide[0][0:8], sea_wide[1][0:8])
        arrived = inc_ref[z] if i == 3 else home_ref[z]
        back = jnp.dot(arrived, spread, preferred_element_type=F32)
        back = back.reshape(bins // 8, 8, NLON) * sea_row[None]
        out_ref[:, cols] = out_ref[:, cols] + back.reshape(bins, NLON)

    for n in range(3):
        for copy in point_copies(n):
            copy.wait_send()
    for copy in raw_copies():
        copy.wait_send()

    def halo_left(k, carry):
        @pl.when(n0 + 2 * k < groups)
        def _():
            for p in range(2):
                halo_copy(k, p).wait_send()
        return carry

    lax.fori_loop(0, kmax, halo_left, 0)
    prop_copy().wait_send()
    cross_copy().wait_send()
    give_w().wait_send()
    for i in range(ncomp - 1):
        for h in range(2):
            whole_copy(h, i).wait_send()
        home_copy(target(i)).wait_send()


def write_kernel(src_ref, dst_ref, sems):
    pieces = sems.shape[0]
    rows = src_ref.shape[0] // pieces
    copies = [pltpu.make_async_copy(
        src_ref.at[pl.ds(i * rows, rows)], dst_ref.at[pl.ds(i * rows, rows)], sems.at[i])
        for i in range(pieces)]
    for copy in copies:
        copy.start()
    for copy in copies:
        copy.wait()


def fast_device(ncomp, spectrum, sea_mask, neighbours, substeps, courant, source_operator):
    bins, points = spectrum.shape
    groups = bins // 32
    kmax = (groups + 1) // 2
    lanes = NLON // 2
    total = bins * ncomp
    vmem = pl.BlockSpec(memory_space=pltpu.VMEM)
    hbm = pl.BlockSpec(memory_space=pltpu.HBM)
    dma = pltpu.SemaphoreType.DMA
    result = pl.pallas_call(
        functools.partial(fast_kernel, ncomp),
        out_shape=pltpu.VMEM((bins, points), F32),
        in_specs=[hbm] * 6,
        out_specs=vmem,
        scratch_shapes=[
            pltpu.VMEM((2, 2, 1, points), jnp.int32),
            pltpu.VMEM((2, 2, 4, points), jnp.int32),
            pltpu.SMEM(substeps.shape, jnp.int32),
            pltpu.SMEM(courant.shape, F32),
            pltpu.VMEM((total, total), BF16),
            pltpu.VMEM((2 * kmax, 4, 16, NLON), F32),
            pltpu.VMEM((2 * kmax, 2, 16, NLON), F32),
            pltpu.VMEM((kmax, 2, 2, 16, NLON), BF16),
            pltpu.VMEM((kmax, 4, 16, NLON), BF16),
            pltpu.VMEM((2, 4, 5, 8, NLON), F32),
            pltpu.VMEM((2, 2, 16, lanes), F32),
            pltpu.VMEM((2, NLON, NLON), BF16),
            pltpu.VMEM((2 * kmax, 4, 16, NLON), F32),
            pltpu.VMEM((groups, 2, 16, NLON), F32),
            pltpu.VMEM((2, ncomp, 2 * kmax, 16, lanes), BF16),
            pltpu.VMEM((2, ncomp * groups, 2, 16, lanes), BF16),
            pltpu.VMEM((total, lanes), F32),
            pltpu.VMEM((total, lanes), F32),
            pltpu.VMEM((ncomp, bins, lanes), BF16),
            pltpu.VMEM((ncomp, bins, lanes), BF16),
            dma((4,)), dma((4,)), dma, dma((3, 2)), dma((3, 2)), dma((2,)), dma((2,)), dma, dma,
            dma((kmax, 2)), dma((kmax, 2)), dma((2, ncomp)), dma((ncomp, 2)), dma, dma, dma,
            dma((ncomp,)), dma((ncomp,)),
        ],
        compiler_params=pltpu.CompilerParams(
            collective_id=1, has_side_effects=True, vmem_limit_bytes=60 * 1024 * 1024),
    )(spectrum.reshape(groups, 2, 16, points), sea_mask.reshape(1, points), neighbours, substeps, courant,
      source_operator)
    return pl.pallas_call(
        write_kernel,
        out_shape=jax.ShapeDtypeStruct((bins, points), F32),
        in_specs=[vmem],
        out_specs=hbm,
        scratch_shapes=[dma((4,))],
        compiler_params=pltpu.CompilerParams(vmem_limit_bytes=4 * 1024 * 1024),
    )(result)


def solution(mesh):
    nlat, ncomp = mesh.shape["lat"], mesh.shape["comp"]

    def per_device(spectrum, sea_mask, neighbours, substeps, courant, source_operator):
        bins, points = spectrum.shape
        even = bins % 32 == 0 and (bins // 32 + 1) // 2 % NEAR == 0 and bins // 32 % BACK == 0
        if nlat == 2 and ncomp == 4 and points == 2 * NLON and even:
            return fast_device(ncomp, spectrum, sea_mask, neighbours, substeps, courant, source_operator)
        size = 16 if bins % 16 == 0 else 8
        chunks = bins // size
        group = 5 if chunks % 5 == 0 else 1
        share = points // ncomp
        total = bins * ncomp
        angles = (np.arange(ND, dtype=np.float32) + np.float32(0.5)) * np.float32(2.0 * math.pi / ND)
        spread = lambda v: jnp.asarray(
            np.broadcast_to(np.abs(v).astype(np.float32)[:, None], (ND, NLON)).reshape(ND // 8, 8, NLON))
        vmem = pl.BlockSpec(memory_space=pltpu.VMEM)
        smem = pl.BlockSpec(memory_space=pltpu.SMEM)
        kinds = 3 if nlat == 2 else 4
        return pl.pallas_call(
            functools.partial(kernel, nlat, ncomp, group),
            out_shape=jax.ShapeDtypeStruct((bins, points), F32),
            in_specs=[vmem, vmem, vmem, smem, smem, vmem, vmem, pl.BlockSpec(memory_space=pl.ANY)],
            out_specs=vmem,
            scratch_shapes=[
                pltpu.VMEM((total, total), BF16),
                pltpu.VMEM((chunks + 2, size, points), BF16),
                pltpu.VMEM((3, chunks + 2, size, points), BF16),
                pltpu.VMEM((2, SLOTS, 4, 8, NLON), F32),
                pltpu.VMEM((chunks, size, points), F32),
                pltpu.VMEM((ncomp, chunks, size, share), BF16),
                pltpu.VMEM((ncomp, chunks, size, share), BF16),
                pltpu.VMEM((total, share), F32),
                pltpu.VMEM((total, share), F32),
                pltpu.VMEM((2, total, share), BF16),
                pltpu.VMEM((ncomp, bins, share), BF16),
                pltpu.VMEM((ncomp, bins, share), BF16),
                pltpu.SemaphoreType.DMA((kinds, chunks + 2)),
                pltpu.SemaphoreType.DMA((kinds, chunks + 2)),
                pltpu.SemaphoreType.DMA,
                pltpu.SemaphoreType.DMA,
                pltpu.SemaphoreType.DMA,
                pltpu.SemaphoreType.DMA((ncomp,)),
                pltpu.SemaphoreType.DMA((ncomp,)),
                pltpu.SemaphoreType.DMA((ncomp,)),
                pltpu.SemaphoreType.DMA((ncomp,)),
            ],
            compiler_params=pltpu.CompilerParams(
                collective_id=0, has_side_effects=True, vmem_limit_bytes=56 * 1024 * 1024),
        )(spectrum, sea_mask.reshape(1, points), neighbours, substeps, courant,
          spread(np.cos(angles)), spread(np.sin(angles)), source_operator)

    placed = (
        P("comp", ("members", "lat", "sub")),
        P(("members", "lat", "sub")),
        P(None, ("members", "lat", "sub")),
        P(),
        P(),
        P("sub", None),
    )
    return jax.shard_map(
        per_device,
        mesh=mesh,
        in_specs=placed,
        out_specs=P("comp", ("members", "lat", "sub")),
        check_vma=False,
    )
```

```python
import functools
import math

import jax
import jax.numpy as jnp
import numpy as np
from jax import lax
from jax.experimental import pallas as pl
from jax.experimental.pallas import tpu as pltpu
from jax.sharding import PartitionSpec as P

NF = 30
ND = 64
NLON = 256
MAXSTEPS = 6
SRC_STEPS = 4
STEP_SIZE = 0.1
MESH = pl.DeviceIdType.MESH
HALF = ND // 2
TILES = 4
SLOTS = 8
NEAR = 4
FAR = 2
BACK = 5
F32 = jnp.float32
BF16 = jnp.bfloat16


def kernel(
    nlat, ncomp, group, spec_ref, mask_ref, nb_ref, steps_ref, cour_ref, cos_ref, sin_ref, op_ref,
    out_ref, w_ref, own_ref, halo_ref, code_ref, prop_ref, away_ref, got_ref, start_ref, state_ref,
    low_ref, inc_ref, home_ref,
    h_send, h_recv, w_send, w_recv, w_local, a_send, a_recv, b_send, b_recv,
):
    lat = lax.axis_index("lat")
    sub = lax.axis_index("sub")
    me = lax.axis_index("comp")
    bins, points = spec_ref.shape
    chunks, size = prop_ref.shape[0], prop_ref.shape[1]
    planes = size // 8
    share = points // ncomp
    total = bins * ncomp
    half_rows = total // 2
    first = me * bins
    last_lat = nlat - 1
    partner = {"sub": 1 - sub}

    barrier = pltpu.get_barrier_semaphore()
    peers = [partner]
    if nlat == 2:
        peers.append({"lat": 1 - lat})
    else:
        for move in (1, -1):
            peers.append({"lat": lax.rem(lat + move + nlat, nlat)})
            peers.append({"lat": lax.rem(lat + 2 * move + nlat, nlat), "sub": 1 - sub})
    for j in range(1, ncomp):
        peers.append({"comp": lax.rem(me + j, ncomp)})
    for peer in peers:
        pl.semaphore_signal(barrier, inc=1, device_id=peer, device_id_type=MESH)

    own_half = pl.ds(pl.multiple_of(sub * half_rows, 16), half_rows)
    load_w = pltpu.make_async_copy(op_ref, w_ref.at[own_half], w_local)
    load_w.start()

    lane = lax.broadcasted_iota(jnp.int32, (1, points), 1)
    column = lane & (NLON - 1)
    position = (lat * 2 + sub) * points + lane
    sea = mask_ref[...].astype(F32)
    west = (column - nb_ref[0:1, :]) & (NLON - 1)
    east = (nb_ref[1:2, :] - column) & (NLON - 1)

    def vertical(index_row):
        moved = ((index_row - column + 1) & (NLON - 1)) - 1
        return jnp.where(index_row == position, 2, moved)

    rows = lax.broadcasted_iota(jnp.int32, (size, points), 0)
    codes = jnp.zeros((size, points), F32)
    entries = [west, east, vertical(nb_ref[2:3, :]), vertical(nb_ref[3:4, :])]
    for k, entry in enumerate([e.astype(F32) for e in entries] + [sea]):
        codes = jnp.where(rows == k, jnp.broadcast_to(entry, (size, points)), codes)
    own_ref[0] = codes.astype(BF16)
    own_ref[1] = codes.astype(BF16)

    pl.semaphore_wait(barrier, len(peers))

    def kind(q):
        return lax.rem(lax.div(first + (q - 2) * size, HALF), 2)

    def has_from(ty, far):
        return jnp.where(ty == 0, lat >= far, lat <= last_lat - far)

    def has_to(ty, far):
        return jnp.where(ty == 0, lat <= last_lat - far, lat >= far)

    def pair_copy(q):
        return pltpu.make_async_remote_copy(
            src_ref=own_ref.at[q], dst_ref=halo_ref.at[0, q], send_sem=h_send.at[0, q],
            recv_sem=h_recv.at[0, q], device_id=partner, device_id_type=MESH)

    def side_copy(q, ty):
        to = jnp.clip(lat + 1 - 2 * ty, 0, last_lat)
        return pltpu.make_async_remote_copy(
            src_ref=own_ref.at[q], dst_ref=halo_ref.at[1, q], send_sem=h_send.at[1, q],
            recv_sem=h_recv.at[1, q], device_id={"lat": to}, device_id_type=MESH)

    def hand_copy(q, ty):
        slot = jnp.where(sub == ty, 2, 0)
        return pltpu.make_async_remote_copy(
            src_ref=halo_ref.at[1, q], dst_ref=halo_ref.at[slot, q], send_sem=h_send.at[2, q],
            recv_sem=h_recv.at[2, q], device_id=partner, device_id_type=MESH)

    def far_copy(q, ty):
        to = jnp.clip(lat + 2 - 4 * ty, 0, last_lat)
        return pltpu.make_async_remote_copy(
            src_ref=own_ref.at[q], dst_ref=halo_ref.at[2, q], send_sem=h_send.at[3, q],
            recv_sem=h_recv.at[3, q], device_id={"lat": to, "sub": 1 - sub}, device_id_type=MESH)

    def send_own(q, ty):
        @pl.when(has_to(ty, 1))
        def _():
            side_copy(q, ty).start()

        @pl.when(sub == ty)
        def _():
            pair_copy(q).start()

        if nlat > 2:
            @pl.when((sub != ty) & has_to(ty, 2))
            def _():
                far_copy(q, ty).start()

    def hand_on(q, ty):
        @pl.when(has_from(ty, 1))
        def _():
            side_copy(q, ty).wait_recv()
            hand_copy(q, ty).start()

    def arrive(q, ty):
        @pl.when(has_from(ty, 1))
        def _():
            hand_copy(q, ty).wait_recv()

        @pl.when(sub != ty)
        def _():
            pair_copy(q).wait_recv()

        if nlat > 2:
            @pl.when((sub == ty) & has_from(ty, 2))
            def _():
                far_copy(q, ty).wait_recv()

    def sent(q, ty):
        @pl.when(has_to(ty, 1))
        def _():
            side_copy(q, ty).wait_send()

        @pl.when(sub == ty)
        def _():
            pair_copy(q).wait_send()

        if nlat > 2:
            @pl.when((sub != ty) & has_to(ty, 2))
            def _():
                far_copy(q, ty).wait_send()

        @pl.when(has_from(ty, 1))
        def _():
            hand_copy(q, ty).wait_send()

    send_own(0, 0)
    send_own(1, 1)

    def prepare(i, carry):
        chunk = sea * spec_ref[pl.ds(pl.multiple_of(i * size, size), size), :]
        own_ref[i + 2] = chunk.astype(BF16)
        send_own(i + 2, kind(i + 2))
        return carry

    lax.fori_loop(0, chunks, prepare, 0)

    give_w = pltpu.make_async_remote_copy(
        src_ref=op_ref, dst_ref=w_ref.at[own_half], send_sem=w_send, recv_sem=w_recv,
        device_id=partner, device_id_type=MESH)
    give_w.start()

    for q in (0, 1):
        hand_on(q, q)
    ahead = min(6, chunks)
    for q in range(2, 2 + ahead):
        hand_on(q, kind(q))

    for ty in (0, 1):
        arrive(ty, ty)
        for slot in range(SLOTS):
            row = slot % 2 if ty == 0 else 1 - slot % 2
            cols = slice(row * NLON, (row + 1) * NLON)
            if slot < 6:
                part = halo_ref[2 - slot // 2, ty, :, cols].astype(F32)
            else:
                part = own_ref[ty, :, cols].astype(F32)
            for k, source in enumerate((0, 1, 2 + ty, 4)):
                code_ref[ty, slot, k] = jnp.broadcast_to(part[source:source + 1, :], (8, NLON))

    def propagate(i):
        q = i + 2
        ty = kind(q)

        @pl.when(i + ahead < chunks)
        def _():
            hand_on(q + ahead, kind(q + ahead))

        arrive(q, ty)
        bin0 = first + i * size
        freq = lax.div(bin0, ND)
        direction = lax.rem(bin0, ND)
        to_east = jnp.where((direction < ND // 4) | (direction >= 3 * ND // 4), 1, 0)
        steps = steps_ref[freq]
        speed = cour_ref[freq]
        sign = jnp.where(to_east == 1, 1.0, -1.0)
        shift1 = jnp.where(to_east == 1, 1, NLON - 1)
        shift2 = jnp.where(to_east == 1, 2, NLON - 2)
        back1 = NLON - shift1
        d8 = lax.div(direction, 8)
        abs_cos = cos_ref[pl.ds(d8, planes)]
        abs_sin = sin_ref[pl.ds(d8, planes)]

        def lanes(slot):
            row = jnp.where(ty == 0, slot % 2, 1 - slot % 2)
            return pl.ds(pl.multiple_of(row * NLON, NLON), NLON)

        values = []
        for slot in range(SLOTS):
            if slot < 6:
                part = halo_ref[2 - slot // 2, q, :, lanes(slot)].astype(F32)
            else:
                part = spec_ref[pl.ds(pl.multiple_of(i * size, size), size), lanes(slot)]
            part = part.reshape(planes, 8, NLON)
            if slot >= 6:
                part = part * code_ref[ty, slot, 3][None]
            values.append(part)
        for t in range(MAXSTEPS):
            live = jnp.where(t < steps, speed, 0.0)
            wx = live * abs_cos
            wy = live * abs_sin
            keep = 1.0 - wx - wy
            fresh = list(values)
            for slot in range(t + 1, SLOTS):
                x = values[slot]
                below = values[slot - 1]
                near = code_ref[ty, slot, 1 - to_east][None] == 1.0
                vert = code_ref[ty, slot, 2][None] * sign
                lon = jnp.where(near, pltpu.roll(x, shift1, 2), pltpu.roll(x, shift2, 2))
                up = jnp.where(vert == -1.0, pltpu.roll(below, shift1, 2),
                               jnp.where(vert == 1.0, pltpu.roll(below, back1, 2), below))
                up = jnp.where(jnp.abs(vert) == 2.0, x, up)
                fresh[slot] = code_ref[ty, slot, 3][None] * (keep * x + wx * lon + wy * up)
            values = fresh
        for slot in (6, 7):
            prop_ref[i, :, lanes(slot)] = values[slot].reshape(size, NLON)
        whole = prop_ref[i]
        for c in range(ncomp):
            away_ref[c, i] = whole[:, c * share:(c + 1) * share].astype(BF16)

    groups = chunks // group

    def out_copy(j, g):
        to = lax.rem(me + j, ncomp)
        span = pl.ds(g * group, group)
        return pltpu.make_async_remote_copy(
            src_ref=away_ref.at[to, span], dst_ref=got_ref.at[me, span],
            send_sem=a_send.at[j], recv_sem=a_recv.at[j],
            device_id={"comp": to}, device_id_type=MESH)

    def whole_copy(j):
        to = lax.rem(me + j, ncomp)
        return pltpu.make_async_remote_copy(
            src_ref=away_ref.at[to], dst_ref=got_ref.at[me],
            send_sem=a_send.at[j], recv_sem=a_recv.at[j],
            device_id={"comp": to}, device_id_type=MESH)

    def run_group(g, carry):
        def one(i, inner):
            propagate(g * group + i)
            return inner

        lax.fori_loop(0, group, one, 0)
        for j in range(1, ncomp):
            out_copy(j, g).start()
        return carry

    lax.fori_loop(0, groups, run_group, 0)

    for q in (0, 1):
        sent(q, q)

    def drain(q, carry):
        sent(q, kind(q))
        return carry

    lax.fori_loop(2, chunks + 2, drain, 0)
    got_ref[me] = away_ref[me]
    load_w.wait()
    give_w.wait()

    for j in range(1, ncomp):
        whole_copy(j).wait()
    for c in range(ncomp):
        start_ref[c * bins:(c + 1) * bins, :] = got_ref[c].astype(F32).reshape(bins, share)
    tile = total // TILES
    per_tile = bins // tile if bins >= tile else tile // bins
    for m in range(TILES):
        span = slice(m * tile, (m + 1) * tile)
        low_ref[0, span, :] = start_ref[span, :].astype(BF16)

    def tile_rows(m):
        return pl.ds(pl.multiple_of(m * tile, 16), tile)

    def advance(step, m):
        span = tile_rows(m)
        driving = jnp.dot(w_ref[span, :], low_ref[step % 2], preferred_element_type=F32)
        now = start_ref[span, :] if step == 0 else state_ref[span, :]
        return span, now + STEP_SIZE * now * driving

    for step in range(SRC_STEPS - 1):
        def one_tile(m, carry, step=step):
            span, now = advance(step, m)
            state_ref[span, :] = now
            low_ref[(step + 1) % 2, span, :] = now.astype(BF16)
            return carry

        lax.fori_loop(0, TILES, one_tile, 0)

    def home_copy(j, to):
        return pltpu.make_async_remote_copy(
            src_ref=inc_ref.at[to], dst_ref=home_ref.at[me],
            send_sem=b_send.at[j], recv_sem=b_recv.at[j],
            device_id={"comp": to}, device_id_type=MESH)

    mine = lax.div(me * TILES, ncomp)

    def last_tile(i, carry):
        m = lax.rem(mine + 1 + i, TILES)
        span, now = advance(SRC_STEPS - 1, m)
        gain = now - start_ref[span, :]
        for k in range(per_tile):
            to = m * per_tile + k
            inc_ref[to] = gain[k * bins:(k + 1) * bins, :].astype(BF16)
            j = lax.rem(to - me + ncomp, ncomp)

            @pl.when(to != me)
            def _():
                home_copy(j, to).start()

        return carry

    lax.fori_loop(0, TILES, last_tile, 0)
    home_ref[me] = inc_ref[me]
    for c in range(ncomp):
        j = lax.rem(me - c + ncomp, ncomp)

        @pl.when(me != c)
        def _():
            home_copy(j, lax.rem(me + j, ncomp)).wait()

        cols = slice(c * share, (c + 1) * share)
        before = prop_ref[:, :, cols].reshape(bins, share)
        out_ref[:, cols] = sea[:, cols] * (before + home_ref[c].astype(F32))


def fast_kernel(
    ncomp, spec_ref, mask_hbm, nb_hbm, steps_hbm, cour_hbm, op_ref,
    out_ref, mask_ref, nb_ref, steps_ref, cour_ref, w_ref, full_ref, oth_ref, hsend_ref, halo_ref, code_ref, ang_ref, perm_ref,
    pout_ref, pin_ref, away_ref, x_ref, start_ref, state_ref, inc_ref, home_ref,
    l_sem, i_sem, w_sem, c_send, c_recv, r_send, r_recv, g_send, g_recv, h_send, h_recv,
    a_send, a_recv, o_sem, p_send, p_recv, b_send, b_recv,
):
    lat = lax.axis_index("lat")
    sub = lax.axis_index("sub")
    me = lax.axis_index("comp")
    groups = spec_ref.shape[0]
    bins = groups * 2 * 16
    kmax = halo_ref.shape[0]
    lanes = NLON // 2
    total = bins * ncomp
    partner = {"sub": 1 - sub}
    others = [partner, {"lat": 1 - lat}, {"lat": 1 - lat, "sub": 1 - sub}]

    small = [pltpu.make_async_copy(src, dst, i_sem.at[n]) for n, (src, dst) in enumerate((
        (mask_hbm, mask_ref.at[lat, sub]), (nb_hbm, nb_ref.at[lat, sub]),
        (steps_hbm, steps_ref), (cour_hbm, cour_ref)))]
    loads = []
    for r in range(2):
        cols = slice(r * NLON, (r + 1) * NLON)
        loads.append(pltpu.make_async_copy(
            spec_ref.at[:, 1 - sub, :, cols], oth_ref.at[pl.ds(0, groups), r], l_sem.at[r]))
        loads.append(pltpu.make_async_copy(
            spec_ref.at[:, sub, :, cols], full_ref.at[pl.ds(0, groups), 2 * sub + r], l_sem.at[2 + r]))
    for load in (small[0], *loads, *small[1:]):
        load.start()
    own_half = pl.ds(pl.multiple_of(sub * (total // 2), 16), total // 2)
    load_w = pltpu.make_async_copy(op_ref, w_ref.at[own_half], w_sem)

    barrier = pltpu.get_barrier_semaphore()
    peers = list(others)
    for d in range(1, ncomp):
        z = lax.rem(me + d, ncomp)
        peers += [{"comp": z}, {"comp": z, "sub": 1 - sub}]
    for peer in peers:
        pl.semaphore_signal(barrier, inc=1, device_id=peer, device_id_type=MESH)

    a = lax.broadcasted_iota(jnp.int32, (NLON, NLON), 0)
    b = lax.broadcasted_iota(jnp.int32, (NLON, NLON), 1)
    split = lambda c: jnp.where(c < lanes, 2 * c, 2 * (c - lanes) + 1)
    perm_ref[0] = (a == split(b)).astype(F32).astype(BF16)
    perm_ref[1] = (b == split(a)).astype(F32).astype(BF16)

    near_ty = lat
    far_ty = 1 - lat
    n0 = lax.rem(lat + me * groups, 2)
    f0 = 1 - n0
    for q, ty in enumerate((near_ty, far_ty)):
        d = lax.broadcasted_iota(jnp.int32, (16, lanes), 0) + 16 * (2 * ty + sub)
        angle = (d.astype(F32) + 0.5) * np.float32(2.0 * math.pi / ND)
        ang_ref[q, 0] = jnp.abs(jnp.cos(angle))
        ang_ref[q, 1] = jnp.abs(jnp.sin(angle))

    def point_copies(n):
        return [pltpu.make_async_remote_copy(
            src_ref=ref.at[lat, sub], dst_ref=ref.at[lat, sub], send_sem=c_send.at[n, m],
            recv_sem=c_recv.at[n, m], device_id=others[n], device_id_type=MESH)
            for m, ref in enumerate((mask_ref, nb_ref))]

    def raw_copies():
        return [pltpu.make_async_remote_copy(
            src_ref=spec_ref.at[:, 1 - sub, :, r * NLON:(r + 1) * NLON],
            dst_ref=full_ref.at[pl.ds(0, groups), 2 * sub + r],
            send_sem=r_send.at[r], recv_sem=r_recv.at[r], device_id=partner, device_id_type=MESH)
            for r in range(2)]

    def raw_waits():
        for r in range(2):
            pltpu.make_async_remote_copy(
                src_ref=spec_ref.at[:, 1 - sub, :, r * NLON:(r + 1) * NLON],
                dst_ref=full_ref.at[pl.ds(0, groups), 2 * (1 - sub) + r],
                send_sem=r_send.at[r], recv_sem=r_recv.at[r],
                device_id=partner, device_id_type=MESH).wait_recv()

    small[0].wait()
    small[1].wait()
    sea = mask_ref[lat, sub].astype(F32)
    for load in loads:
        load.wait()
    sea_rows = [jnp.broadcast_to(sea[:, r * NLON:(r + 1) * NLON], (16, NLON)) for r in range(2)]

    def convert(k, carry):
        j = n0 + 2 * k
        for r in range(2):
            mine = full_ref[j, 2 * sub + r] * sea_rows[r]
            other = oth_ref[j, r] * sea_rows[r]
            hsend_ref[k, sub, r] = mine.astype(BF16)
            hsend_ref[k, 1 - sub, r] = other.astype(BF16)
        return carry

    lax.fori_loop(0, kmax, convert, 0)
    pl.semaphore_wait(barrier, len(peers))
    def halo_copy(k, p):
        return pltpu.make_async_remote_copy(
            src_ref=hsend_ref.at[k, p], dst_ref=halo_ref.at[k, pl.ds(2 * sub, 2)],
            send_sem=h_send.at[k, p], recv_sem=h_recv.at[k, sub],
            device_id={"lat": 1 - lat, "sub": p}, device_id_type=MESH)

    def halo_wait(k, s):
        pltpu.make_async_remote_copy(
            src_ref=hsend_ref.at[k, s], dst_ref=halo_ref.at[k, pl.ds(2 * s, 2)],
            send_sem=h_send.at[k, s], recv_sem=h_recv.at[k, s],
            device_id={"lat": 1 - lat, "sub": s}, device_id_type=MESH).wait_recv()

    def give_w():
        return pltpu.make_async_remote_copy(
            src_ref=op_ref, dst_ref=w_ref.at[own_half], send_sem=g_send, recv_sem=g_recv,
            device_id=partner, device_id_type=MESH)

    def take_w():
        other_half = pl.ds(pl.multiple_of((1 - sub) * (total // 2), 16), total // 2)
        return pltpu.make_async_remote_copy(
            src_ref=op_ref, dst_ref=w_ref.at[other_half], send_sem=g_send, recv_sem=g_recv,
            device_id=partner, device_id_type=MESH)

    def send_halo(k, carry):
        @pl.when(n0 + 2 * k < groups)
        def _():
            for p in range(2):
                halo_copy(k, p).start()
        return carry

    for copy in point_copies(0):
        copy.start()
    lax.fori_loop(0, FAR, send_halo, 0)
    for copy in (*raw_copies(), *point_copies(1), *point_copies(2)):
        copy.start()
    lax.fori_loop(FAR, kmax, send_halo, 0)
    load_w.start()
    give_w().start()
    for load in small[2:]:
        load.wait()

    points = mask_ref.shape[-1]
    lane = lax.broadcasted_iota(jnp.int32, (1, points), 1)
    column = lane & (NLON - 1)
    index = lax.broadcasted_iota(jnp.int32, (8, points), 0)

    def decode(chip):
        for s in range(2):
            nb = nb_ref[chip, s]
            west = (column - nb[0:1, :]) & (NLON - 1)
            east = (nb[1:2, :] - column) & (NLON - 1)
            moves = [((nb[k:k + 1, :] - column + 1) & (NLON - 1)) - 1 for k in (2, 3)]
            codes = jnp.zeros((8, points), F32)
            for k, entry in enumerate((west, east, *moves, mask_ref[chip, s])):
                codes = jnp.where(index == k, jnp.broadcast_to(entry.astype(F32), (8, points)), codes)
            for r in range(2):
                part = codes[:, r * NLON:(r + 1) * NLON].astype(BF16)
                both = jnp.dot(part, perm_ref[0], preferred_element_type=F32)
                for k in range(5):
                    code_ref[chip, 2 * s + r, k] = jnp.broadcast_to(both[k:k + 1, :], (8, NLON))

    side = lax.div(me, 2)

    def target(i):
        near = me + 1 - 2 * lax.rem(me, 2)
        return jnp.where(i == 0, 3 - 3 * side, jnp.where(i == 1, 2 - side, jnp.where(i == 2, near, me)))

    def chunk_copy(h, j, i):
        to = target(i)
        return pltpu.make_async_remote_copy(
            src_ref=away_ref.at[h, to, j], dst_ref=x_ref.at[0, me * groups + j, sub],
            send_sem=a_send.at[h, i], recv_sem=a_recv.at[me, sub],
            device_id={"comp": to, "sub": h}, device_id_type=MESH)

    def whole_copy(h, i):
        to = target(i)
        return pltpu.make_async_remote_copy(
            src_ref=away_ref.at[h, to, pl.ds(0, groups)],
            dst_ref=x_ref.at[0, pl.ds(me * groups, groups), sub],
            send_sem=a_send.at[h, i], recv_sem=a_recv.at[me, sub],
            device_id={"comp": to, "sub": h}, device_id_type=MESH)

    def whole_wait(z, s):
        pltpu.make_async_remote_copy(
            src_ref=away_ref.at[0, z, pl.ds(0, groups)],
            dst_ref=x_ref.at[0, pl.ds(z * groups, groups), s],
            send_sem=a_send.at[0, 0], recv_sem=a_recv.at[z, s],
            device_id={"comp": z, "sub": s}, device_id_type=MESH).wait_recv()

    def pick(ty, i):
        return ty * 3 + (1 - 2 * ty) * i

    def separate(x):
        high = x.astype(BF16)
        low = (x - high.astype(F32)).astype(BF16)
        return high, low

    def propagate(ks, far, to_east):
        ty = far_ty if far else near_ty
        js = [(f0 if far else n0) + 2 * k for k in ks]
        vert = 2 + ty
        lowest = 0 if far else 4

        def code(q, k, half):
            chip = lat if q >= 4 else 1 - lat
            part = code_ref[chip, pick(ty, q % 4), k, :, half * lanes:(half + 1) * lanes]
            return jnp.concatenate([part, part], axis=0)

        raw = jnp.concatenate([full_ref[j, pick(ty, i)] for j in js for i in range(4)], axis=0)
        high, low = separate(raw)
        mixed = (jnp.dot(high, perm_ref[0], preferred_element_type=F32)
                 + jnp.dot(low, perm_ref[0], preferred_element_type=F32))
        if far:
            edge = jnp.concatenate([halo_ref[k, pick(ty, i)] for k in ks for i in range(4)], axis=0)
            edge = jnp.dot(edge, perm_ref[0], preferred_element_type=F32)
        cells = []
        weights = []
        for n, j in enumerate(js):
            values = [None] * 8
            for i in range(4):
                rows = slice((n * 4 + i) * 16, (n * 4 + i + 1) * 16)
                values[4 + i] = tuple(
                    mixed[rows, half * lanes:(half + 1) * lanes] * code(4 + i, 4, half)
                    for half in range(2))
                if far:
                    values[i] = tuple(edge[rows, half * lanes:(half + 1) * lanes] for half in range(2))
            cells.append(values)
            freq = jnp.minimum(lax.div(me * bins + j * 32, ND), steps_ref.shape[0] - 1)
            weights.append((steps_ref[freq], cour_ref[freq]))
        abs_cos, abs_sin = ang_ref[int(far), 0], ang_ref[int(far), 1]
        ahead, behind = (1, lanes - 1)
        for t in range(MAXSTEPS):
            slots = [q for q in range(7, lowest - 1, -1) if q >= 4 or t <= q + 1]
            for n, (steps, speed) in enumerate(weights):
                live = jnp.where(t < steps, speed, 0.0)
                wx = live * abs_cos
                wy = live * abs_sin
                keep = 1.0 - wx - wy
                values = cells[n]
                fresh = list(values)
                turned = {}

                def turn(q, half, shift):
                    key = (q, half, shift)
                    if key not in turned:
                        turned[key] = pltpu.roll(values[q][half], shift, 1)
                    return turned[key]

                def left(q):
                    return turn(q, 1, ahead), values[q][0]

                def right(q):
                    return values[q][1], turn(q, 0, behind)

                for q in slots:
                    shift = ahead if to_east else behind
                    one = left(q) if to_east else right(q)
                    lon_code = 0 if to_east else 1
                    new = []
                    for half in range(2):
                        x = values[q][half]
                        lon = jnp.where(code(q, lon_code, half) == 1.0, one[half], turn(q, half, shift))
                        if q == lowest:
                            up = x
                        else:
                            move = code(q, vert, half)
                            up = jnp.where(move == -1.0, left(q - 1)[half],
                                           jnp.where(move == 1.0, right(q - 1)[half], values[q - 1][half]))
                        new.append(code(q, 4, half) * (keep * x + wx * lon + wy * up))
                    fresh[q] = tuple(new)
                cells[n] = fresh
        for n, j in enumerate(js):
            for i in range(4):
                r = pick(ty, i)
                for half in range(2):
                    value = cells[n][4 + i][half]
                    pout_ref[j, r, :, half * lanes:(half + 1) * lanes] = value
                    away_ref[lax.div(r, 2), 2 * lax.rem(r, 2) + half, j] = value.astype(BF16)
        for n, j in enumerate(js):
            @pl.when(j < groups)
            def _():
                for i in range(ncomp - 1):
                    chunk_copy(0, j, i).start()

    straight = sub == lat
    for copy in point_copies(0):
        copy.wait_recv()
    decode(lat)
    raw_waits()

    def near_body(g, carry):
        ks = [g * NEAR + n for n in range(NEAR)]

        @pl.when(straight)
        def _():
            propagate(ks, False, True)

        @pl.when(jnp.logical_not(straight))
        def _():
            propagate(ks, False, False)
        return carry

    lax.fori_loop(0, kmax // NEAR, near_body, 0)
    for n in (1, 2):
        for copy in point_copies(n):
            copy.wait_recv()
    decode(1 - lat)

    def far_body(g, carry):
        ks = [g * FAR + n for n in range(FAR)]
        for k in ks:
            @pl.when(f0 + 2 * k < groups)
            def _():
                for s in range(2):
                    halo_wait(k, s)

        @pl.when(straight)
        def _():
            propagate(ks, True, False)

        @pl.when(jnp.logical_not(straight))
        def _():
            propagate(ks, True, True)

        for k in ks:
            @pl.when((n0 + 2 * k < groups) & (k < NEAR))
            def _():
                for i in range(ncomp - 1):
                    chunk_copy(1, n0 + 2 * k, i).start()
        return carry

    lax.fori_loop(0, kmax // FAR, far_body, 0)

    own_copy = pltpu.make_async_copy(
        away_ref.at[sub, me, pl.ds(0, groups)], x_ref.at[0, pl.ds(me * groups, groups), sub], o_sem)

    def cross_copy():
        return pltpu.make_async_remote_copy(
            src_ref=away_ref.at[1 - sub, me, pl.ds(0, groups)],
            dst_ref=x_ref.at[0, pl.ds(me * groups, groups), sub],
            send_sem=a_send.at[0, ncomp - 1], recv_sem=a_recv.at[me, sub],
            device_id=partner, device_id_type=MESH)

    def prop_copy():
        return pltpu.make_async_remote_copy(
            src_ref=pout_ref.at[pl.ds(0, groups), pl.ds(2 * (1 - sub), 2)],
            dst_ref=pin_ref, send_sem=p_send, recv_sem=p_recv,
            device_id=partner, device_id_type=MESH)

    own_copy.start()
    cross_copy().start()

    def send_rest(k, carry):
        @pl.when(f0 + 2 * k < groups)
        def _():
            for i in range(ncomp - 1):
                chunk_copy(1, f0 + 2 * k, i).start()
        return carry

    def send_near(k, carry):
        @pl.when(n0 + 2 * k < groups)
        def _():
            for i in range(ncomp - 1):
                chunk_copy(1, n0 + 2 * k, i).start()
        return carry

    lax.fori_loop(0, kmax, send_rest, 0)
    lax.fori_loop(NEAR, kmax, send_near, 0)
    prop_copy().start()

    def home_copy(m):
        return pltpu.make_async_remote_copy(
            src_ref=inc_ref.at[m], dst_ref=home_ref.at[me],
            send_sem=b_send.at[m], recv_sem=b_recv.at[me],
            device_id={"comp": m}, device_id_type=MESH)

    early = (2 * bins) // 128 * 128
    late = total - early

    once = 1 + lax.div(me, ncomp)

    def partial(start, span, use):
        def one(i, carry):
            rows = pl.ds(pl.multiple_of(i * total, 16), total)
            field = x_ref[0, pl.ds(lax.div(start, 32), span // 32)].reshape(span, lanes)
            cols = pl.ds(pl.multiple_of(start, 128), span)
            use(rows, jnp.dot(w_ref[rows, cols], field, preferred_element_type=F32))
            return carry

        lax.fori_loop(0, once, one, 0)

    def begin():
        def use(rows, driving):
            state_ref[rows, :] = driving

        partial(side * late, early, use)

    def first_step():
        def use(rows, driving):
            start = x_ref[0].reshape(total, lanes).astype(F32)
            now = start + STEP_SIZE * start * (state_ref[rows, :] + driving)
            start_ref[rows, :] = start
            state_ref[rows, :] = now
            x_ref[1] = now.astype(BF16).reshape(ncomp * groups, 2, 16, lanes)

        partial((1 - side) * early, late, use)

    def advance(step, carry):
        field = x_ref[lax.rem(step, 2)].reshape(total, lanes)
        driving = jnp.dot(w_ref[...], field, preferred_element_type=F32)
        now = state_ref[...]
        now = now + STEP_SIZE * now * driving
        state_ref[...] = now
        x_ref[lax.rem(step + 1, 2)] = now.astype(BF16).reshape(ncomp * groups, 2, 16, lanes)
        return carry

    def finish():
        def one(i, carry):
            m = target(i)
            rows = pl.ds(pl.multiple_of(m * bins, 16), bins)
            field = x_ref[(SRC_STEPS - 1) % 2].reshape(total, lanes)
            driving = jnp.dot(w_ref[rows, :], field, preferred_element_type=F32)
            now = state_ref[rows, :]
            now = now + STEP_SIZE * now * driving
            inc_ref[m] = (now - start_ref[rows, :]).astype(BF16)

            @pl.when(m != me)
            def _():
                home_copy(m).start()
            return carry

        lax.fori_loop(0, ncomp, one, 0)

    sea_wide = [jnp.broadcast_to(sea[:, r * NLON:(r + 1) * NLON], (16, NLON)) for r in range(2)]

    def restore(g, carry):
        js = [g * BACK + n for n in range(BACK)]
        parts = [ref for j in js for ref in (
            pout_ref[j, 2 * sub], pout_ref[j, 2 * sub + 1], pin_ref[j, 0], pin_ref[j, 1])]
        high, low = separate(jnp.concatenate(parts, axis=0))
        plain = (jnp.dot(high, perm_ref[1], preferred_element_type=F32)
                 + jnp.dot(low, perm_ref[1], preferred_element_type=F32))
        for n in range(4 * BACK):
            p = sub if n % 4 < 2 else 1 - sub
            rows = pl.ds(pl.multiple_of((2 * js[n // 4] + p) * 16, 16), 16)
            r = n % 2
            out_ref[rows, r * NLON:(r + 1) * NLON] = sea_wide[r] * plain[n * 16:(n + 1) * 16, :]
        return carry

    def restore_all():
        prop_copy().wait_recv()
        lax.fori_loop(0, groups // BACK, restore, 0)

    pl.when(sub == 1)(restore_all)
    load_w.wait()
    take_w().wait_recv()
    own_copy.wait()
    whole_wait(me, 1 - sub)
    for s in range(2):
        whole_wait(target(2), s)
    begin()
    for i in (1, 0):
        for s in range(2):
            whole_wait(target(i), s)
    first_step()
    lax.fori_loop(1, SRC_STEPS - 1, advance, 0)
    finish()

    pl.when(sub == 0)(restore_all)
    for i in (3, 2, 1, 0):
        z = target(i)

        def land():
            pltpu.make_async_remote_copy(
                src_ref=inc_ref.at[z], dst_ref=home_ref.at[z],
                send_sem=b_send.at[z], recv_sem=b_recv.at[z],
                device_id={"comp": z}, device_id_type=MESH).wait_recv()

        if i < 3:
            land()
        r = lax.div(z, 2)
        half = lax.rem(z, 2)
        cols = pl.ds(pl.multiple_of(r * NLON, NLON), NLON)
        spread = perm_ref[1, pl.ds(pl.multiple_of(half * lanes, lanes), lanes), :]
        sea_row = jnp.where(r == 0, sea_wide[0][0:8], sea_wide[1][0:8])
        arrived = inc_ref[z] if i == 3 else home_ref[z]
        back = jnp.dot(arrived, spread, preferred_element_type=F32)
        back = back.reshape(bins // 8, 8, NLON) * sea_row[None]
        out_ref[:, cols] = out_ref[:, cols] + back.reshape(bins, NLON)

    for n in range(3):
        for copy in point_copies(n):
            copy.wait_send()
    for copy in raw_copies():
        copy.wait_send()

    def halo_left(k, carry):
        @pl.when(n0 + 2 * k < groups)
        def _():
            for p in range(2):
                halo_copy(k, p).wait_send()
        return carry

    lax.fori_loop(0, kmax, halo_left, 0)
    prop_copy().wait_send()
    cross_copy().wait_send()
    give_w().wait_send()
    for i in range(ncomp - 1):
        for h in range(2):
            whole_copy(h, i).wait_send()
        home_copy(target(i)).wait_send()


def write_kernel(src_ref, dst_ref, sems):
    pieces = sems.shape[0]
    rows = src_ref.shape[0] // pieces
    copies = [pltpu.make_async_copy(
        src_ref.at[pl.ds(i * rows, rows)], dst_ref.at[pl.ds(i * rows, rows)], sems.at[i])
        for i in range(pieces)]
    for copy in copies:
        copy.start()
    for copy in copies:
        copy.wait()


def fast_device(ncomp, spectrum, sea_mask, neighbours, substeps, courant, source_operator):
    bins, points = spectrum.shape
    groups = bins // 32
    kmax = (groups + 1) // 2
    lanes = NLON // 2
    total = bins * ncomp
    vmem = pl.BlockSpec(memory_space=pltpu.VMEM)
    hbm = pl.BlockSpec(memory_space=pltpu.HBM)
    dma = pltpu.SemaphoreType.DMA
    result = pl.pallas_call(
        functools.partial(fast_kernel, ncomp),
        out_shape=pltpu.VMEM((bins, points), F32),
        in_specs=[hbm] * 6,
        out_specs=vmem,
        scratch_shapes=[
            pltpu.VMEM((2, 2, 1, points), jnp.int32),
            pltpu.VMEM((2, 2, 4, points), jnp.int32),
            pltpu.SMEM(substeps.shape, jnp.int32),
            pltpu.SMEM(courant.shape, F32),
            pltpu.VMEM((total, total), BF16),
            pltpu.VMEM((2 * kmax, 4, 16, NLON), F32),
            pltpu.VMEM((2 * kmax, 2, 16, NLON), F32),
            pltpu.VMEM((kmax, 2, 2, 16, NLON), BF16),
            pltpu.VMEM((kmax, 4, 16, NLON), BF16),
            pltpu.VMEM((2, 4, 5, 8, NLON), F32),
            pltpu.VMEM((2, 2, 16, lanes), F32),
            pltpu.VMEM((2, NLON, NLON), BF16),
            pltpu.VMEM((2 * kmax, 4, 16, NLON), F32),
            pltpu.VMEM((groups, 2, 16, NLON), F32),
            pltpu.VMEM((2, ncomp, 2 * kmax, 16, lanes), BF16),
            pltpu.VMEM((2, ncomp * groups, 2, 16, lanes), BF16),
            pltpu.VMEM((total, lanes), F32),
            pltpu.VMEM((total, lanes), F32),
            pltpu.VMEM((ncomp, bins, lanes), BF16),
            pltpu.VMEM((ncomp, bins, lanes), BF16),
            dma((4,)), dma((4,)), dma, dma((3, 2)), dma((3, 2)), dma((2,)), dma((2,)), dma, dma,
            dma((kmax, 2)), dma((kmax, 2)), dma((2, ncomp)), dma((ncomp, 2)), dma, dma, dma,
            dma((ncomp,)), dma((ncomp,)),
        ],
        compiler_params=pltpu.CompilerParams(
            collective_id=1, has_side_effects=True, vmem_limit_bytes=60 * 1024 * 1024),
    )(spectrum.reshape(groups, 2, 16, points), sea_mask.reshape(1, points), neighbours, substeps, courant,
      source_operator)
    return pl.pallas_call(
        write_kernel,
        out_shape=jax.ShapeDtypeStruct((bins, points), F32),
        in_specs=[vmem],
        out_specs=hbm,
        scratch_shapes=[dma((4,))],
        compiler_params=pltpu.CompilerParams(vmem_limit_bytes=4 * 1024 * 1024),
    )(result)


def solution(mesh):
    nlat, ncomp = mesh.shape["lat"], mesh.shape["comp"]

    def per_device(spectrum, sea_mask, neighbours, substeps, courant, source_operator):
        bins, points = spectrum.shape
        even = bins % 32 == 0 and (bins // 32 + 1) // 2 % NEAR == 0 and bins // 32 % BACK == 0
        if nlat == 2 and ncomp == 4 and points == 2 * NLON and even:
            return fast_device(ncomp, spectrum, sea_mask, neighbours, substeps, courant, source_operator)
        size = 16 if bins % 16 == 0 else 8
        chunks = bins // size
        group = 5 if chunks % 5 == 0 else 1
        share = points // ncomp
        total = bins * ncomp
        angles = (np.arange(ND, dtype=np.float32) + np.float32(0.5)) * np.float32(2.0 * math.pi / ND)
        spread = lambda v: jnp.asarray(
            np.broadcast_to(np.abs(v).astype(np.float32)[:, None], (ND, NLON)).reshape(ND // 8, 8, NLON))
        vmem = pl.BlockSpec(memory_space=pltpu.VMEM)
        smem = pl.BlockSpec(memory_space=pltpu.SMEM)
        kinds = 3 if nlat == 2 else 4
        return pl.pallas_call(
            functools.partial(kernel, nlat, ncomp, group),
            out_shape=jax.ShapeDtypeStruct((bins, points), F32),
            in_specs=[vmem, vmem, vmem, smem, smem, vmem, vmem, pl.BlockSpec(memory_space=pl.ANY)],
            out_specs=vmem,
            scratch_shapes=[
                pltpu.VMEM((total, total), BF16),
                pltpu.VMEM((chunks + 2, size, points), BF16),
                pltpu.VMEM((3, chunks + 2, size, points), BF16),
                pltpu.VMEM((2, SLOTS, 4, 8, NLON), F32),
                pltpu.VMEM((chunks, size, points), F32),
                pltpu.VMEM((ncomp, chunks, size, share), BF16),
                pltpu.VMEM((ncomp, chunks, size, share), BF16),
                pltpu.VMEM((total, share), F32),
                pltpu.VMEM((total, share), F32),
                pltpu.VMEM((2, total, share), BF16),
                pltpu.VMEM((ncomp, bins, share), BF16),
                pltpu.VMEM((ncomp, bins, share), BF16),
                pltpu.SemaphoreType.DMA((kinds, chunks + 2)),
                pltpu.SemaphoreType.DMA((kinds, chunks + 2)),
                pltpu.SemaphoreType.DMA,
                pltpu.SemaphoreType.DMA,
                pltpu.SemaphoreType.DMA,
                pltpu.SemaphoreType.DMA((ncomp,)),
                pltpu.SemaphoreType.DMA((ncomp,)),
                pltpu.SemaphoreType.DMA((ncomp,)),
                pltpu.SemaphoreType.DMA((ncomp,)),
            ],
            compiler_params=pltpu.CompilerParams(
                collective_id=0, has_side_effects=True, vmem_limit_bytes=56 * 1024 * 1024),
        )(spectrum, sea_mask.reshape(1, points), neighbours, substeps, courant,
          spread(np.cos(angles)), spread(np.sin(angles)), source_operator)

    placed = (
        P("comp", ("members", "lat", "sub")),
        P(("members", "lat", "sub")),
        P(None, ("members", "lat", "sub")),
        P(),
        P(),
        P("sub", None),
    )
    return jax.shard_map(
        per_device,
        mesh=mesh,
        in_specs=placed,
        out_specs=P("comp", ("members", "lat", "sub")),
        check_vma=False,
    )
```

```python
import functools
import math

import jax
import jax.numpy as jnp
import numpy as np
from jax import lax
from jax.experimental import pallas as pl
from jax.experimental.pallas import tpu as pltpu
from jax.sharding import PartitionSpec as P

NF = 30
ND = 64
NLON = 256
MAXSTEPS = 6
SRC_STEPS = 4
STEP_SIZE = 0.1
MESH = pl.DeviceIdType.MESH
HALF = ND // 2
TILES = 4
SLOTS = 8
NEAR = 4
FAR = 2
BACK = 5
AHEAD = 2
PIECES = 2
F32 = jnp.float32
BF16 = jnp.bfloat16


def kernel(
    nlat, ncomp, group, spec_ref, mask_ref, nb_ref, steps_ref, cour_ref, cos_ref, sin_ref, op_ref,
    out_ref, w_ref, own_ref, halo_ref, code_ref, prop_ref, away_ref, got_ref, start_ref, state_ref,
    low_ref, inc_ref, home_ref,
    h_send, h_recv, w_send, w_recv, w_local, a_send, a_recv, b_send, b_recv,
):
    lat = lax.axis_index("lat")
    sub = lax.axis_index("sub")
    me = lax.axis_index("comp")
    bins, points = spec_ref.shape
    chunks, size = prop_ref.shape[0], prop_ref.shape[1]
    planes = size // 8
    share = points // ncomp
    total = bins * ncomp
    half_rows = total // 2
    first = me * bins
    last_lat = nlat - 1
    partner = {"sub": 1 - sub}

    barrier = pltpu.get_barrier_semaphore()
    peers = [partner]
    if nlat == 2:
        peers.append({"lat": 1 - lat})
    else:
        for move in (1, -1):
            peers.append({"lat": lax.rem(lat + move + nlat, nlat)})
            peers.append({"lat": lax.rem(lat + 2 * move + nlat, nlat), "sub": 1 - sub})
    for j in range(1, ncomp):
        peers.append({"comp": lax.rem(me + j, ncomp)})
    for peer in peers:
        pl.semaphore_signal(barrier, inc=1, device_id=peer, device_id_type=MESH)

    own_half = pl.ds(pl.multiple_of(sub * half_rows, 16), half_rows)
    load_w = pltpu.make_async_copy(op_ref, w_ref.at[own_half], w_local)
    load_w.start()

    lane = lax.broadcasted_iota(jnp.int32, (1, points), 1)
    column = lane & (NLON - 1)
    position = (lat * 2 + sub) * points + lane
    sea = mask_ref[...].astype(F32)
    west = (column - nb_ref[0:1, :]) & (NLON - 1)
    east = (nb_ref[1:2, :] - column) & (NLON - 1)

    def vertical(index_row):
        moved = ((index_row - column + 1) & (NLON - 1)) - 1
        return jnp.where(index_row == position, 2, moved)

    rows = lax.broadcasted_iota(jnp.int32, (size, points), 0)
    codes = jnp.zeros((size, points), F32)
    entries = [west, east, vertical(nb_ref[2:3, :]), vertical(nb_ref[3:4, :])]
    for k, entry in enumerate([e.astype(F32) for e in entries] + [sea]):
        codes = jnp.where(rows == k, jnp.broadcast_to(entry, (size, points)), codes)
    own_ref[0] = codes.astype(BF16)
    own_ref[1] = codes.astype(BF16)

    pl.semaphore_wait(barrier, len(peers))

    def kind(q):
        return lax.rem(lax.div(first + (q - 2) * size, HALF), 2)

    def has_from(ty, far):
        return jnp.where(ty == 0, lat >= far, lat <= last_lat - far)

    def has_to(ty, far):
        return jnp.where(ty == 0, lat <= last_lat - far, lat >= far)

    def pair_copy(q):
        return pltpu.make_async_remote_copy(
            src_ref=own_ref.at[q], dst_ref=halo_ref.at[0, q], send_sem=h_send.at[0, q],
            recv_sem=h_recv.at[0, q], device_id=partner, device_id_type=MESH)

    def side_copy(q, ty):
        to = jnp.clip(lat + 1 - 2 * ty, 0, last_lat)
        return pltpu.make_async_remote_copy(
            src_ref=own_ref.at[q], dst_ref=halo_ref.at[1, q], send_sem=h_send.at[1, q],
            recv_sem=h_recv.at[1, q], device_id={"lat": to}, device_id_type=MESH)

    def hand_copy(q, ty):
        slot = jnp.where(sub == ty, 2, 0)
        return pltpu.make_async_remote_copy(
            src_ref=halo_ref.at[1, q], dst_ref=halo_ref.at[slot, q], send_sem=h_send.at[2, q],
            recv_sem=h_recv.at[2, q], device_id=partner, device_id_type=MESH)

    def far_copy(q, ty):
        to = jnp.clip(lat + 2 - 4 * ty, 0, last_lat)
        return pltpu.make_async_remote_copy(
            src_ref=own_ref.at[q], dst_ref=halo_ref.at[2, q], send_sem=h_send.at[3, q],
            recv_sem=h_recv.at[3, q], device_id={"lat": to, "sub": 1 - sub}, device_id_type=MESH)

    def send_own(q, ty):
        @pl.when(has_to(ty, 1))
        def _():
            side_copy(q, ty).start()

        @pl.when(sub == ty)
        def _():
            pair_copy(q).start()

        if nlat > 2:
            @pl.when((sub != ty) & has_to(ty, 2))
            def _():
                far_copy(q, ty).start()

    def hand_on(q, ty):
        @pl.when(has_from(ty, 1))
        def _():
            side_copy(q, ty).wait_recv()
            hand_copy(q, ty).start()

    def arrive(q, ty):
        @pl.when(has_from(ty, 1))
        def _():
            hand_copy(q, ty).wait_recv()

        @pl.when(sub != ty)
        def _():
            pair_copy(q).wait_recv()

        if nlat > 2:
            @pl.when((sub == ty) & has_from(ty, 2))
            def _():
                far_copy(q, ty).wait_recv()

    def sent(q, ty):
        @pl.when(has_to(ty, 1))
        def _():
            side_copy(q, ty).wait_send()

        @pl.when(sub == ty)
        def _():
            pair_copy(q).wait_send()

        if nlat > 2:
            @pl.when((sub != ty) & has_to(ty, 2))
            def _():
                far_copy(q, ty).wait_send()

        @pl.when(has_from(ty, 1))
        def _():
            hand_copy(q, ty).wait_send()

    send_own(0, 0)
    send_own(1, 1)

    def prepare(i, carry):
        chunk = sea * spec_ref[pl.ds(pl.multiple_of(i * size, size), size), :]
        own_ref[i + 2] = chunk.astype(BF16)
        send_own(i + 2, kind(i + 2))
        return carry

    lax.fori_loop(0, chunks, prepare, 0)

    give_w = pltpu.make_async_remote_copy(
        src_ref=op_ref, dst_ref=w_ref.at[own_half], send_sem=w_send, recv_sem=w_recv,
        device_id=partner, device_id_type=MESH)
    give_w.start()

    for q in (0, 1):
        hand_on(q, q)
    ahead = min(6, chunks)
    for q in range(2, 2 + ahead):
        hand_on(q, kind(q))

    for ty in (0, 1):
        arrive(ty, ty)
        for slot in range(SLOTS):
            row = slot % 2 if ty == 0 else 1 - slot % 2
            cols = slice(row * NLON, (row + 1) * NLON)
            if slot < 6:
                part = halo_ref[2 - slot // 2, ty, :, cols].astype(F32)
            else:
                part = own_ref[ty, :, cols].astype(F32)
            for k, source in enumerate((0, 1, 2 + ty, 4)):
                code_ref[ty, slot, k] = jnp.broadcast_to(part[source:source + 1, :], (8, NLON))

    def propagate(i):
        q = i + 2
        ty = kind(q)

        @pl.when(i + ahead < chunks)
        def _():
            hand_on(q + ahead, kind(q + ahead))

        arrive(q, ty)
        bin0 = first + i * size
        freq = lax.div(bin0, ND)
        direction = lax.rem(bin0, ND)
        to_east = jnp.where((direction < ND // 4) | (direction >= 3 * ND // 4), 1, 0)
        steps = steps_ref[freq]
        speed = cour_ref[freq]
        sign = jnp.where(to_east == 1, 1.0, -1.0)
        shift1 = jnp.where(to_east == 1, 1, NLON - 1)
        shift2 = jnp.where(to_east == 1, 2, NLON - 2)
        back1 = NLON - shift1
        d8 = lax.div(direction, 8)
        abs_cos = cos_ref[pl.ds(d8, planes)]
        abs_sin = sin_ref[pl.ds(d8, planes)]

        def lanes(slot):
            row = jnp.where(ty == 0, slot % 2, 1 - slot % 2)
            return pl.ds(pl.multiple_of(row * NLON, NLON), NLON)

        values = []
        for slot in range(SLOTS):
            if slot < 6:
                part = halo_ref[2 - slot // 2, q, :, lanes(slot)].astype(F32)
            else:
                part = spec_ref[pl.ds(pl.multiple_of(i * size, size), size), lanes(slot)]
            part = part.reshape(planes, 8, NLON)
            if slot >= 6:
                part = part * code_ref[ty, slot, 3][None]
            values.append(part)
        for t in range(MAXSTEPS):
            live = jnp.where(t < steps, speed, 0.0)
            wx = live * abs_cos
            wy = live * abs_sin
            keep = 1.0 - wx - wy
            fresh = list(values)
            for slot in range(t + 1, SLOTS):
                x = values[slot]
                below = values[slot - 1]
                near = code_ref[ty, slot, 1 - to_east][None] == 1.0
                vert = code_ref[ty, slot, 2][None] * sign
                lon = jnp.where(near, pltpu.roll(x, shift1, 2), pltpu.roll(x, shift2, 2))
                up = jnp.where(vert == -1.0, pltpu.roll(below, shift1, 2),
                               jnp.where(vert == 1.0, pltpu.roll(below, back1, 2), below))
                up = jnp.where(jnp.abs(vert) == 2.0, x, up)
                fresh[slot] = code_ref[ty, slot, 3][None] * (keep * x + wx * lon + wy * up)
            values = fresh
        for slot in (6, 7):
            prop_ref[i, :, lanes(slot)] = values[slot].reshape(size, NLON)
        whole = prop_ref[i]
        for c in range(ncomp):
            away_ref[c, i] = whole[:, c * share:(c + 1) * share].astype(BF16)

    groups = chunks // group

    def out_copy(j, g):
        to = lax.rem(me + j, ncomp)
        span = pl.ds(g * group, group)
        return pltpu.make_async_remote_copy(
            src_ref=away_ref.at[to, span], dst_ref=got_ref.at[me, span],
            send_sem=a_send.at[j], recv_sem=a_recv.at[j],
            device_id={"comp": to}, device_id_type=MESH)

    def whole_copy(j):
        to = lax.rem(me + j, ncomp)
        return pltpu.make_async_remote_copy(
            src_ref=away_ref.at[to], dst_ref=got_ref.at[me],
            send_sem=a_send.at[j], recv_sem=a_recv.at[j],
            device_id={"comp": to}, device_id_type=MESH)

    def run_group(g, carry):
        def one(i, inner):
            propagate(g * group + i)
            return inner

        lax.fori_loop(0, group, one, 0)
        for j in range(1, ncomp):
            out_copy(j, g).start()
        return carry

    lax.fori_loop(0, groups, run_group, 0)

    for q in (0, 1):
        sent(q, q)

    def drain(q, carry):
        sent(q, kind(q))
        return carry

    lax.fori_loop(2, chunks + 2, drain, 0)
    got_ref[me] = away_ref[me]
    load_w.wait()
    give_w.wait()

    for j in range(1, ncomp):
        whole_copy(j).wait()
    for c in range(ncomp):
        start_ref[c * bins:(c + 1) * bins, :] = got_ref[c].astype(F32).reshape(bins, share)
    tile = total // TILES
    per_tile = bins // tile if bins >= tile else tile // bins
    for m in range(TILES):
        span = slice(m * tile, (m + 1) * tile)
        low_ref[0, span, :] = start_ref[span, :].astype(BF16)

    def tile_rows(m):
        return pl.ds(pl.multiple_of(m * tile, 16), tile)

    def advance(step, m):
        span = tile_rows(m)
        driving = jnp.dot(w_ref[span, :], low_ref[step % 2], preferred_element_type=F32)
        now = start_ref[span, :] if step == 0 else state_ref[span, :]
        return span, now + STEP_SIZE * now * driving

    for step in range(SRC_STEPS - 1):
        def one_tile(m, carry, step=step):
            span, now = advance(step, m)
            state_ref[span, :] = now
            low_ref[(step + 1) % 2, span, :] = now.astype(BF16)
            return carry

        lax.fori_loop(0, TILES, one_tile, 0)

    def home_copy(j, to):
        return pltpu.make_async_remote_copy(
            src_ref=inc_ref.at[to], dst_ref=home_ref.at[me],
            send_sem=b_send.at[j], recv_sem=b_recv.at[j],
            device_id={"comp": to}, device_id_type=MESH)

    mine = lax.div(me * TILES, ncomp)

    def last_tile(i, carry):
        m = lax.rem(mine + 1 + i, TILES)
        span, now = advance(SRC_STEPS - 1, m)
        gain = now - start_ref[span, :]
        for k in range(per_tile):
            to = m * per_tile + k
            inc_ref[to] = gain[k * bins:(k + 1) * bins, :].astype(BF16)
            j = lax.rem(to - me + ncomp, ncomp)

            @pl.when(to != me)
            def _():
                home_copy(j, to).start()

        return carry

    lax.fori_loop(0, TILES, last_tile, 0)
    home_ref[me] = inc_ref[me]
    for c in range(ncomp):
        j = lax.rem(me - c + ncomp, ncomp)

        @pl.when(me != c)
        def _():
            home_copy(j, lax.rem(me + j, ncomp)).wait()

        cols = slice(c * share, (c + 1) * share)
        before = prop_ref[:, :, cols].reshape(bins, share)
        out_ref[:, cols] = sea[:, cols] * (before + home_ref[c].astype(F32))


def fast_kernel(
    ncomp, spec_ref, mask_hbm, nb_hbm, steps_hbm, cour_hbm, op_ref,
    out_ref, mask_ref, nb_ref, steps_ref, cour_ref, w_ref, full_ref, oth_ref, hsend_ref, halo_ref, code_ref, ang_ref, perm_ref,
    pout_ref, pin_ref, away_ref, x_ref, start_ref, state_ref, inc_ref, home_ref,
    l_sem, i_sem, w_sem, c_send, c_recv, r_send, r_recv, g_send, g_recv, h_send, h_recv,
    a_send, a_recv, t_send, t_recv, o_sem, p_send, p_recv, b_send, b_recv,
):
    lat = lax.axis_index("lat")
    sub = lax.axis_index("sub")
    me = lax.axis_index("comp")
    groups = spec_ref.shape[0]
    bins = groups * 2 * 16
    kmax = halo_ref.shape[0]
    lanes = NLON // 2
    total = bins * ncomp
    partner = {"sub": 1 - sub}
    others = [partner, {"lat": 1 - lat}, {"lat": 1 - lat, "sub": 1 - sub}]

    small = [pltpu.make_async_copy(src, dst, i_sem.at[n]) for n, (src, dst) in enumerate((
        (mask_hbm, mask_ref.at[lat, sub]), (nb_hbm, nb_ref.at[lat, sub]),
        (steps_hbm, steps_ref), (cour_hbm, cour_ref)))]
    loads = []
    for r in range(2):
        cols = slice(r * NLON, (r + 1) * NLON)
        loads.append(pltpu.make_async_copy(
            spec_ref.at[:, 1 - sub, :, cols], oth_ref.at[pl.ds(0, groups), r], l_sem.at[r]))
        loads.append(pltpu.make_async_copy(
            spec_ref.at[:, sub, :, cols], full_ref.at[pl.ds(0, groups), 2 * sub + r], l_sem.at[2 + r]))
    for load in (small[0], *loads, *small[1:]):
        load.start()
    own_half = pl.ds(pl.multiple_of(sub * (total // 2), 16), total // 2)
    load_w = pltpu.make_async_copy(op_ref, w_ref.at[own_half], w_sem)

    barrier = pltpu.get_barrier_semaphore()
    peers = list(others)
    for d in range(1, ncomp):
        z = lax.rem(me + d, ncomp)
        peers += [{"comp": z}, {"comp": z, "sub": 1 - sub}]
    for peer in peers:
        pl.semaphore_signal(barrier, inc=1, device_id=peer, device_id_type=MESH)

    a = lax.broadcasted_iota(jnp.int32, (NLON, NLON), 0)
    b = lax.broadcasted_iota(jnp.int32, (NLON, NLON), 1)
    split = lambda c: jnp.where(c < lanes, 2 * c, 2 * (c - lanes) + 1)
    perm_ref[0] = (a == split(b)).astype(F32).astype(BF16)
    perm_ref[1] = (b == split(a)).astype(F32).astype(BF16)

    near_ty = lat
    far_ty = 1 - lat
    n0 = lax.rem(lat + me * groups, 2)
    f0 = 1 - n0
    for q, ty in enumerate((near_ty, far_ty)):
        d = lax.broadcasted_iota(jnp.int32, (16, lanes), 0) + 16 * (2 * ty + sub)
        angle = (d.astype(F32) + 0.5) * np.float32(2.0 * math.pi / ND)
        ang_ref[q, 0] = jnp.abs(jnp.cos(angle))
        ang_ref[q, 1] = jnp.abs(jnp.sin(angle))

    def point_copies(n):
        return [pltpu.make_async_remote_copy(
            src_ref=ref.at[lat, sub], dst_ref=ref.at[lat, sub], send_sem=c_send.at[n, m],
            recv_sem=c_recv.at[n, m], device_id=others[n], device_id_type=MESH)
            for m, ref in enumerate((mask_ref, nb_ref))]

    def raw_copies():
        return [pltpu.make_async_remote_copy(
            src_ref=spec_ref.at[:, 1 - sub, :, r * NLON:(r + 1) * NLON],
            dst_ref=full_ref.at[pl.ds(0, groups), 2 * sub + r],
            send_sem=r_send.at[r], recv_sem=r_recv.at[r], device_id=partner, device_id_type=MESH)
            for r in range(2)]

    def raw_waits():
        for r in range(2):
            pltpu.make_async_remote_copy(
                src_ref=spec_ref.at[:, 1 - sub, :, r * NLON:(r + 1) * NLON],
                dst_ref=full_ref.at[pl.ds(0, groups), 2 * (1 - sub) + r],
                send_sem=r_send.at[r], recv_sem=r_recv.at[r],
                device_id=partner, device_id_type=MESH).wait_recv()

    small[0].wait()
    small[1].wait()
    sea = mask_ref[lat, sub].astype(F32)
    for load in loads:
        load.wait()
    sea_rows = [jnp.broadcast_to(sea[:, r * NLON:(r + 1) * NLON], (16, NLON)) for r in range(2)]

    def convert(k, carry):
        j = n0 + 2 * k
        for r in range(2):
            mine = full_ref[j, 2 * sub + r] * sea_rows[r]
            other = oth_ref[j, r] * sea_rows[r]
            hsend_ref[k, sub, r] = mine.astype(BF16)
            hsend_ref[k, 1 - sub, r] = other.astype(BF16)
        return carry

    lax.fori_loop(0, kmax, convert, 0)
    pl.semaphore_wait(barrier, len(peers))
    def halo_copy(k, p):
        return pltpu.make_async_remote_copy(
            src_ref=hsend_ref.at[k, p], dst_ref=halo_ref.at[k, pl.ds(2 * sub, 2)],
            send_sem=h_send.at[k, p], recv_sem=h_recv.at[k, sub],
            device_id={"lat": 1 - lat, "sub": p}, device_id_type=MESH)

    def halo_wait(k, s):
        pltpu.make_async_remote_copy(
            src_ref=hsend_ref.at[k, s], dst_ref=halo_ref.at[k, pl.ds(2 * s, 2)],
            send_sem=h_send.at[k, s], recv_sem=h_recv.at[k, s],
            device_id={"lat": 1 - lat, "sub": s}, device_id_type=MESH).wait_recv()

    def give_w():
        return pltpu.make_async_remote_copy(
            src_ref=op_ref, dst_ref=w_ref.at[own_half], send_sem=g_send, recv_sem=g_recv,
            device_id=partner, device_id_type=MESH)

    def take_w():
        other_half = pl.ds(pl.multiple_of((1 - sub) * (total // 2), 16), total // 2)
        return pltpu.make_async_remote_copy(
            src_ref=op_ref, dst_ref=w_ref.at[other_half], send_sem=g_send, recv_sem=g_recv,
            device_id=partner, device_id_type=MESH)

    def send_halo(k, carry):
        @pl.when(n0 + 2 * k < groups)
        def _():
            for p in range(2):
                halo_copy(k, p).start()
        return carry

    for copy in point_copies(0):
        copy.start()
    lax.fori_loop(0, AHEAD, send_halo, 0)
    for copy in (*raw_copies(), *point_copies(1), *point_copies(2)):
        copy.start()
    lax.fori_loop(AHEAD, kmax, send_halo, 0)
    load_w.start()
    give_w().start()
    for load in small[2:]:
        load.wait()

    points = mask_ref.shape[-1]
    lane = lax.broadcasted_iota(jnp.int32, (1, points), 1)
    column = lane & (NLON - 1)
    index = lax.broadcasted_iota(jnp.int32, (8, points), 0)

    def decode(chip):
        for s in range(2):
            nb = nb_ref[chip, s]
            west = (column - nb[0:1, :]) & (NLON - 1)
            east = (nb[1:2, :] - column) & (NLON - 1)
            moves = [((nb[k:k + 1, :] - column + 1) & (NLON - 1)) - 1 for k in (2, 3)]
            codes = jnp.zeros((8, points), F32)
            for k, entry in enumerate((west, east, *moves, mask_ref[chip, s])):
                codes = jnp.where(index == k, jnp.broadcast_to(entry.astype(F32), (8, points)), codes)
            for r in range(2):
                part = codes[:, r * NLON:(r + 1) * NLON].astype(BF16)
                both = jnp.dot(part, perm_ref[0], preferred_element_type=F32)
                for k in range(5):
                    code_ref[chip, 2 * s + r, k] = jnp.broadcast_to(both[k:k + 1, :], (8, NLON))

    side = lax.div(me, 2)

    def target(i):
        near = me + 1 - 2 * lax.rem(me, 2)
        return jnp.where(i == 0, 3 - 3 * side, jnp.where(i == 1, 2 - side, jnp.where(i == 2, near, me)))

    def chunk_copy(h, j, i):
        to = target(i)
        return pltpu.make_async_remote_copy(
            src_ref=away_ref.at[h, to, j], dst_ref=x_ref.at[0, me * groups + j, sub, :, 0:lanes],
            send_sem=a_send.at[h, i], recv_sem=a_recv.at[me, sub],
            device_id={"comp": to, "sub": h}, device_id_type=MESH)

    def whole_copy(h, i):
        to = target(i)
        return pltpu.make_async_remote_copy(
            src_ref=away_ref.at[h, to, pl.ds(0, groups)],
            dst_ref=x_ref.at[0, pl.ds(me * groups, groups), sub, :, 0:lanes],
            send_sem=a_send.at[h, i], recv_sem=a_recv.at[me, sub],
            device_id={"comp": to, "sub": h}, device_id_type=MESH)

    def whole_wait(z, s):
        pltpu.make_async_remote_copy(
            src_ref=away_ref.at[0, z, pl.ds(0, groups)],
            dst_ref=x_ref.at[0, pl.ds(z * groups, groups), s, :, 0:lanes],
            send_sem=a_send.at[0, 0], recv_sem=a_recv.at[z, s],
            device_id={"comp": z, "sub": s}, device_id_type=MESH).wait_recv()

    def pick(ty, i):
        return ty * 3 + (1 - 2 * ty) * i

    def separate(x):
        high = x.astype(BF16)
        low = (x - high.astype(F32)).astype(BF16)
        return high, low

    def propagate(ks, far, to_east):
        ty = far_ty if far else near_ty
        js = [(f0 if far else n0) + 2 * k for k in ks]
        vert = 2 + ty
        lowest = 0 if far else 4

        def code(q, k, half):
            chip = lat if q >= 4 else 1 - lat
            part = code_ref[chip, pick(ty, q % 4), k, :, half * lanes:(half + 1) * lanes]
            return jnp.concatenate([part, part], axis=0)

        raw = jnp.concatenate([full_ref[j, pick(ty, i)] for j in js for i in range(4)], axis=0)
        high, low = separate(raw)
        mixed = (jnp.dot(high, perm_ref[0], preferred_element_type=F32)
                 + jnp.dot(low, perm_ref[0], preferred_element_type=F32))
        if far:
            edge = jnp.concatenate([halo_ref[k, pick(ty, i)] for k in ks for i in range(4)], axis=0)
            edge = jnp.dot(edge, perm_ref[0], preferred_element_type=F32)
        cells = []
        weights = []
        for n, j in enumerate(js):
            values = [None] * 8
            for i in range(4):
                rows = slice((n * 4 + i) * 16, (n * 4 + i + 1) * 16)
                values[4 + i] = tuple(
                    mixed[rows, half * lanes:(half + 1) * lanes] * code(4 + i, 4, half)
                    for half in range(2))
                if far:
                    values[i] = tuple(edge[rows, half * lanes:(half + 1) * lanes] for half in range(2))
            cells.append(values)
            freq = jnp.minimum(lax.div(me * bins + j * 32, ND), steps_ref.shape[0] - 1)
            weights.append((steps_ref[freq], cour_ref[freq]))
        abs_cos, abs_sin = ang_ref[int(far), 0], ang_ref[int(far), 1]
        ahead, behind = (1, lanes - 1)
        for t in range(MAXSTEPS):
            slots = [q for q in range(7, lowest - 1, -1) if q >= 4 or t <= q + 1]
            for n, (steps, speed) in enumerate(weights):
                live = jnp.where(t < steps, speed, 0.0)
                wx = live * abs_cos
                wy = live * abs_sin
                keep = 1.0 - wx - wy
                values = cells[n]
                fresh = list(values)
                turned = {}

                def turn(q, half, shift):
                    key = (q, half, shift)
                    if key not in turned:
                        turned[key] = pltpu.roll(values[q][half], shift, 1)
                    return turned[key]

                def left(q):
                    return turn(q, 1, ahead), values[q][0]

                def right(q):
                    return values[q][1], turn(q, 0, behind)

                for q in slots:
                    shift = ahead if to_east else behind
                    one = left(q) if to_east else right(q)
                    lon_code = 0 if to_east else 1
                    new = []
                    for half in range(2):
                        x = values[q][half]
                        lon = jnp.where(code(q, lon_code, half) == 1.0, one[half], turn(q, half, shift))
                        if q == lowest:
                            up = x
                        else:
                            move = code(q, vert, half)
                            up = jnp.where(move == -1.0, left(q - 1)[half],
                                           jnp.where(move == 1.0, right(q - 1)[half], values[q - 1][half]))
                        new.append(code(q, 4, half) * (keep * x + wx * lon + wy * up))
                    fresh[q] = tuple(new)
                cells[n] = fresh
        for n, j in enumerate(js):
            for i in range(4):
                r = pick(ty, i)
                for half in range(2):
                    value = cells[n][4 + i][half]
                    pout_ref[j, r, :, half * lanes:(half + 1) * lanes] = value
                    away_ref[lax.div(r, 2), 2 * lax.rem(r, 2) + half, j] = value.astype(BF16)
        for n, j in enumerate(js):
            @pl.when(j < groups)
            def _():
                for i in range(ncomp - 1):
                    chunk_copy(0, j, i).start()

    straight = sub == lat
    for copy in point_copies(0):
        copy.wait_recv()
    decode(lat)
    raw_waits()

    def near_body(g, carry):
        ks = [g * NEAR + n for n in range(NEAR)]

        @pl.when(straight)
        def _():
            propagate(ks, False, True)

        @pl.when(jnp.logical_not(straight))
        def _():
            propagate(ks, False, False)
        return carry

    lax.fori_loop(0, kmax // NEAR, near_body, 0)
    for n in (1, 2):
        for copy in point_copies(n):
            copy.wait_recv()
    decode(1 - lat)

    def far_body(g, carry):
        ks = [g * FAR + n for n in range(FAR)]
        for k in ks:
            @pl.when(f0 + 2 * k < groups)
            def _():
                for s in range(2):
                    halo_wait(k, s)

        @pl.when(straight)
        def _():
            propagate(ks, True, False)

        @pl.when(jnp.logical_not(straight))
        def _():
            propagate(ks, True, True)

        for k in ks:
            @pl.when((n0 + 2 * k < groups) & (k < NEAR))
            def _():
                for i in range(ncomp - 1):
                    chunk_copy(1, n0 + 2 * k, i).start()
        return carry

    lax.fori_loop(0, kmax // FAR, far_body, 0)

    own_copy = pltpu.make_async_copy(
        away_ref.at[sub, me, pl.ds(0, groups)], x_ref.at[0, pl.ds(me * groups, groups), sub, :, 0:lanes], o_sem.at[0])

    def cross_copy():
        return pltpu.make_async_remote_copy(
            src_ref=away_ref.at[1 - sub, me, pl.ds(0, groups)],
            dst_ref=x_ref.at[0, pl.ds(me * groups, groups), sub, :, 0:lanes],
            send_sem=a_send.at[0, ncomp - 1], recv_sem=a_recv.at[me, sub],
            device_id=partner, device_id_type=MESH)

    def prop_copy():
        return pltpu.make_async_remote_copy(
            src_ref=pout_ref.at[pl.ds(0, groups), pl.ds(2 * (1 - sub), 2)],
            dst_ref=pin_ref, send_sem=p_send, recv_sem=p_recv,
            device_id=partner, device_id_type=MESH)

    own_copy.start()
    cross_copy().start()

    def send_rest(k, carry):
        @pl.when(f0 + 2 * k < groups)
        def _():
            for i in range(ncomp - 1):
                chunk_copy(1, f0 + 2 * k, i).start()
        return carry

    def send_near(k, carry):
        @pl.when(n0 + 2 * k < groups)
        def _():
            for i in range(ncomp - 1):
                chunk_copy(1, n0 + 2 * k, i).start()
        return carry

    lax.fori_loop(0, kmax, send_rest, 0)
    lax.fori_loop(NEAR, kmax, send_near, 0)

    wide = (sub == 1) & (lax.div(me + 1, 2) == 1)

    def twin_copy(block, to):
        return pltpu.make_async_remote_copy(
            src_ref=away_ref.at[1, block, pl.ds(0, groups)],
            dst_ref=x_ref.at[0, pl.ds(me * groups, groups), sub, :, lanes:2 * lanes],
            send_sem=t_send.at[block], recv_sem=t_recv.at[me, sub],
            device_id={"comp": to, "sub": 1}, device_id_type=MESH)

    def twin_local(block):
        return pltpu.make_async_copy(
            away_ref.at[1, block, pl.ds(0, groups)],
            x_ref.at[0, pl.ds(me * groups, groups), sub, :, lanes:2 * lanes], o_sem.at[1])

    def twin_wait(z, s):
        pltpu.make_async_remote_copy(
            src_ref=away_ref.at[1, 0, pl.ds(0, groups)],
            dst_ref=x_ref.at[0, pl.ds(z * groups, groups), s, :, lanes:2 * lanes],
            send_sem=t_send.at[0], recv_sem=t_recv.at[z, s],
            device_id={"comp": z, "sub": s}, device_id_type=MESH).wait_recv()

    def twin_here(to):
        return (me == to) & (sub == 1)

    for block, to in ((1, 2), (2, 1)):
        @pl.when(jnp.logical_not(twin_here(to)))
        def _():
            twin_copy(block, to).start()

        @pl.when(twin_here(to))
        def _():
            twin_local(block).start()
    prop_copy().start()

    piece = bins // PIECES

    def home_copy(source, block, to, start, size):
        span = pl.ds(pl.multiple_of(start, 16), size)
        return pltpu.make_async_remote_copy(
            src_ref=inc_ref.at[source, span], dst_ref=home_ref.at[block, span],
            send_sem=b_send.at[source], recv_sem=b_recv.at[block],
            device_id={"comp": to}, device_id_type=MESH)

    early = (2 * bins) // 128 * 128
    late = total - early

    once = 1 + lax.div(me, ncomp)

    def integrate(width):
        def partial(start, span, use):
            def one(i, carry):
                rows = pl.ds(pl.multiple_of(i * total, 16), total)
                field = x_ref[0, pl.ds(lax.div(start, 32), span // 32), :, :, 0:width].reshape(span, width)
                cols = pl.ds(pl.multiple_of(start, 128), span)
                use(rows, jnp.dot(w_ref[rows, cols], field, preferred_element_type=F32))
                return carry

            lax.fori_loop(0, once, one, 0)

        def begin(rows, driving):
            state_ref[rows, 0:width] = driving

        def first_step(rows, driving):
            start = x_ref[0, :, :, :, 0:width].reshape(total, width).astype(F32)
            now = start + STEP_SIZE * start * (state_ref[rows, 0:width] + driving)
            start_ref[rows, 0:width] = start
            state_ref[rows, 0:width] = now
            x_ref[1, :, :, :, 0:width] = now.astype(BF16).reshape(ncomp * groups, 2, 16, width)

        def advance(step, carry):
            field = x_ref[lax.rem(step, 2), :, :, :, 0:width].reshape(total, width)
            driving = jnp.dot(w_ref[...], field, preferred_element_type=F32)
            now = state_ref[:, 0:width]
            now = now + STEP_SIZE * now * driving
            state_ref[:, 0:width] = now
            x_ref[lax.rem(step + 1, 2), :, :, :, 0:width] = now.astype(BF16).reshape(
                ncomp * groups, 2, 16, width)
            return carry

        def last(m, start):
            rows = pl.ds(pl.multiple_of(m * bins + start, 16), piece)
            field = x_ref[(SRC_STEPS - 1) % 2, :, :, :, 0:width].reshape(total, width)
            driving = jnp.dot(w_ref[rows, :], field, preferred_element_type=F32)
            now = state_ref[rows, 0:width]
            now = now + STEP_SIZE * now * driving
            return (now - start_ref[rows, 0:width]).astype(BF16)

        def finish(n, carry):
            m = target(lax.div(n, PIECES))
            start = lax.rem(n, PIECES) * piece
            span = pl.ds(pl.multiple_of(start, 16), piece)
            gain = last(m, start)

            @pl.when(m == me)
            def _():
                home_ref[me, span] = gain

            @pl.when(m != me)
            def _():
                inc_ref[m, span] = gain
                home_copy(m, me, m, start, piece).start()
            return carry

        def finish_wide(n, carry):
            m = target(lax.div(n, PIECES))
            start = lax.rem(n, PIECES) * piece
            span = pl.ds(pl.multiple_of(start, 16), piece)
            gain = last(m, start)
            blocks = ((me, gain[:, 0:lanes]), (3 - me, gain[:, lanes:2 * lanes]))

            @pl.when(m == me)
            def _():
                for block, part in blocks:
                    home_ref[block, span] = part

            @pl.when(m != me)
            def _():
                for source, (block, part) in enumerate(blocks):
                    inc_ref[source, span] = part
                    home_copy(source, block, m, start, piece).start()
            return carry

        both = width > lanes
        whole_wait(me, 1 - sub)
        for s in range(2):
            whole_wait(target(2), s)
        if both:
            twin_local(3 - me).wait()
            twin_wait(me, 0)
            for s in range(2):
                twin_wait(target(2), s)
        partial(side * late, early, begin)
        for i in (1, 0):
            for s in range(2):
                whole_wait(target(i), s)
                if both:
                    twin_wait(target(i), s)
        partial((1 - side) * early, late, first_step)
        lax.fori_loop(1, SRC_STEPS - 1, advance, 0)
        if both:
            lax.fori_loop((ncomp - 2) * PIECES, ncomp * PIECES, finish_wide, 0)
        else:
            lax.fori_loop(0, ncomp * PIECES, finish, 0)

    sea_wide = [jnp.broadcast_to(sea[:, r * NLON:(r + 1) * NLON], (16, NLON)) for r in range(2)]

    def restore(g, carry):
        js = [g * BACK + n for n in range(BACK)]
        parts = [ref for j in js for ref in (
            pout_ref[j, 2 * sub], pout_ref[j, 2 * sub + 1], pin_ref[j, 0], pin_ref[j, 1])]
        high, low = separate(jnp.concatenate(parts, axis=0))
        plain = (jnp.dot(high, perm_ref[1], preferred_element_type=F32)
                 + jnp.dot(low, perm_ref[1], preferred_element_type=F32))
        for n in range(4 * BACK):
            p = sub if n % 4 < 2 else 1 - sub
            rows = pl.ds(pl.multiple_of((2 * js[n // 4] + p) * 16, 16), 16)
            r = n % 2
            out_ref[rows, r * NLON:(r + 1) * NLON] = sea_wide[r] * plain[n * 16:(n + 1) * 16, :]
        return carry

    def restore_all():
        prop_copy().wait_recv()
        lax.fori_loop(0, groups // BACK, restore, 0)

    pl.when(sub == 1)(restore_all)
    load_w.wait()
    take_w().wait_recv()
    own_copy.wait()
    @pl.when(wide)
    def _():
        integrate(2 * lanes)

    @pl.when(jnp.logical_not(wide))
    def _():
        integrate(lanes)

    pl.when(sub == 0)(restore_all)
    for i in (3, 2, 0, 1):
        z = target(i)

        def land():
            pltpu.make_async_remote_copy(
                src_ref=inc_ref.at[z], dst_ref=home_ref.at[z],
                send_sem=b_send.at[z], recv_sem=b_recv.at[z],
                device_id={"comp": z}, device_id_type=MESH).wait_recv()

        if i < 3:
            pl.when(jnp.logical_not(wide & (z == 3 - me)))(land)
        r = lax.div(z, 2)
        half = lax.rem(z, 2)
        cols = pl.ds(pl.multiple_of(r * NLON, NLON), NLON)
        spread = perm_ref[1, pl.ds(pl.multiple_of(half * lanes, lanes), lanes), :]
        sea_row = jnp.where(r == 0, sea_wide[0][0:8], sea_wide[1][0:8])
        back = jnp.dot(home_ref[z], spread, preferred_element_type=F32)
        back = back.reshape(bins // 8, 8, NLON) * sea_row[None]
        out_ref[:, cols] = out_ref[:, cols] + back.reshape(bins, NLON)

    for n in range(3):
        for copy in point_copies(n):
            copy.wait_send()
    for copy in raw_copies():
        copy.wait_send()

    def halo_left(k, carry):
        @pl.when(n0 + 2 * k < groups)
        def _():
            for p in range(2):
                halo_copy(k, p).wait_send()
        return carry

    lax.fori_loop(0, kmax, halo_left, 0)
    prop_copy().wait_send()
    cross_copy().wait_send()
    give_w().wait_send()
    for i in range(ncomp - 1):
        for h in range(2):
            whole_copy(h, i).wait_send()

        @pl.when(jnp.logical_not(wide))
        def _():
            m = target(i)
            home_copy(m, me, m, 0, bins).wait_send()

    @pl.when(wide)
    def _():
        for source, block in enumerate((me, 3 - me)):
            home_copy(source, block, target(2), 0, bins).wait_send()

    for block, to in ((1, 2), (2, 1)):
        @pl.when(jnp.logical_not(twin_here(to)))
        def _():
            twin_copy(block, to).wait_send()


def write_kernel(src_ref, dst_ref, sems):
    pieces = sems.shape[0]
    rows = src_ref.shape[0] // pieces
    copies = [pltpu.make_async_copy(
        src_ref.at[pl.ds(i * rows, rows)], dst_ref.at[pl.ds(i * rows, rows)], sems.at[i])
        for i in range(pieces)]
    for copy in copies:
        copy.start()
    for copy in copies:
        copy.wait()


def fast_device(ncomp, spectrum, sea_mask, neighbours, substeps, courant, source_operator):
    bins, points = spectrum.shape
    groups = bins // 32
    kmax = (groups + 1) // 2
    lanes = NLON // 2
    total = bins * ncomp
    vmem = pl.BlockSpec(memory_space=pltpu.VMEM)
    hbm = pl.BlockSpec(memory_space=pltpu.HBM)
    dma = pltpu.SemaphoreType.DMA
    result = pl.pallas_call(
        functools.partial(fast_kernel, ncomp),
        out_shape=pltpu.VMEM((bins, points), F32),
        in_specs=[hbm] * 6,
        out_specs=vmem,
        scratch_shapes=[
            pltpu.VMEM((2, 2, 1, points), jnp.int32),
            pltpu.VMEM((2, 2, 4, points), jnp.int32),
            pltpu.SMEM(substeps.shape, jnp.int32),
            pltpu.SMEM(courant.shape, F32),
            pltpu.VMEM((total, total), BF16),
            pltpu.VMEM((2 * kmax, 4, 16, NLON), F32),
            pltpu.VMEM((2 * kmax, 2, 16, NLON), F32),
            pltpu.VMEM((kmax, 2, 2, 16, NLON), BF16),
            pltpu.VMEM((kmax, 4, 16, NLON), BF16),
            pltpu.VMEM((2, 4, 5, 8, NLON), F32),
            pltpu.VMEM((2, 2, 16, lanes), F32),
            pltpu.VMEM((2, NLON, NLON), BF16),
            pltpu.VMEM((2 * kmax, 4, 16, NLON), F32),
            pltpu.VMEM((groups, 2, 16, NLON), F32),
            pltpu.VMEM((2, ncomp, 2 * kmax, 16, lanes), BF16),
            pltpu.VMEM((2, ncomp * groups, 2, 16, 2 * lanes), BF16),
            pltpu.VMEM((total, 2 * lanes), F32),
            pltpu.VMEM((total, 2 * lanes), F32),
            pltpu.VMEM((ncomp, bins, lanes), BF16),
            pltpu.VMEM((ncomp, bins, lanes), BF16),
            dma((4,)), dma((4,)), dma, dma((3, 2)), dma((3, 2)), dma((2,)), dma((2,)), dma, dma,
            dma((kmax, 2)), dma((kmax, 2)), dma((2, ncomp)), dma((ncomp, 2)), dma((ncomp,)), dma((ncomp, 2)),
            dma((2,)), dma, dma,
            dma((ncomp,)), dma((ncomp,)),
        ],
        compiler_params=pltpu.CompilerParams(
            collective_id=1, has_side_effects=True, vmem_limit_bytes=60 * 1024 * 1024),
    )(spectrum.reshape(groups, 2, 16, points), sea_mask.reshape(1, points), neighbours, substeps, courant,
      source_operator)
    return pl.pallas_call(
        write_kernel,
        out_shape=jax.ShapeDtypeStruct((bins, points), F32),
        in_specs=[vmem],
        out_specs=hbm,
        scratch_shapes=[dma((4,))],
        compiler_params=pltpu.CompilerParams(vmem_limit_bytes=4 * 1024 * 1024),
    )(result)


def solution(mesh):
    nlat, ncomp = mesh.shape["lat"], mesh.shape["comp"]

    def per_device(spectrum, sea_mask, neighbours, substeps, courant, source_operator):
        bins, points = spectrum.shape
        even = bins % 32 == 0 and (bins // 32 + 1) // 2 % NEAR == 0 and bins // 32 % BACK == 0
        if nlat == 2 and ncomp == 4 and points == 2 * NLON and even:
            return fast_device(ncomp, spectrum, sea_mask, neighbours, substeps, courant, source_operator)
        size = 16 if bins % 16 == 0 else 8
        chunks = bins // size
        group = 5 if chunks % 5 == 0 else 1
        share = points // ncomp
        total = bins * ncomp
        angles = (np.arange(ND, dtype=np.float32) + np.float32(0.5)) * np.float32(2.0 * math.pi / ND)
        spread = lambda v: jnp.asarray(
            np.broadcast_to(np.abs(v).astype(np.float32)[:, None], (ND, NLON)).reshape(ND // 8, 8, NLON))
        vmem = pl.BlockSpec(memory_space=pltpu.VMEM)
        smem = pl.BlockSpec(memory_space=pltpu.SMEM)
        kinds = 3 if nlat == 2 else 4
        return pl.pallas_call(
            functools.partial(kernel, nlat, ncomp, group),
            out_shape=jax.ShapeDtypeStruct((bins, points), F32),
            in_specs=[vmem, vmem, vmem, smem, smem, vmem, vmem, pl.BlockSpec(memory_space=pl.ANY)],
            out_specs=vmem,
            scratch_shapes=[
                pltpu.VMEM((total, total), BF16),
                pltpu.VMEM((chunks + 2, size, points), BF16),
                pltpu.VMEM((3, chunks + 2, size, points), BF16),
                pltpu.VMEM((2, SLOTS, 4, 8, NLON), F32),
                pltpu.VMEM((chunks, size, points), F32),
                pltpu.VMEM((ncomp, chunks, size, share), BF16),
                pltpu.VMEM((ncomp, chunks, size, share), BF16),
                pltpu.VMEM((total, share), F32),
                pltpu.VMEM((total, share), F32),
                pltpu.VMEM((2, total, share), BF16),
                pltpu.VMEM((ncomp, bins, share), BF16),
                pltpu.VMEM((ncomp, bins, share), BF16),
                pltpu.SemaphoreType.DMA((kinds, chunks + 2)),
                pltpu.SemaphoreType.DMA((kinds, chunks + 2)),
                pltpu.SemaphoreType.DMA,
                pltpu.SemaphoreType.DMA,
                pltpu.SemaphoreType.DMA,
                pltpu.SemaphoreType.DMA((ncomp,)),
                pltpu.SemaphoreType.DMA((ncomp,)),
                pltpu.SemaphoreType.DMA((ncomp,)),
                pltpu.SemaphoreType.DMA((ncomp,)),
            ],
            compiler_params=pltpu.CompilerParams(
                collective_id=0, has_side_effects=True, vmem_limit_bytes=56 * 1024 * 1024),
        )(spectrum, sea_mask.reshape(1, points), neighbours, substeps, courant,
          spread(np.cos(angles)), spread(np.sin(angles)), source_operator)

    placed = (
        P("comp", ("members", "lat", "sub")),
        P(("members", "lat", "sub")),
        P(None, ("members", "lat", "sub")),
        P(),
        P(),
        P("sub", None),
    )
    return jax.shard_map(
        per_device,
        mesh=mesh,
        in_specs=placed,
        out_specs=P("comp", ("members", "lat", "sub")),
        check_vma=False,
    )
```

```python
import functools
import math

import jax
import jax.numpy as jnp
import numpy as np
from jax import lax
from jax.experimental import pallas as pl
from jax.experimental.pallas import tpu as pltpu
from jax.sharding import PartitionSpec as P

NF = 30
ND = 64
NLON = 256
MAXSTEPS = 6
SRC_STEPS = 4
STEP_SIZE = 0.1
MESH = pl.DeviceIdType.MESH
HALF = ND // 2
TILES = 4
SLOTS = 8
NEAR = 4
FAR = 2
BACK = 5
AHEAD = 2
PIECES = 2
F32 = jnp.float32
BF16 = jnp.bfloat16


def kernel(
    nlat, ncomp, group, spec_ref, mask_ref, nb_ref, steps_ref, cour_ref, cos_ref, sin_ref, op_ref,
    out_ref, w_ref, own_ref, halo_ref, code_ref, prop_ref, away_ref, got_ref, start_ref, state_ref,
    low_ref, inc_ref, home_ref,
    h_send, h_recv, w_send, w_recv, w_local, a_send, a_recv, b_send, b_recv,
):
    lat = lax.axis_index("lat")
    sub = lax.axis_index("sub")
    me = lax.axis_index("comp")
    bins, points = spec_ref.shape
    chunks, size = prop_ref.shape[0], prop_ref.shape[1]
    planes = size // 8
    share = points // ncomp
    total = bins * ncomp
    half_rows = total // 2
    first = me * bins
    last_lat = nlat - 1
    partner = {"sub": 1 - sub}

    barrier = pltpu.get_barrier_semaphore()
    peers = [partner]
    if nlat == 2:
        peers.append({"lat": 1 - lat})
    else:
        for move in (1, -1):
            peers.append({"lat": lax.rem(lat + move + nlat, nlat)})
            peers.append({"lat": lax.rem(lat + 2 * move + nlat, nlat), "sub": 1 - sub})
    for j in range(1, ncomp):
        peers.append({"comp": lax.rem(me + j, ncomp)})
    for peer in peers:
        pl.semaphore_signal(barrier, inc=1, device_id=peer, device_id_type=MESH)

    own_half = pl.ds(pl.multiple_of(sub * half_rows, 16), half_rows)
    load_w = pltpu.make_async_copy(op_ref, w_ref.at[own_half], w_local)
    load_w.start()

    lane = lax.broadcasted_iota(jnp.int32, (1, points), 1)
    column = lane & (NLON - 1)
    position = (lat * 2 + sub) * points + lane
    sea = mask_ref[...].astype(F32)
    west = (column - nb_ref[0:1, :]) & (NLON - 1)
    east = (nb_ref[1:2, :] - column) & (NLON - 1)

    def vertical(index_row):
        moved = ((index_row - column + 1) & (NLON - 1)) - 1
        return jnp.where(index_row == position, 2, moved)

    rows = lax.broadcasted_iota(jnp.int32, (size, points), 0)
    codes = jnp.zeros((size, points), F32)
    entries = [west, east, vertical(nb_ref[2:3, :]), vertical(nb_ref[3:4, :])]
    for k, entry in enumerate([e.astype(F32) for e in entries] + [sea]):
        codes = jnp.where(rows == k, jnp.broadcast_to(entry, (size, points)), codes)
    own_ref[0] = codes.astype(BF16)
    own_ref[1] = codes.astype(BF16)

    pl.semaphore_wait(barrier, len(peers))

    def kind(q):
        return lax.rem(lax.div(first + (q - 2) * size, HALF), 2)

    def has_from(ty, far):
        return jnp.where(ty == 0, lat >= far, lat <= last_lat - far)

    def has_to(ty, far):
        return jnp.where(ty == 0, lat <= last_lat - far, lat >= far)

    def pair_copy(q):
        return pltpu.make_async_remote_copy(
            src_ref=own_ref.at[q], dst_ref=halo_ref.at[0, q], send_sem=h_send.at[0, q],
            recv_sem=h_recv.at[0, q], device_id=partner, device_id_type=MESH)

    def side_copy(q, ty):
        to = jnp.clip(lat + 1 - 2 * ty, 0, last_lat)
        return pltpu.make_async_remote_copy(
            src_ref=own_ref.at[q], dst_ref=halo_ref.at[1, q], send_sem=h_send.at[1, q],
            recv_sem=h_recv.at[1, q], device_id={"lat": to}, device_id_type=MESH)

    def hand_copy(q, ty):
        slot = jnp.where(sub == ty, 2, 0)
        return pltpu.make_async_remote_copy(
            src_ref=halo_ref.at[1, q], dst_ref=halo_ref.at[slot, q], send_sem=h_send.at[2, q],
            recv_sem=h_recv.at[2, q], device_id=partner, device_id_type=MESH)

    def far_copy(q, ty):
        to = jnp.clip(lat + 2 - 4 * ty, 0, last_lat)
        return pltpu.make_async_remote_copy(
            src_ref=own_ref.at[q], dst_ref=halo_ref.at[2, q], send_sem=h_send.at[3, q],
            recv_sem=h_recv.at[3, q], device_id={"lat": to, "sub": 1 - sub}, device_id_type=MESH)

    def send_own(q, ty):
        @pl.when(has_to(ty, 1))
        def _():
            side_copy(q, ty).start()

        @pl.when(sub == ty)
        def _():
            pair_copy(q).start()

        if nlat > 2:
            @pl.when((sub != ty) & has_to(ty, 2))
            def _():
                far_copy(q, ty).start()

    def hand_on(q, ty):
        @pl.when(has_from(ty, 1))
        def _():
            side_copy(q, ty).wait_recv()
            hand_copy(q, ty).start()

    def arrive(q, ty):
        @pl.when(has_from(ty, 1))
        def _():
            hand_copy(q, ty).wait_recv()

        @pl.when(sub != ty)
        def _():
            pair_copy(q).wait_recv()

        if nlat > 2:
            @pl.when((sub == ty) & has_from(ty, 2))
            def _():
                far_copy(q, ty).wait_recv()

    def sent(q, ty):
        @pl.when(has_to(ty, 1))
        def _():
            side_copy(q, ty).wait_send()

        @pl.when(sub == ty)
        def _():
            pair_copy(q).wait_send()

        if nlat > 2:
            @pl.when((sub != ty) & has_to(ty, 2))
            def _():
                far_copy(q, ty).wait_send()

        @pl.when(has_from(ty, 1))
        def _():
            hand_copy(q, ty).wait_send()

    send_own(0, 0)
    send_own(1, 1)

    def prepare(i, carry):
        chunk = sea * spec_ref[pl.ds(pl.multiple_of(i * size, size), size), :]
        own_ref[i + 2] = chunk.astype(BF16)
        send_own(i + 2, kind(i + 2))
        return carry

    lax.fori_loop(0, chunks, prepare, 0)

    give_w = pltpu.make_async_remote_copy(
        src_ref=op_ref, dst_ref=w_ref.at[own_half], send_sem=w_send, recv_sem=w_recv,
        device_id=partner, device_id_type=MESH)
    give_w.start()

    for q in (0, 1):
        hand_on(q, q)
    ahead = min(6, chunks)
    for q in range(2, 2 + ahead):
        hand_on(q, kind(q))

    for ty in (0, 1):
        arrive(ty, ty)
        for slot in range(SLOTS):
            row = slot % 2 if ty == 0 else 1 - slot % 2
            cols = slice(row * NLON, (row + 1) * NLON)
            if slot < 6:
                part = halo_ref[2 - slot // 2, ty, :, cols].astype(F32)
            else:
                part = own_ref[ty, :, cols].astype(F32)
            for k, source in enumerate((0, 1, 2 + ty, 4)):
                code_ref[ty, slot, k] = jnp.broadcast_to(part[source:source + 1, :], (8, NLON))

    def propagate(i):
        q = i + 2
        ty = kind(q)

        @pl.when(i + ahead < chunks)
        def _():
            hand_on(q + ahead, kind(q + ahead))

        arrive(q, ty)
        bin0 = first + i * size
        freq = lax.div(bin0, ND)
        direction = lax.rem(bin0, ND)
        to_east = jnp.where((direction < ND // 4) | (direction >= 3 * ND // 4), 1, 0)
        steps = steps_ref[freq]
        speed = cour_ref[freq]
        sign = jnp.where(to_east == 1, 1.0, -1.0)
        shift1 = jnp.where(to_east == 1, 1, NLON - 1)
        shift2 = jnp.where(to_east == 1, 2, NLON - 2)
        back1 = NLON - shift1
        d8 = lax.div(direction, 8)
        abs_cos = cos_ref[pl.ds(d8, planes)]
        abs_sin = sin_ref[pl.ds(d8, planes)]

        def lanes(slot):
            row = jnp.where(ty == 0, slot % 2, 1 - slot % 2)
            return pl.ds(pl.multiple_of(row * NLON, NLON), NLON)

        values = []
        for slot in range(SLOTS):
            if slot < 6:
                part = halo_ref[2 - slot // 2, q, :, lanes(slot)].astype(F32)
            else:
                part = spec_ref[pl.ds(pl.multiple_of(i * size, size), size), lanes(slot)]
            part = part.reshape(planes, 8, NLON)
            if slot >= 6:
                part = part * code_ref[ty, slot, 3][None]
            values.append(part)
        for t in range(MAXSTEPS):
            live = jnp.where(t < steps, speed, 0.0)
            wx = live * abs_cos
            wy = live * abs_sin
            keep = 1.0 - wx - wy
            fresh = list(values)
            for slot in range(t + 1, SLOTS):
                x = values[slot]
                below = values[slot - 1]
                near = code_ref[ty, slot, 1 - to_east][None] == 1.0
                vert = code_ref[ty, slot, 2][None] * sign
                lon = jnp.where(near, pltpu.roll(x, shift1, 2), pltpu.roll(x, shift2, 2))
                up = jnp.where(vert == -1.0, pltpu.roll(below, shift1, 2),
                               jnp.where(vert == 1.0, pltpu.roll(below, back1, 2), below))
                up = jnp.where(jnp.abs(vert) == 2.0, x, up)
                fresh[slot] = code_ref[ty, slot, 3][None] * (keep * x + wx * lon + wy * up)
            values = fresh
        for slot in (6, 7):
            prop_ref[i, :, lanes(slot)] = values[slot].reshape(size, NLON)
        whole = prop_ref[i]
        for c in range(ncomp):
            away_ref[c, i] = whole[:, c * share:(c + 1) * share].astype(BF16)

    groups = chunks // group

    def out_copy(j, g):
        to = lax.rem(me + j, ncomp)
        span = pl.ds(g * group, group)
        return pltpu.make_async_remote_copy(
            src_ref=away_ref.at[to, span], dst_ref=got_ref.at[me, span],
            send_sem=a_send.at[j], recv_sem=a_recv.at[j],
            device_id={"comp": to}, device_id_type=MESH)

    def whole_copy(j):
        to = lax.rem(me + j, ncomp)
        return pltpu.make_async_remote_copy(
            src_ref=away_ref.at[to], dst_ref=got_ref.at[me],
            send_sem=a_send.at[j], recv_sem=a_recv.at[j],
            device_id={"comp": to}, device_id_type=MESH)

    def run_group(g, carry):
        def one(i, inner):
            propagate(g * group + i)
            return inner

        lax.fori_loop(0, group, one, 0)
        for j in range(1, ncomp):
            out_copy(j, g).start()
        return carry

    lax.fori_loop(0, groups, run_group, 0)

    for q in (0, 1):
        sent(q, q)

    def drain(q, carry):
        sent(q, kind(q))
        return carry

    lax.fori_loop(2, chunks + 2, drain, 0)
    got_ref[me] = away_ref[me]
    load_w.wait()
    give_w.wait()

    for j in range(1, ncomp):
        whole_copy(j).wait()
    for c in range(ncomp):
        start_ref[c * bins:(c + 1) * bins, :] = got_ref[c].astype(F32).reshape(bins, share)
    tile = total // TILES
    per_tile = bins // tile if bins >= tile else tile // bins
    for m in range(TILES):
        span = slice(m * tile, (m + 1) * tile)
        low_ref[0, span, :] = start_ref[span, :].astype(BF16)

    def tile_rows(m):
        return pl.ds(pl.multiple_of(m * tile, 16), tile)

    def advance(step, m):
        span = tile_rows(m)
        driving = jnp.dot(w_ref[span, :], low_ref[step % 2], preferred_element_type=F32)
        now = start_ref[span, :] if step == 0 else state_ref[span, :]
        return span, now + STEP_SIZE * now * driving

    for step in range(SRC_STEPS - 1):
        def one_tile(m, carry, step=step):
            span, now = advance(step, m)
            state_ref[span, :] = now
            low_ref[(step + 1) % 2, span, :] = now.astype(BF16)
            return carry

        lax.fori_loop(0, TILES, one_tile, 0)

    def home_copy(j, to):
        return pltpu.make_async_remote_copy(
            src_ref=inc_ref.at[to], dst_ref=home_ref.at[me],
            send_sem=b_send.at[j], recv_sem=b_recv.at[j],
            device_id={"comp": to}, device_id_type=MESH)

    mine = lax.div(me * TILES, ncomp)

    def last_tile(i, carry):
        m = lax.rem(mine + 1 + i, TILES)
        span, now = advance(SRC_STEPS - 1, m)
        gain = now - start_ref[span, :]
        for k in range(per_tile):
            to = m * per_tile + k
            inc_ref[to] = gain[k * bins:(k + 1) * bins, :].astype(BF16)
            j = lax.rem(to - me + ncomp, ncomp)

            @pl.when(to != me)
            def _():
                home_copy(j, to).start()

        return carry

    lax.fori_loop(0, TILES, last_tile, 0)
    home_ref[me] = inc_ref[me]
    for c in range(ncomp):
        j = lax.rem(me - c + ncomp, ncomp)

        @pl.when(me != c)
        def _():
            home_copy(j, lax.rem(me + j, ncomp)).wait()

        cols = slice(c * share, (c + 1) * share)
        before = prop_ref[:, :, cols].reshape(bins, share)
        out_ref[:, cols] = sea[:, cols] * (before + home_ref[c].astype(F32))


def fast_kernel(
    ncomp, spec_ref, mask_hbm, nb_hbm, steps_hbm, cour_hbm, op_ref,
    out_ref, mask_ref, nb_ref, steps_ref, cour_ref, w_ref, full_ref, oth_ref, hsend_ref, halo_ref, code_ref, ang_ref, perm_ref,
    pout_ref, pin_ref, away_ref, x_ref, start_ref, state_ref, inc_ref, home_ref,
    l_sem, i_sem, w_sem, c_send, c_recv, r_send, r_recv, g_send, g_recv, h_send, h_recv,
    a_send, a_recv, t_send, t_recv, o_sem, p_send, p_recv, b_send, b_recv,
):
    lat = lax.axis_index("lat")
    sub = lax.axis_index("sub")
    me = lax.axis_index("comp")
    groups = spec_ref.shape[0]
    bins = groups * 2 * 16
    kmax = halo_ref.shape[0]
    lanes = NLON // 2
    total = bins * ncomp
    partner = {"sub": 1 - sub}
    others = [partner, {"lat": 1 - lat}, {"lat": 1 - lat, "sub": 1 - sub}]

    small = [pltpu.make_async_copy(src, dst, i_sem.at[n]) for n, (src, dst) in enumerate((
        (mask_hbm, mask_ref.at[lat, sub]), (nb_hbm, nb_ref.at[lat, sub]),
        (steps_hbm, steps_ref), (cour_hbm, cour_ref)))]
    loads = []
    for r in range(2):
        cols = slice(r * NLON, (r + 1) * NLON)
        loads.append(pltpu.make_async_copy(
            spec_ref.at[:, 1 - sub, :, cols], oth_ref.at[pl.ds(0, groups), r], l_sem.at[r]))
        loads.append(pltpu.make_async_copy(
            spec_ref.at[:, sub, :, cols], full_ref.at[pl.ds(0, groups), 2 * sub + r], l_sem.at[2 + r]))
    for load in (small[0], *loads, *small[1:]):
        load.start()
    own_half = pl.ds(pl.multiple_of(sub * (total // 2), 16), total // 2)
    load_w = pltpu.make_async_copy(op_ref, w_ref.at[own_half], w_sem)

    barrier = pltpu.get_barrier_semaphore()
    peers = list(others)
    for d in range(1, ncomp):
        z = lax.rem(me + d, ncomp)
        peers += [{"comp": z}, {"comp": z, "sub": 1 - sub}]
    for peer in peers:
        pl.semaphore_signal(barrier, inc=1, device_id=peer, device_id_type=MESH)

    a = lax.broadcasted_iota(jnp.int32, (NLON, NLON), 0)
    b = lax.broadcasted_iota(jnp.int32, (NLON, NLON), 1)
    split = lambda c: jnp.where(c < lanes, 2 * c, 2 * (c - lanes) + 1)
    perm_ref[0] = (a == split(b)).astype(F32).astype(BF16)
    perm_ref[1] = (b == split(a)).astype(F32).astype(BF16)

    near_ty = lat
    far_ty = 1 - lat
    n0 = lax.rem(lat + me * groups, 2)
    f0 = 1 - n0
    for q, ty in enumerate((near_ty, far_ty)):
        d = lax.broadcasted_iota(jnp.int32, (16, lanes), 0) + 16 * (2 * ty + sub)
        angle = (d.astype(F32) + 0.5) * np.float32(2.0 * math.pi / ND)
        ang_ref[q, 0] = jnp.abs(jnp.cos(angle))
        ang_ref[q, 1] = jnp.abs(jnp.sin(angle))

    def point_copies(n):
        return [pltpu.make_async_remote_copy(
            src_ref=ref.at[lat, sub], dst_ref=ref.at[lat, sub], send_sem=c_send.at[n, m],
            recv_sem=c_recv.at[n, m], device_id=others[n], device_id_type=MESH)
            for m, ref in enumerate((mask_ref, nb_ref))]

    def raw_copies():
        return [pltpu.make_async_remote_copy(
            src_ref=spec_ref.at[:, 1 - sub, :, r * NLON:(r + 1) * NLON],
            dst_ref=full_ref.at[pl.ds(0, groups), 2 * sub + r],
            send_sem=r_send.at[r], recv_sem=r_recv.at[r], device_id=partner, device_id_type=MESH)
            for r in range(2)]

    def raw_waits():
        for r in range(2):
            pltpu.make_async_remote_copy(
                src_ref=spec_ref.at[:, 1 - sub, :, r * NLON:(r + 1) * NLON],
                dst_ref=full_ref.at[pl.ds(0, groups), 2 * (1 - sub) + r],
                send_sem=r_send.at[r], recv_sem=r_recv.at[r],
                device_id=partner, device_id_type=MESH).wait_recv()

    small[0].wait()
    small[1].wait()
    sea = mask_ref[lat, sub].astype(F32)
    for load in loads:
        load.wait()
    sea_rows = [jnp.broadcast_to(sea[:, r * NLON:(r + 1) * NLON], (16, NLON)) for r in range(2)]

    def convert(k, carry):
        j = n0 + 2 * k
        for r in range(2):
            mine = full_ref[j, 2 * sub + r] * sea_rows[r]
            other = oth_ref[j, r] * sea_rows[r]
            hsend_ref[k, sub, r] = mine.astype(BF16)
            hsend_ref[k, 1 - sub, r] = other.astype(BF16)
        return carry

    lax.fori_loop(0, kmax, convert, 0)
    pl.semaphore_wait(barrier, len(peers))
    def halo_copy(k, p):
        return pltpu.make_async_remote_copy(
            src_ref=hsend_ref.at[k, p], dst_ref=halo_ref.at[k, pl.ds(2 * sub, 2)],
            send_sem=h_send.at[k, p], recv_sem=h_recv.at[k, sub],
            device_id={"lat": 1 - lat, "sub": p}, device_id_type=MESH)

    def halo_wait(k, s):
        pltpu.make_async_remote_copy(
            src_ref=hsend_ref.at[k, s], dst_ref=halo_ref.at[k, pl.ds(2 * s, 2)],
            send_sem=h_send.at[k, s], recv_sem=h_recv.at[k, s],
            device_id={"lat": 1 - lat, "sub": s}, device_id_type=MESH).wait_recv()

    def give_w():
        return pltpu.make_async_remote_copy(
            src_ref=op_ref, dst_ref=w_ref.at[own_half], send_sem=g_send, recv_sem=g_recv,
            device_id=partner, device_id_type=MESH)

    def take_w():
        other_half = pl.ds(pl.multiple_of((1 - sub) * (total // 2), 16), total // 2)
        return pltpu.make_async_remote_copy(
            src_ref=op_ref, dst_ref=w_ref.at[other_half], send_sem=g_send, recv_sem=g_recv,
            device_id=partner, device_id_type=MESH)

    def send_halo(k, carry):
        @pl.when(n0 + 2 * k < groups)
        def _():
            for p in range(2):
                halo_copy(k, p).start()
        return carry

    for copy in point_copies(0):
        copy.start()
    lax.fori_loop(0, AHEAD, send_halo, 0)
    for copy in (*raw_copies(), *point_copies(1), *point_copies(2)):
        copy.start()
    lax.fori_loop(AHEAD, kmax, send_halo, 0)
    load_w.start()
    give_w().start()
    for load in small[2:]:
        load.wait()

    points = mask_ref.shape[-1]
    lane = lax.broadcasted_iota(jnp.int32, (1, points), 1)
    column = lane & (NLON - 1)
    index = lax.broadcasted_iota(jnp.int32, (8, points), 0)

    def decode(chip):
        for s in range(2):
            nb = nb_ref[chip, s]
            west = (column - nb[0:1, :]) & (NLON - 1)
            east = (nb[1:2, :] - column) & (NLON - 1)
            moves = [((nb[k:k + 1, :] - column + 1) & (NLON - 1)) - 1 for k in (2, 3)]
            codes = jnp.zeros((8, points), F32)
            for k, entry in enumerate((west, east, *moves, mask_ref[chip, s])):
                codes = jnp.where(index == k, jnp.broadcast_to(entry.astype(F32), (8, points)), codes)
            for r in range(2):
                part = codes[:, r * NLON:(r + 1) * NLON].astype(BF16)
                both = jnp.dot(part, perm_ref[0], preferred_element_type=F32)
                for k in range(5):
                    code_ref[chip, 2 * s + r, k] = jnp.broadcast_to(both[k:k + 1, :], (8, NLON))

    side = lax.div(me, 2)

    def target(i):
        near = me + 1 - 2 * lax.rem(me, 2)
        return jnp.where(i == 0, 3 - 3 * side, jnp.where(i == 1, 2 - side, jnp.where(i == 2, near, me)))

    def chunk_copy(h, j, to):
        return pltpu.make_async_remote_copy(
            src_ref=away_ref.at[h, to, j], dst_ref=x_ref.at[0, me * groups + j, sub, :, 0:lanes],
            send_sem=a_send.at[h, to], recv_sem=a_recv.at[me, sub],
            device_id={"comp": to, "sub": h}, device_id_type=MESH)

    def whole_copy(h, to):
        return pltpu.make_async_remote_copy(
            src_ref=away_ref.at[h, to, pl.ds(0, groups)],
            dst_ref=x_ref.at[0, pl.ds(me * groups, groups), sub, :, 0:lanes],
            send_sem=a_send.at[h, to], recv_sem=a_recv.at[me, sub],
            device_id={"comp": to, "sub": h}, device_id_type=MESH)

    def whole_wait(z, s):
        pltpu.make_async_remote_copy(
            src_ref=away_ref.at[0, z, pl.ds(0, groups)],
            dst_ref=x_ref.at[0, pl.ds(z * groups, groups), s, :, 0:lanes],
            send_sem=a_send.at[0, 0], recv_sem=a_recv.at[z, s],
            device_id={"comp": z, "sub": s}, device_id_type=MESH).wait_recv()

    def pick(ty, i):
        return ty * 3 + (1 - 2 * ty) * i

    def separate(x):
        high = x.astype(BF16)
        low = (x - high.astype(F32)).astype(BF16)
        return high, low

    def propagate(ks, far, to_east):
        ty = far_ty if far else near_ty
        js = [(f0 if far else n0) + 2 * k for k in ks]
        vert = 2 + ty
        lowest = 0 if far else 4

        def code(q, k, half):
            chip = lat if q >= 4 else 1 - lat
            part = code_ref[chip, pick(ty, q % 4), k, :, half * lanes:(half + 1) * lanes]
            return jnp.concatenate([part, part], axis=0)

        raw = jnp.concatenate([full_ref[j, pick(ty, i)] for j in js for i in range(4)], axis=0)
        high, low = separate(raw)
        mixed = (jnp.dot(high, perm_ref[0], preferred_element_type=F32)
                 + jnp.dot(low, perm_ref[0], preferred_element_type=F32))
        if far:
            edge = jnp.concatenate([halo_ref[k, pick(ty, i)] for k in ks for i in range(4)], axis=0)
            edge = jnp.dot(edge, perm_ref[0], preferred_element_type=F32)
        cells = []
        weights = []
        for n, j in enumerate(js):
            values = [None] * 8
            for i in range(4):
                rows = slice((n * 4 + i) * 16, (n * 4 + i + 1) * 16)
                values[4 + i] = tuple(
                    mixed[rows, half * lanes:(half + 1) * lanes] * code(4 + i, 4, half)
                    for half in range(2))
                if far:
                    values[i] = tuple(edge[rows, half * lanes:(half + 1) * lanes] for half in range(2))
            cells.append(values)
            freq = jnp.minimum(lax.div(me * bins + j * 32, ND), steps_ref.shape[0] - 1)
            weights.append((steps_ref[freq], cour_ref[freq]))
        abs_cos, abs_sin = ang_ref[int(far), 0], ang_ref[int(far), 1]
        ahead, behind = (1, lanes - 1)
        for t in range(MAXSTEPS):
            slots = [q for q in range(7, lowest - 1, -1) if q >= 4 or t <= q + 1]
            for n, (steps, speed) in enumerate(weights):
                live = jnp.where(t < steps, speed, 0.0)
                wx = live * abs_cos
                wy = live * abs_sin
                keep = 1.0 - wx - wy
                values = cells[n]
                fresh = list(values)
                turned = {}

                def turn(q, half, shift):
                    key = (q, half, shift)
                    if key not in turned:
                        turned[key] = pltpu.roll(values[q][half], shift, 1)
                    return turned[key]

                def left(q):
                    return turn(q, 1, ahead), values[q][0]

                def right(q):
                    return values[q][1], turn(q, 0, behind)

                for q in slots:
                    shift = ahead if to_east else behind
                    one = left(q) if to_east else right(q)
                    lon_code = 0 if to_east else 1
                    new = []
                    for half in range(2):
                        x = values[q][half]
                        lon = jnp.where(code(q, lon_code, half) == 1.0, one[half], turn(q, half, shift))
                        if q == lowest:
                            up = x
                        else:
                            move = code(q, vert, half)
                            up = jnp.where(move == -1.0, left(q - 1)[half],
                                           jnp.where(move == 1.0, right(q - 1)[half], values[q - 1][half]))
                        new.append(code(q, 4, half) * (keep * x + wx * lon + wy * up))
                    fresh[q] = tuple(new)
                cells[n] = fresh
        for n, j in enumerate(js):
            for i in range(4):
                r = pick(ty, i)
                for half in range(2):
                    value = cells[n][4 + i][half]
                    pout_ref[j, r, :, half * lanes:(half + 1) * lanes] = value
                    away_ref[lax.div(r, 2), 2 * lax.rem(r, 2) + half, j] = value.astype(BF16)
        for n, j in enumerate(js):
            @pl.when(j < groups)
            def _():
                for i in range(ncomp - 1):
                    chunk_copy(0, j, target(i)).start()

    straight = sub == lat
    for copy in point_copies(0):
        copy.wait_recv()
    decode(lat)
    raw_waits()

    def near_body(g, carry):
        ks = [g * NEAR + n for n in range(NEAR)]

        @pl.when(straight)
        def _():
            propagate(ks, False, True)

        @pl.when(jnp.logical_not(straight))
        def _():
            propagate(ks, False, False)
        return carry

    lax.fori_loop(0, kmax // NEAR, near_body, 0)
    for n in (1, 2):
        for copy in point_copies(n):
            copy.wait_recv()
    decode(1 - lat)

    eager = 3 - 2 * side
    patient = 2 - 2 * side

    def far_body(g, carry):
        ks = [g * FAR + n for n in range(FAR)]
        for k in ks:
            @pl.when(f0 + 2 * k < groups)
            def _():
                for s in range(2):
                    halo_wait(k, s)

        @pl.when(straight)
        def _():
            propagate(ks, True, False)

        @pl.when(jnp.logical_not(straight))
        def _():
            propagate(ks, True, True)

        for k in ks:
            @pl.when(n0 + 2 * k < groups)
            def _():
                chunk_copy(1, n0 + 2 * k, eager).start()
        return carry

    lax.fori_loop(0, kmax // FAR, far_body, 0)

    own_copy = pltpu.make_async_copy(
        away_ref.at[sub, me, pl.ds(0, groups)], x_ref.at[0, pl.ds(me * groups, groups), sub, :, 0:lanes], o_sem.at[0])

    def cross_copy():
        return pltpu.make_async_remote_copy(
            src_ref=away_ref.at[1 - sub, me, pl.ds(0, groups)],
            dst_ref=x_ref.at[0, pl.ds(me * groups, groups), sub, :, 0:lanes],
            send_sem=a_send.at[0, me], recv_sem=a_recv.at[me, sub],
            device_id=partner, device_id_type=MESH)

    def prop_copy():
        return pltpu.make_async_remote_copy(
            src_ref=pout_ref.at[pl.ds(0, groups), pl.ds(2 * (1 - sub), 2)],
            dst_ref=pin_ref, send_sem=p_send, recv_sem=p_recv,
            device_id=partner, device_id_type=MESH)

    own_copy.start()
    cross_copy().start()

    def send_rest(k, carry):
        @pl.when(f0 + 2 * k < groups)
        def _():
            chunk_copy(1, f0 + 2 * k, eager).start()
        return carry

    lax.fori_loop(0, kmax, send_rest, 0)

    wide = (sub == 1) & (lax.div(me + 1, 2) == 1)

    def twin_copy(block, to):
        return pltpu.make_async_remote_copy(
            src_ref=away_ref.at[1, block, pl.ds(0, groups)],
            dst_ref=x_ref.at[0, pl.ds(me * groups, groups), sub, :, lanes:2 * lanes],
            send_sem=t_send.at[block], recv_sem=t_recv.at[me, sub],
            device_id={"comp": to, "sub": 1}, device_id_type=MESH)

    def twin_local(block):
        return pltpu.make_async_copy(
            away_ref.at[1, block, pl.ds(0, groups)],
            x_ref.at[0, pl.ds(me * groups, groups), sub, :, lanes:2 * lanes], o_sem.at[1])

    def twin_wait(z, s):
        pltpu.make_async_remote_copy(
            src_ref=away_ref.at[1, 0, pl.ds(0, groups)],
            dst_ref=x_ref.at[0, pl.ds(z * groups, groups), s, :, lanes:2 * lanes],
            send_sem=t_send.at[0], recv_sem=t_recv.at[z, s],
            device_id={"comp": z, "sub": s}, device_id_type=MESH).wait_recv()

    def twin_here(to):
        return (me == to) & (sub == 1)

    def send_twin(block, to):
        @pl.when(jnp.logical_not(twin_here(to)))
        def _():
            twin_copy(block, to).start()

        @pl.when(twin_here(to))
        def _():
            twin_local(block).start()

    send_twin(2, 1)
    whole_copy(1, target(2)).start()
    whole_copy(1, patient).start()
    send_twin(1, 2)
    prop_copy().start()

    piece = bins // PIECES

    def home_copy(source, block, to, start, size):
        span = pl.ds(pl.multiple_of(start, 16), size)
        return pltpu.make_async_remote_copy(
            src_ref=inc_ref.at[source, span], dst_ref=home_ref.at[block, span],
            send_sem=b_send.at[source], recv_sem=b_recv.at[block],
            device_id={"comp": to}, device_id_type=MESH)

    early = (2 * bins) // 128 * 128
    late = total - early

    once = 1 + lax.div(me, ncomp)

    def integrate(width):
        def partial(start, span, use):
            def one(i, carry):
                rows = pl.ds(pl.multiple_of(i * total, 16), total)
                field = x_ref[0, pl.ds(lax.div(start, 32), span // 32), :, :, 0:width].reshape(span, width)
                cols = pl.ds(pl.multiple_of(start, 128), span)
                use(rows, jnp.dot(w_ref[rows, cols], field, preferred_element_type=F32))
                return carry

            lax.fori_loop(0, once, one, 0)

        def begin(rows, driving):
            state_ref[rows, 0:width] = driving

        def first_step(rows, driving):
            start = x_ref[0, :, :, :, 0:width].reshape(total, width).astype(F32)
            now = start + STEP_SIZE * start * (state_ref[rows, 0:width] + driving)
            start_ref[rows, 0:width] = start
            state_ref[rows, 0:width] = now
            x_ref[1, :, :, :, 0:width] = now.astype(BF16).reshape(ncomp * groups, 2, 16, width)

        def advance(step, carry):
            field = x_ref[lax.rem(step, 2), :, :, :, 0:width].reshape(total, width)
            driving = jnp.dot(w_ref[...], field, preferred_element_type=F32)
            now = state_ref[:, 0:width]
            now = now + STEP_SIZE * now * driving
            state_ref[:, 0:width] = now
            x_ref[lax.rem(step + 1, 2), :, :, :, 0:width] = now.astype(BF16).reshape(
                ncomp * groups, 2, 16, width)
            return carry

        def last(m, start):
            rows = pl.ds(pl.multiple_of(m * bins + start, 16), piece)
            field = x_ref[(SRC_STEPS - 1) % 2, :, :, :, 0:width].reshape(total, width)
            driving = jnp.dot(w_ref[rows, :], field, preferred_element_type=F32)
            now = state_ref[rows, 0:width]
            now = now + STEP_SIZE * now * driving
            return (now - start_ref[rows, 0:width]).astype(BF16)

        def finish(n, carry):
            m = target(lax.div(n, PIECES))
            start = lax.rem(n, PIECES) * piece
            span = pl.ds(pl.multiple_of(start, 16), piece)
            gain = last(m, start)

            @pl.when(m == me)
            def _():
                home_ref[me, span] = gain

            @pl.when(m != me)
            def _():
                inc_ref[m, span] = gain
                home_copy(m, me, m, start, piece).start()
            return carry

        def finish_wide(n, carry):
            m = target(lax.div(n, PIECES))
            start = lax.rem(n, PIECES) * piece
            span = pl.ds(pl.multiple_of(start, 16), piece)
            gain = last(m, start)
            blocks = ((me, gain[:, 0:lanes]), (3 - me, gain[:, lanes:2 * lanes]))

            @pl.when(m == me)
            def _():
                for block, part in blocks:
                    home_ref[block, span] = part

            @pl.when(m != me)
            def _():
                for source, (block, part) in enumerate(blocks):
                    inc_ref[source, span] = part
                    home_copy(source, block, m, start, piece).start()
            return carry

        both = width > lanes
        whole_wait(me, 1 - sub)
        for s in range(2):
            whole_wait(target(2), s)
        if both:
            twin_local(3 - me).wait()
            twin_wait(me, 0)
            for s in range(2):
                twin_wait(target(2), s)
        partial(side * late, early, begin)
        for i in (1, 0):
            for s in range(2):
                whole_wait(target(i), s)
                if both:
                    twin_wait(target(i), s)
        partial((1 - side) * early, late, first_step)
        lax.fori_loop(1, SRC_STEPS - 1, advance, 0)
        if both:
            lax.fori_loop((ncomp - 2) * PIECES, ncomp * PIECES, finish_wide, 0)
        else:
            lax.fori_loop(0, ncomp * PIECES, finish, 0)

    sea_wide = [jnp.broadcast_to(sea[:, r * NLON:(r + 1) * NLON], (16, NLON)) for r in range(2)]

    def restore(g, carry):
        js = [g * BACK + n for n in range(BACK)]
        parts = [ref for j in js for ref in (
            pout_ref[j, 2 * sub], pout_ref[j, 2 * sub + 1], pin_ref[j, 0], pin_ref[j, 1])]
        high, low = separate(jnp.concatenate(parts, axis=0))
        plain = (jnp.dot(high, perm_ref[1], preferred_element_type=F32)
                 + jnp.dot(low, perm_ref[1], preferred_element_type=F32))
        for n in range(4 * BACK):
            p = sub if n % 4 < 2 else 1 - sub
            rows = pl.ds(pl.multiple_of((2 * js[n // 4] + p) * 16, 16), 16)
            r = n % 2
            out_ref[rows, r * NLON:(r + 1) * NLON] = sea_wide[r] * plain[n * 16:(n + 1) * 16, :]
        return carry

    def restore_all():
        prop_copy().wait_recv()
        lax.fori_loop(0, groups // BACK, restore, 0)

    pl.when(sub == 1)(restore_all)
    load_w.wait()
    take_w().wait_recv()
    own_copy.wait()
    @pl.when(wide)
    def _():
        integrate(2 * lanes)

    @pl.when(jnp.logical_not(wide))
    def _():
        integrate(lanes)

    pl.when(sub == 0)(restore_all)
    for i in (3, 2, 0, 1):
        z = target(i)

        def land():
            pltpu.make_async_remote_copy(
                src_ref=inc_ref.at[z], dst_ref=home_ref.at[z],
                send_sem=b_send.at[z], recv_sem=b_recv.at[z],
                device_id={"comp": z}, device_id_type=MESH).wait_recv()

        if i < 3:
            pl.when(jnp.logical_not(wide & (z == 3 - me)))(land)
        r = lax.div(z, 2)
        half = lax.rem(z, 2)
        cols = pl.ds(pl.multiple_of(r * NLON, NLON), NLON)
        spread = perm_ref[1, pl.ds(pl.multiple_of(half * lanes, lanes), lanes), :]
        sea_row = jnp.where(r == 0, sea_wide[0][0:8], sea_wide[1][0:8])
        back = jnp.dot(home_ref[z], spread, preferred_element_type=F32)
        back = back.reshape(bins // 8, 8, NLON) * sea_row[None]
        out_ref[:, cols] = out_ref[:, cols] + back.reshape(bins, NLON)

    for n in range(3):
        for copy in point_copies(n):
            copy.wait_send()
    for copy in raw_copies():
        copy.wait_send()

    def halo_left(k, carry):
        @pl.when(n0 + 2 * k < groups)
        def _():
            for p in range(2):
                halo_copy(k, p).wait_send()
        return carry

    lax.fori_loop(0, kmax, halo_left, 0)
    prop_copy().wait_send()
    cross_copy().wait_send()
    give_w().wait_send()
    for i in range(ncomp - 1):
        for h in range(2):
            whole_copy(h, target(i)).wait_send()

        @pl.when(jnp.logical_not(wide))
        def _():
            m = target(i)
            home_copy(m, me, m, 0, bins).wait_send()

    @pl.when(wide)
    def _():
        for source, block in enumerate((me, 3 - me)):
            home_copy(source, block, target(2), 0, bins).wait_send()

    for block, to in ((1, 2), (2, 1)):
        @pl.when(jnp.logical_not(twin_here(to)))
        def _():
            twin_copy(block, to).wait_send()


def write_kernel(src_ref, dst_ref, sems):
    pieces = sems.shape[0]
    rows = src_ref.shape[0] // pieces
    copies = [pltpu.make_async_copy(
        src_ref.at[pl.ds(i * rows, rows)], dst_ref.at[pl.ds(i * rows, rows)], sems.at[i])
        for i in range(pieces)]
    for copy in copies:
        copy.start()
    for copy in copies:
        copy.wait()


def fast_device(ncomp, spectrum, sea_mask, neighbours, substeps, courant, source_operator):
    bins, points = spectrum.shape
    groups = bins // 32
    kmax = (groups + 1) // 2
    lanes = NLON // 2
    total = bins * ncomp
    vmem = pl.BlockSpec(memory_space=pltpu.VMEM)
    hbm = pl.BlockSpec(memory_space=pltpu.HBM)
    dma = pltpu.SemaphoreType.DMA
    result = pl.pallas_call(
        functools.partial(fast_kernel, ncomp),
        out_shape=pltpu.VMEM((bins, points), F32),
        in_specs=[hbm] * 6,
        out_specs=vmem,
        scratch_shapes=[
            pltpu.VMEM((2, 2, 1, points), jnp.int32),
            pltpu.VMEM((2, 2, 4, points), jnp.int32),
            pltpu.SMEM(substeps.shape, jnp.int32),
            pltpu.SMEM(courant.shape, F32),
            pltpu.VMEM((total, total), BF16),
            pltpu.VMEM((2 * kmax, 4, 16, NLON), F32),
            pltpu.VMEM((2 * kmax, 2, 16, NLON), F32),
            pltpu.VMEM((kmax, 2, 2, 16, NLON), BF16),
            pltpu.VMEM((kmax, 4, 16, NLON), BF16),
            pltpu.VMEM((2, 4, 5, 8, NLON), F32),
            pltpu.VMEM((2, 2, 16, lanes), F32),
            pltpu.VMEM((2, NLON, NLON), BF16),
            pltpu.VMEM((2 * kmax, 4, 16, NLON), F32),
            pltpu.VMEM((groups, 2, 16, NLON), F32),
            pltpu.VMEM((2, ncomp, 2 * kmax, 16, lanes), BF16),
            pltpu.VMEM((2, ncomp * groups, 2, 16, 2 * lanes), BF16),
            pltpu.VMEM((total, 2 * lanes), F32),
            pltpu.VMEM((total, 2 * lanes), F32),
            pltpu.VMEM((ncomp, bins, lanes), BF16),
            pltpu.VMEM((ncomp, bins, lanes), BF16),
            dma((4,)), dma((4,)), dma, dma((3, 2)), dma((3, 2)), dma((2,)), dma((2,)), dma, dma,
            dma((kmax, 2)), dma((kmax, 2)), dma((2, ncomp)), dma((ncomp, 2)), dma((ncomp,)), dma((ncomp, 2)),
            dma((2,)), dma, dma,
            dma((ncomp,)), dma((ncomp,)),
        ],
        compiler_params=pltpu.CompilerParams(
            collective_id=1, has_side_effects=True, vmem_limit_bytes=60 * 1024 * 1024),
    )(spectrum.reshape(groups, 2, 16, points), sea_mask.reshape(1, points), neighbours, substeps, courant,
      source_operator)
    return pl.pallas_call(
        write_kernel,
        out_shape=jax.ShapeDtypeStruct((bins, points), F32),
        in_specs=[vmem],
        out_specs=hbm,
        scratch_shapes=[dma((4,))],
        compiler_params=pltpu.CompilerParams(vmem_limit_bytes=4 * 1024 * 1024),
    )(result)


def solution(mesh):
    nlat, ncomp = mesh.shape["lat"], mesh.shape["comp"]

    def per_device(spectrum, sea_mask, neighbours, substeps, courant, source_operator):
        bins, points = spectrum.shape
        even = bins % 32 == 0 and (bins // 32 + 1) // 2 % NEAR == 0 and bins // 32 % BACK == 0
        if nlat == 2 and ncomp == 4 and points == 2 * NLON and even:
            return fast_device(ncomp, spectrum, sea_mask, neighbours, substeps, courant, source_operator)
        size = 16 if bins % 16 == 0 else 8
        chunks = bins // size
        group = 5 if chunks % 5 == 0 else 1
        share = points // ncomp
        total = bins * ncomp
        angles = (np.arange(ND, dtype=np.float32) + np.float32(0.5)) * np.float32(2.0 * math.pi / ND)
        spread = lambda v: jnp.asarray(
            np.broadcast_to(np.abs(v).astype(np.float32)[:, None], (ND, NLON)).reshape(ND // 8, 8, NLON))
        vmem = pl.BlockSpec(memory_space=pltpu.VMEM)
        smem = pl.BlockSpec(memory_space=pltpu.SMEM)
        kinds = 3 if nlat == 2 else 4
        return pl.pallas_call(
            functools.partial(kernel, nlat, ncomp, group),
            out_shape=jax.ShapeDtypeStruct((bins, points), F32),
            in_specs=[vmem, vmem, vmem, smem, smem, vmem, vmem, pl.BlockSpec(memory_space=pl.ANY)],
            out_specs=vmem,
            scratch_shapes=[
                pltpu.VMEM((total, total), BF16),
                pltpu.VMEM((chunks + 2, size, points), BF16),
                pltpu.VMEM((3, chunks + 2, size, points), BF16),
                pltpu.VMEM((2, SLOTS, 4, 8, NLON), F32),
                pltpu.VMEM((chunks, size, points), F32),
                pltpu.VMEM((ncomp, chunks, size, share), BF16),
                pltpu.VMEM((ncomp, chunks, size, share), BF16),
                pltpu.VMEM((total, share), F32),
                pltpu.VMEM((total, share), F32),
                pltpu.VMEM((2, total, share), BF16),
                pltpu.VMEM((ncomp, bins, share), BF16),
                pltpu.VMEM((ncomp, bins, share), BF16),
                pltpu.SemaphoreType.DMA((kinds, chunks + 2)),
                pltpu.SemaphoreType.DMA((kinds, chunks + 2)),
                pltpu.SemaphoreType.DMA,
                pltpu.SemaphoreType.DMA,
                pltpu.SemaphoreType.DMA,
                pltpu.SemaphoreType.DMA((ncomp,)),
                pltpu.SemaphoreType.DMA((ncomp,)),
                pltpu.SemaphoreType.DMA((ncomp,)),
                pltpu.SemaphoreType.DMA((ncomp,)),
            ],
            compiler_params=pltpu.CompilerParams(
                collective_id=0, has_side_effects=True, vmem_limit_bytes=56 * 1024 * 1024),
        )(spectrum, sea_mask.reshape(1, points), neighbours, substeps, courant,
          spread(np.cos(angles)), spread(np.sin(angles)), source_operator)

    placed = (
        P("comp", ("members", "lat", "sub")),
        P(("members", "lat", "sub")),
        P(None, ("members", "lat", "sub")),
        P(),
        P(),
        P("sub", None),
    )
    return jax.shard_map(
        per_device,
        mesh=mesh,
        in_specs=placed,
        out_specs=P("comp", ("members", "lat", "sub")),
        check_vma=False,
    )
```

```python
import functools
import math

import jax
import jax.numpy as jnp
import numpy as np
from jax import lax
from jax.experimental import pallas as pl
from jax.experimental.pallas import tpu as pltpu
from jax.sharding import PartitionSpec as P

NF = 30
ND = 64
NLON = 256
MAXSTEPS = 6
SRC_STEPS = 4
STEP_SIZE = 0.1
MESH = pl.DeviceIdType.MESH
HALF = ND // 2
TILES = 4
SLOTS = 8
NEAR = 4
FAR = 2
BACK = 5
AHEAD = 2
PIECES = 2
F32 = jnp.float32
BF16 = jnp.bfloat16


def kernel(
    nlat, ncomp, group, spec_ref, mask_ref, nb_ref, steps_ref, cour_ref, cos_ref, sin_ref, op_ref,
    out_ref, w_ref, own_ref, halo_ref, code_ref, prop_ref, away_ref, got_ref, start_ref, state_ref,
    low_ref, inc_ref, home_ref,
    h_send, h_recv, w_send, w_recv, w_local, a_send, a_recv, b_send, b_recv,
):
    lat = lax.axis_index("lat")
    sub = lax.axis_index("sub")
    me = lax.axis_index("comp")
    bins, points = spec_ref.shape
    chunks, size = prop_ref.shape[0], prop_ref.shape[1]
    planes = size // 8
    share = points // ncomp
    total = bins * ncomp
    half_rows = total // 2
    first = me * bins
    last_lat = nlat - 1
    partner = {"sub": 1 - sub}

    barrier = pltpu.get_barrier_semaphore()
    peers = [partner]
    if nlat == 2:
        peers.append({"lat": 1 - lat})
    else:
        for move in (1, -1):
            peers.append({"lat": lax.rem(lat + move + nlat, nlat)})
            peers.append({"lat": lax.rem(lat + 2 * move + nlat, nlat), "sub": 1 - sub})
    for j in range(1, ncomp):
        peers.append({"comp": lax.rem(me + j, ncomp)})
    for peer in peers:
        pl.semaphore_signal(barrier, inc=1, device_id=peer, device_id_type=MESH)

    own_half = pl.ds(pl.multiple_of(sub * half_rows, 16), half_rows)
    load_w = pltpu.make_async_copy(op_ref, w_ref.at[own_half], w_local)
    load_w.start()

    lane = lax.broadcasted_iota(jnp.int32, (1, points), 1)
    column = lane & (NLON - 1)
    position = (lat * 2 + sub) * points + lane
    sea = mask_ref[...].astype(F32)
    west = (column - nb_ref[0:1, :]) & (NLON - 1)
    east = (nb_ref[1:2, :] - column) & (NLON - 1)

    def vertical(index_row):
        moved = ((index_row - column + 1) & (NLON - 1)) - 1
        return jnp.where(index_row == position, 2, moved)

    rows = lax.broadcasted_iota(jnp.int32, (size, points), 0)
    codes = jnp.zeros((size, points), F32)
    entries = [west, east, vertical(nb_ref[2:3, :]), vertical(nb_ref[3:4, :])]
    for k, entry in enumerate([e.astype(F32) for e in entries] + [sea]):
        codes = jnp.where(rows == k, jnp.broadcast_to(entry, (size, points)), codes)
    own_ref[0] = codes.astype(BF16)
    own_ref[1] = codes.astype(BF16)

    pl.semaphore_wait(barrier, len(peers))

    def kind(q):
        return lax.rem(lax.div(first + (q - 2) * size, HALF), 2)

    def has_from(ty, far):
        return jnp.where(ty == 0, lat >= far, lat <= last_lat - far)

    def has_to(ty, far):
        return jnp.where(ty == 0, lat <= last_lat - far, lat >= far)

    def pair_copy(q):
        return pltpu.make_async_remote_copy(
            src_ref=own_ref.at[q], dst_ref=halo_ref.at[0, q], send_sem=h_send.at[0, q],
            recv_sem=h_recv.at[0, q], device_id=partner, device_id_type=MESH)

    def side_copy(q, ty):
        to = jnp.clip(lat + 1 - 2 * ty, 0, last_lat)
        return pltpu.make_async_remote_copy(
            src_ref=own_ref.at[q], dst_ref=halo_ref.at[1, q], send_sem=h_send.at[1, q],
            recv_sem=h_recv.at[1, q], device_id={"lat": to}, device_id_type=MESH)

    def hand_copy(q, ty):
        slot = jnp.where(sub == ty, 2, 0)
        return pltpu.make_async_remote_copy(
            src_ref=halo_ref.at[1, q], dst_ref=halo_ref.at[slot, q], send_sem=h_send.at[2, q],
            recv_sem=h_recv.at[2, q], device_id=partner, device_id_type=MESH)

    def far_copy(q, ty):
        to = jnp.clip(lat + 2 - 4 * ty, 0, last_lat)
        return pltpu.make_async_remote_copy(
            src_ref=own_ref.at[q], dst_ref=halo_ref.at[2, q], send_sem=h_send.at[3, q],
            recv_sem=h_recv.at[3, q], device_id={"lat": to, "sub": 1 - sub}, device_id_type=MESH)

    def send_own(q, ty):
        @pl.when(has_to(ty, 1))
        def _():
            side_copy(q, ty).start()

        @pl.when(sub == ty)
        def _():
            pair_copy(q).start()

        if nlat > 2:
            @pl.when((sub != ty) & has_to(ty, 2))
            def _():
                far_copy(q, ty).start()

    def hand_on(q, ty):
        @pl.when(has_from(ty, 1))
        def _():
            side_copy(q, ty).wait_recv()
            hand_copy(q, ty).start()

    def arrive(q, ty):
        @pl.when(has_from(ty, 1))
        def _():
            hand_copy(q, ty).wait_recv()

        @pl.when(sub != ty)
        def _():
            pair_copy(q).wait_recv()

        if nlat > 2:
            @pl.when((sub == ty) & has_from(ty, 2))
            def _():
                far_copy(q, ty).wait_recv()

    def sent(q, ty):
        @pl.when(has_to(ty, 1))
        def _():
            side_copy(q, ty).wait_send()

        @pl.when(sub == ty)
        def _():
            pair_copy(q).wait_send()

        if nlat > 2:
            @pl.when((sub != ty) & has_to(ty, 2))
            def _():
                far_copy(q, ty).wait_send()

        @pl.when(has_from(ty, 1))
        def _():
            hand_copy(q, ty).wait_send()

    send_own(0, 0)
    send_own(1, 1)

    def prepare(i, carry):
        chunk = sea * spec_ref[pl.ds(pl.multiple_of(i * size, size), size), :]
        own_ref[i + 2] = chunk.astype(BF16)
        send_own(i + 2, kind(i + 2))
        return carry

    lax.fori_loop(0, chunks, prepare, 0)

    give_w = pltpu.make_async_remote_copy(
        src_ref=op_ref, dst_ref=w_ref.at[own_half], send_sem=w_send, recv_sem=w_recv,
        device_id=partner, device_id_type=MESH)
    give_w.start()

    for q in (0, 1):
        hand_on(q, q)
    ahead = min(6, chunks)
    for q in range(2, 2 + ahead):
        hand_on(q, kind(q))

    for ty in (0, 1):
        arrive(ty, ty)
        for slot in range(SLOTS):
            row = slot % 2 if ty == 0 else 1 - slot % 2
            cols = slice(row * NLON, (row + 1) * NLON)
            if slot < 6:
                part = halo_ref[2 - slot // 2, ty, :, cols].astype(F32)
            else:
                part = own_ref[ty, :, cols].astype(F32)
            for k, source in enumerate((0, 1, 2 + ty, 4)):
                code_ref[ty, slot, k] = jnp.broadcast_to(part[source:source + 1, :], (8, NLON))

    def propagate(i):
        q = i + 2
        ty = kind(q)

        @pl.when(i + ahead < chunks)
        def _():
            hand_on(q + ahead, kind(q + ahead))

        arrive(q, ty)
        bin0 = first + i * size
        freq = lax.div(bin0, ND)
        direction = lax.rem(bin0, ND)
        to_east = jnp.where((direction < ND // 4) | (direction >= 3 * ND // 4), 1, 0)
        steps = steps_ref[freq]
        speed = cour_ref[freq]
        sign = jnp.where(to_east == 1, 1.0, -1.0)
        shift1 = jnp.where(to_east == 1, 1, NLON - 1)
        shift2 = jnp.where(to_east == 1, 2, NLON - 2)
        back1 = NLON - shift1
        d8 = lax.div(direction, 8)
        abs_cos = cos_ref[pl.ds(d8, planes)]
        abs_sin = sin_ref[pl.ds(d8, planes)]

        def lanes(slot):
            row = jnp.where(ty == 0, slot % 2, 1 - slot % 2)
            return pl.ds(pl.multiple_of(row * NLON, NLON), NLON)

        values = []
        for slot in range(SLOTS):
            if slot < 6:
                part = halo_ref[2 - slot // 2, q, :, lanes(slot)].astype(F32)
            else:
                part = spec_ref[pl.ds(pl.multiple_of(i * size, size), size), lanes(slot)]
            part = part.reshape(planes, 8, NLON)
            if slot >= 6:
                part = part * code_ref[ty, slot, 3][None]
            values.append(part)
        for t in range(MAXSTEPS):
            live = jnp.where(t < steps, speed, 0.0)
            wx = live * abs_cos
            wy = live * abs_sin
            keep = 1.0 - wx - wy
            fresh = list(values)
            for slot in range(t + 1, SLOTS):
                x = values[slot]
                below = values[slot - 1]
                near = code_ref[ty, slot, 1 - to_east][None] == 1.0
                vert = code_ref[ty, slot, 2][None] * sign
                lon = jnp.where(near, pltpu.roll(x, shift1, 2), pltpu.roll(x, shift2, 2))
                up = jnp.where(vert == -1.0, pltpu.roll(below, shift1, 2),
                               jnp.where(vert == 1.0, pltpu.roll(below, back1, 2), below))
                up = jnp.where(jnp.abs(vert) == 2.0, x, up)
                fresh[slot] = code_ref[ty, slot, 3][None] * (keep * x + wx * lon + wy * up)
            values = fresh
        for slot in (6, 7):
            prop_ref[i, :, lanes(slot)] = values[slot].reshape(size, NLON)
        whole = prop_ref[i]
        for c in range(ncomp):
            away_ref[c, i] = whole[:, c * share:(c + 1) * share].astype(BF16)

    groups = chunks // group

    def out_copy(j, g):
        to = lax.rem(me + j, ncomp)
        span = pl.ds(g * group, group)
        return pltpu.make_async_remote_copy(
            src_ref=away_ref.at[to, span], dst_ref=got_ref.at[me, span],
            send_sem=a_send.at[j], recv_sem=a_recv.at[j],
            device_id={"comp": to}, device_id_type=MESH)

    def whole_copy(j):
        to = lax.rem(me + j, ncomp)
        return pltpu.make_async_remote_copy(
            src_ref=away_ref.at[to], dst_ref=got_ref.at[me],
            send_sem=a_send.at[j], recv_sem=a_recv.at[j],
            device_id={"comp": to}, device_id_type=MESH)

    def run_group(g, carry):
        def one(i, inner):
            propagate(g * group + i)
            return inner

        lax.fori_loop(0, group, one, 0)
        for j in range(1, ncomp):
            out_copy(j, g).start()
        return carry

    lax.fori_loop(0, groups, run_group, 0)

    for q in (0, 1):
        sent(q, q)

    def drain(q, carry):
        sent(q, kind(q))
        return carry

    lax.fori_loop(2, chunks + 2, drain, 0)
    got_ref[me] = away_ref[me]
    load_w.wait()
    give_w.wait()

    for j in range(1, ncomp):
        whole_copy(j).wait()
    for c in range(ncomp):
        start_ref[c * bins:(c + 1) * bins, :] = got_ref[c].astype(F32).reshape(bins, share)
    tile = total // TILES
    per_tile = bins // tile if bins >= tile else tile // bins
    for m in range(TILES):
        span = slice(m * tile, (m + 1) * tile)
        low_ref[0, span, :] = start_ref[span, :].astype(BF16)

    def tile_rows(m):
        return pl.ds(pl.multiple_of(m * tile, 16), tile)

    def advance(step, m):
        span = tile_rows(m)
        driving = jnp.dot(w_ref[span, :], low_ref[step % 2], preferred_element_type=F32)
        now = start_ref[span, :] if step == 0 else state_ref[span, :]
        return span, now + STEP_SIZE * now * driving

    for step in range(SRC_STEPS - 1):
        def one_tile(m, carry, step=step):
            span, now = advance(step, m)
            state_ref[span, :] = now
            low_ref[(step + 1) % 2, span, :] = now.astype(BF16)
            return carry

        lax.fori_loop(0, TILES, one_tile, 0)

    def home_copy(j, to):
        return pltpu.make_async_remote_copy(
            src_ref=inc_ref.at[to], dst_ref=home_ref.at[me],
            send_sem=b_send.at[j], recv_sem=b_recv.at[j],
            device_id={"comp": to}, device_id_type=MESH)

    mine = lax.div(me * TILES, ncomp)

    def last_tile(i, carry):
        m = lax.rem(mine + 1 + i, TILES)
        span, now = advance(SRC_STEPS - 1, m)
        gain = now - start_ref[span, :]
        for k in range(per_tile):
            to = m * per_tile + k
            inc_ref[to] = gain[k * bins:(k + 1) * bins, :].astype(BF16)
            j = lax.rem(to - me + ncomp, ncomp)

            @pl.when(to != me)
            def _():
                home_copy(j, to).start()

        return carry

    lax.fori_loop(0, TILES, last_tile, 0)
    home_ref[me] = inc_ref[me]
    for c in range(ncomp):
        j = lax.rem(me - c + ncomp, ncomp)

        @pl.when(me != c)
        def _():
            home_copy(j, lax.rem(me + j, ncomp)).wait()

        cols = slice(c * share, (c + 1) * share)
        before = prop_ref[:, :, cols].reshape(bins, share)
        out_ref[:, cols] = sea[:, cols] * (before + home_ref[c].astype(F32))


def fast_kernel(
    ncomp, spec_ref, mask_hbm, nb_hbm, steps_hbm, cour_hbm, op_ref,
    out_ref, mask_ref, nb_ref, steps_ref, cour_ref, w_ref, full_ref, oth_ref, hsend_ref, halo_ref, code_ref, ang_ref, perm_ref,
    pout_ref, pin_ref, away_ref, x_ref, start_ref, state_ref, inc_ref, home_ref,
    l_sem, i_sem, w_sem, c_send, c_recv, r_send, r_recv, g_send, g_recv, h_send, h_recv,
    a_send, a_recv, t_send, t_recv, o_sem, p_send, p_recv, b_send, b_recv,
):
    lat = lax.axis_index("lat")
    sub = lax.axis_index("sub")
    me = lax.axis_index("comp")
    groups = spec_ref.shape[0]
    bins = groups * 2 * 16
    kmax = halo_ref.shape[0]
    lanes = NLON // 2
    total = bins * ncomp
    partner = {"sub": 1 - sub}
    others = [partner, {"lat": 1 - lat}, {"lat": 1 - lat, "sub": 1 - sub}]

    small = [pltpu.make_async_copy(src, dst, i_sem.at[n]) for n, (src, dst) in enumerate((
        (mask_hbm, mask_ref.at[lat, sub]), (nb_hbm, nb_ref.at[lat, sub]),
        (steps_hbm, steps_ref), (cour_hbm, cour_ref)))]
    loads = []
    for r in range(2):
        cols = slice(r * NLON, (r + 1) * NLON)
        loads.append(pltpu.make_async_copy(
            spec_ref.at[:, 1 - sub, :, cols], oth_ref.at[pl.ds(0, groups), r], l_sem.at[r]))
        loads.append(pltpu.make_async_copy(
            spec_ref.at[:, sub, :, cols], full_ref.at[pl.ds(0, groups), 2 * sub + r], l_sem.at[2 + r]))
    for load in (small[0], *loads, *small[1:]):
        load.start()
    own_half = pl.ds(pl.multiple_of(sub * (total // 2), 16), total // 2)
    load_w = pltpu.make_async_copy(op_ref, w_ref.at[own_half], w_sem)

    barrier = pltpu.get_barrier_semaphore()
    peers = list(others)
    for d in range(1, ncomp):
        z = lax.rem(me + d, ncomp)
        peers += [{"comp": z}, {"comp": z, "sub": 1 - sub}]
    for peer in peers:
        pl.semaphore_signal(barrier, inc=1, device_id=peer, device_id_type=MESH)

    a = lax.broadcasted_iota(jnp.int32, (NLON, NLON), 0)
    b = lax.broadcasted_iota(jnp.int32, (NLON, NLON), 1)
    split = lambda c: jnp.where(c < lanes, 2 * c, 2 * (c - lanes) + 1)
    perm_ref[0] = (a == split(b)).astype(F32).astype(BF16)
    perm_ref[1] = (b == split(a)).astype(F32).astype(BF16)

    near_ty = lat
    far_ty = 1 - lat
    n0 = lax.rem(lat + me * groups, 2)
    f0 = 1 - n0
    for q, ty in enumerate((near_ty, far_ty)):
        d = lax.broadcasted_iota(jnp.int32, (16, lanes), 0) + 16 * (2 * ty + sub)
        angle = (d.astype(F32) + 0.5) * np.float32(2.0 * math.pi / ND)
        ang_ref[q, 0] = jnp.abs(jnp.cos(angle))
        ang_ref[q, 1] = jnp.abs(jnp.sin(angle))

    def point_copies(n):
        return [pltpu.make_async_remote_copy(
            src_ref=ref.at[lat, sub], dst_ref=ref.at[lat, sub], send_sem=c_send.at[n, m],
            recv_sem=c_recv.at[n, m], device_id=others[n], device_id_type=MESH)
            for m, ref in enumerate((mask_ref, nb_ref))]

    def raw_copies():
        return [pltpu.make_async_remote_copy(
            src_ref=spec_ref.at[:, 1 - sub, :, r * NLON:(r + 1) * NLON],
            dst_ref=full_ref.at[pl.ds(0, groups), 2 * sub + r],
            send_sem=r_send.at[r], recv_sem=r_recv.at[r], device_id=partner, device_id_type=MESH)
            for r in range(2)]

    def raw_waits():
        for r in range(2):
            pltpu.make_async_remote_copy(
                src_ref=spec_ref.at[:, 1 - sub, :, r * NLON:(r + 1) * NLON],
                dst_ref=full_ref.at[pl.ds(0, groups), 2 * (1 - sub) + r],
                send_sem=r_send.at[r], recv_sem=r_recv.at[r],
                device_id=partner, device_id_type=MESH).wait_recv()

    small[0].wait()
    small[1].wait()
    sea = mask_ref[lat, sub].astype(F32)
    for load in loads:
        load.wait()
    sea_rows = [jnp.broadcast_to(sea[:, r * NLON:(r + 1) * NLON], (16, NLON)) for r in range(2)]

    def convert(k, carry):
        j = n0 + 2 * k
        for r in range(2):
            mine = full_ref[j, 2 * sub + r] * sea_rows[r]
            other = oth_ref[j, r] * sea_rows[r]
            hsend_ref[k, sub, r] = mine.astype(BF16)
            hsend_ref[k, 1 - sub, r] = other.astype(BF16)
        return carry

    lax.fori_loop(0, kmax, convert, 0)
    pl.semaphore_wait(barrier, len(peers))
    def halo_copy(k, p):
        return pltpu.make_async_remote_copy(
            src_ref=hsend_ref.at[k, p], dst_ref=halo_ref.at[k, pl.ds(2 * sub, 2)],
            send_sem=h_send.at[k, p], recv_sem=h_recv.at[k, sub],
            device_id={"lat": 1 - lat, "sub": p}, device_id_type=MESH)

    def halo_wait(k, s):
        pltpu.make_async_remote_copy(
            src_ref=hsend_ref.at[k, s], dst_ref=halo_ref.at[k, pl.ds(2 * s, 2)],
            send_sem=h_send.at[k, s], recv_sem=h_recv.at[k, s],
            device_id={"lat": 1 - lat, "sub": s}, device_id_type=MESH).wait_recv()

    def give_w():
        return pltpu.make_async_remote_copy(
            src_ref=op_ref, dst_ref=w_ref.at[own_half], send_sem=g_send, recv_sem=g_recv,
            device_id=partner, device_id_type=MESH)

    def take_w():
        other_half = pl.ds(pl.multiple_of((1 - sub) * (total // 2), 16), total // 2)
        return pltpu.make_async_remote_copy(
            src_ref=op_ref, dst_ref=w_ref.at[other_half], send_sem=g_send, recv_sem=g_recv,
            device_id=partner, device_id_type=MESH)

    def send_halo(k, carry):
        @pl.when(n0 + 2 * k < groups)
        def _():
            for p in range(2):
                halo_copy(k, p).start()
        return carry

    for copy in point_copies(0):
        copy.start()
    lax.fori_loop(0, AHEAD, send_halo, 0)
    for copy in (*raw_copies(), *point_copies(1), *point_copies(2)):
        copy.start()
    lax.fori_loop(AHEAD, kmax, send_halo, 0)
    load_w.start()
    give_w().start()
    for load in small[2:]:
        load.wait()

    points = mask_ref.shape[-1]
    lane = lax.broadcasted_iota(jnp.int32, (1, points), 1)
    column = lane & (NLON - 1)
    index = lax.broadcasted_iota(jnp.int32, (8, points), 0)

    def decode(chip):
        for s in range(2):
            nb = nb_ref[chip, s]
            west = (column - nb[0:1, :]) & (NLON - 1)
            east = (nb[1:2, :] - column) & (NLON - 1)
            moves = [((nb[k:k + 1, :] - column + 1) & (NLON - 1)) - 1 for k in (2, 3)]
            codes = jnp.zeros((8, points), F32)
            for k, entry in enumerate((west, east, *moves, mask_ref[chip, s])):
                codes = jnp.where(index == k, jnp.broadcast_to(entry.astype(F32), (8, points)), codes)
            for r in range(2):
                part = codes[:, r * NLON:(r + 1) * NLON].astype(BF16)
                both = jnp.dot(part, perm_ref[0], preferred_element_type=F32)
                for k in range(5):
                    code_ref[chip, 2 * s + r, k] = jnp.broadcast_to(both[k:k + 1, :], (8, NLON))

    side = lax.div(me, 2)

    def target(i):
        near = me + 1 - 2 * lax.rem(me, 2)
        return jnp.where(i == 0, 3 - 3 * side, jnp.where(i == 1, 2 - side, jnp.where(i == 2, near, me)))

    def outward(i):
        k = lax.rem(i + 2, 3)
        return target(jnp.where((side == 0) & (sub == 0) & (i < 3), k, i))

    def chunk_copy(h, j, to):
        return pltpu.make_async_remote_copy(
            src_ref=away_ref.at[h, to, j], dst_ref=x_ref.at[0, me * groups + j, sub, :, 0:lanes],
            send_sem=a_send.at[h, to], recv_sem=a_recv.at[me, sub],
            device_id={"comp": to, "sub": h}, device_id_type=MESH)

    def whole_copy(h, to):
        return pltpu.make_async_remote_copy(
            src_ref=away_ref.at[h, to, pl.ds(0, groups)],
            dst_ref=x_ref.at[0, pl.ds(me * groups, groups), sub, :, 0:lanes],
            send_sem=a_send.at[h, to], recv_sem=a_recv.at[me, sub],
            device_id={"comp": to, "sub": h}, device_id_type=MESH)

    def whole_wait(z, s):
        pltpu.make_async_remote_copy(
            src_ref=away_ref.at[0, z, pl.ds(0, groups)],
            dst_ref=x_ref.at[0, pl.ds(z * groups, groups), s, :, 0:lanes],
            send_sem=a_send.at[0, 0], recv_sem=a_recv.at[z, s],
            device_id={"comp": z, "sub": s}, device_id_type=MESH).wait_recv()

    def pick(ty, i):
        return ty * 3 + (1 - 2 * ty) * i

    def separate(x):
        high = x.astype(BF16)
        low = (x - high.astype(F32)).astype(BF16)
        return high, low

    def propagate(ks, far, to_east):
        ty = far_ty if far else near_ty
        js = [(f0 if far else n0) + 2 * k for k in ks]
        vert = 2 + ty
        lowest = 0 if far else 4

        def code(q, k, half):
            chip = lat if q >= 4 else 1 - lat
            part = code_ref[chip, pick(ty, q % 4), k, :, half * lanes:(half + 1) * lanes]
            return jnp.concatenate([part, part], axis=0)

        raw = jnp.concatenate([full_ref[j, pick(ty, i)] for j in js for i in range(4)], axis=0)
        high, low = separate(raw)
        mixed = (jnp.dot(high, perm_ref[0], preferred_element_type=F32)
                 + jnp.dot(low, perm_ref[0], preferred_element_type=F32))
        if far:
            edge = jnp.concatenate([halo_ref[k, pick(ty, i)] for k in ks for i in range(4)], axis=0)
            edge = jnp.dot(edge, perm_ref[0], preferred_element_type=F32)
        cells = []
        weights = []
        for n, j in enumerate(js):
            values = [None] * 8
            for i in range(4):
                rows = slice((n * 4 + i) * 16, (n * 4 + i + 1) * 16)
                values[4 + i] = tuple(
                    mixed[rows, half * lanes:(half + 1) * lanes] * code(4 + i, 4, half)
                    for half in range(2))
                if far:
                    values[i] = tuple(edge[rows, half * lanes:(half + 1) * lanes] for half in range(2))
            cells.append(values)
            freq = jnp.minimum(lax.div(me * bins + j * 32, ND), steps_ref.shape[0] - 1)
            weights.append((steps_ref[freq], cour_ref[freq]))
        abs_cos, abs_sin = ang_ref[int(far), 0], ang_ref[int(far), 1]
        ahead, behind = (1, lanes - 1)
        for t in range(MAXSTEPS):
            slots = [q for q in range(7, lowest - 1, -1) if q >= 4 or t <= q + 1]
            for n, (steps, speed) in enumerate(weights):
                live = jnp.where(t < steps, speed, 0.0)
                wx = live * abs_cos
                wy = live * abs_sin
                keep = 1.0 - wx - wy
                values = cells[n]
                fresh = list(values)
                turned = {}

                def turn(q, half, shift):
                    key = (q, half, shift)
                    if key not in turned:
                        turned[key] = pltpu.roll(values[q][half], shift, 1)
                    return turned[key]

                def left(q):
                    return turn(q, 1, ahead), values[q][0]

                def right(q):
                    return values[q][1], turn(q, 0, behind)

                for q in slots:
                    shift = ahead if to_east else behind
                    one = left(q) if to_east else right(q)
                    lon_code = 0 if to_east else 1
                    new = []
                    for half in range(2):
                        x = values[q][half]
                        lon = jnp.where(code(q, lon_code, half) == 1.0, one[half], turn(q, half, shift))
                        if q == lowest:
                            up = x
                        else:
                            move = code(q, vert, half)
                            up = jnp.where(move == -1.0, left(q - 1)[half],
                                           jnp.where(move == 1.0, right(q - 1)[half], values[q - 1][half]))
                        new.append(code(q, 4, half) * (keep * x + wx * lon + wy * up))
                    fresh[q] = tuple(new)
                cells[n] = fresh
        for n, j in enumerate(js):
            for i in range(4):
                r = pick(ty, i)
                for half in range(2):
                    value = cells[n][4 + i][half]
                    pout_ref[j, r, :, half * lanes:(half + 1) * lanes] = value
                    away_ref[lax.div(r, 2), 2 * lax.rem(r, 2) + half, j] = value.astype(BF16)
        for n, j in enumerate(js):
            @pl.when(j < groups)
            def _():
                for i in range(ncomp - 1):
                    chunk_copy(0, j, target(i)).start()

    straight = sub == lat
    for copy in point_copies(0):
        copy.wait_recv()
    decode(lat)
    raw_waits()

    def near_body(g, carry):
        ks = [g * NEAR + n for n in range(NEAR)]

        @pl.when(straight)
        def _():
            propagate(ks, False, True)

        @pl.when(jnp.logical_not(straight))
        def _():
            propagate(ks, False, False)
        return carry

    lax.fori_loop(0, kmax // NEAR, near_body, 0)
    for n in (1, 2):
        for copy in point_copies(n):
            copy.wait_recv()
    decode(1 - lat)

    eager = 3 - 2 * side
    patient = 2 - 2 * side

    def far_body(g, carry):
        ks = [g * FAR + n for n in range(FAR)]
        for k in ks:
            @pl.when(f0 + 2 * k < groups)
            def _():
                for s in range(2):
                    halo_wait(k, s)

        @pl.when(straight)
        def _():
            propagate(ks, True, False)

        @pl.when(jnp.logical_not(straight))
        def _():
            propagate(ks, True, True)

        for k in ks:
            @pl.when(n0 + 2 * k < groups)
            def _():
                chunk_copy(1, n0 + 2 * k, eager).start()
        return carry

    lax.fori_loop(0, kmax // FAR, far_body, 0)

    own_copy = pltpu.make_async_copy(
        away_ref.at[sub, me, pl.ds(0, groups)], x_ref.at[0, pl.ds(me * groups, groups), sub, :, 0:lanes], o_sem.at[0])

    def cross_copy():
        return pltpu.make_async_remote_copy(
            src_ref=away_ref.at[1 - sub, me, pl.ds(0, groups)],
            dst_ref=x_ref.at[0, pl.ds(me * groups, groups), sub, :, 0:lanes],
            send_sem=a_send.at[0, me], recv_sem=a_recv.at[me, sub],
            device_id=partner, device_id_type=MESH)

    def prop_copy():
        return pltpu.make_async_remote_copy(
            src_ref=pout_ref.at[pl.ds(0, groups), pl.ds(2 * (1 - sub), 2)],
            dst_ref=pin_ref, send_sem=p_send, recv_sem=p_recv,
            device_id=partner, device_id_type=MESH)

    own_copy.start()
    cross_copy().start()

    def send_rest(k, carry):
        @pl.when(f0 + 2 * k < groups)
        def _():
            chunk_copy(1, f0 + 2 * k, eager).start()
        return carry

    lax.fori_loop(0, kmax, send_rest, 0)

    wide = (sub == 1) & (lax.div(me + 1, 2) == 1)

    def twin_copy(block, to):
        return pltpu.make_async_remote_copy(
            src_ref=away_ref.at[1, block, pl.ds(0, groups)],
            dst_ref=x_ref.at[0, pl.ds(me * groups, groups), sub, :, lanes:2 * lanes],
            send_sem=t_send.at[block], recv_sem=t_recv.at[me, sub],
            device_id={"comp": to, "sub": 1}, device_id_type=MESH)

    def twin_local(block):
        return pltpu.make_async_copy(
            away_ref.at[1, block, pl.ds(0, groups)],
            x_ref.at[0, pl.ds(me * groups, groups), sub, :, lanes:2 * lanes], o_sem.at[1])

    def twin_wait(z, s):
        pltpu.make_async_remote_copy(
            src_ref=away_ref.at[1, 0, pl.ds(0, groups)],
            dst_ref=x_ref.at[0, pl.ds(z * groups, groups), s, :, lanes:2 * lanes],
            send_sem=t_send.at[0], recv_sem=t_recv.at[z, s],
            device_id={"comp": z, "sub": s}, device_id_type=MESH).wait_recv()

    def twin_here(to):
        return (me == to) & (sub == 1)

    def send_twin(block, to):
        @pl.when(jnp.logical_not(twin_here(to)))
        def _():
            twin_copy(block, to).start()

        @pl.when(twin_here(to))
        def _():
            twin_local(block).start()

    send_twin(2, 1)
    whole_copy(1, target(2)).start()
    whole_copy(1, patient).start()
    send_twin(1, 2)
    prop_copy().start()

    piece = bins // PIECES

    def home_copy(source, block, to, start, size):
        span = pl.ds(pl.multiple_of(start, 16), size)
        return pltpu.make_async_remote_copy(
            src_ref=inc_ref.at[source, span], dst_ref=home_ref.at[block, span],
            send_sem=b_send.at[source], recv_sem=b_recv.at[block],
            device_id={"comp": to}, device_id_type=MESH)

    early = (2 * bins) // 128 * 128
    late = total - early

    once = 1 + lax.div(me, ncomp)

    def integrate(width):
        def partial(start, span, use):
            def one(i, carry):
                rows = pl.ds(pl.multiple_of(i * total, 16), total)
                field = x_ref[0, pl.ds(lax.div(start, 32), span // 32), :, :, 0:width].reshape(span, width)
                cols = pl.ds(pl.multiple_of(start, 128), span)
                use(rows, jnp.dot(w_ref[rows, cols], field, preferred_element_type=F32))
                return carry

            lax.fori_loop(0, once, one, 0)

        def begin(rows, driving):
            state_ref[rows, 0:width] = driving

        def first_step(rows, driving):
            start = x_ref[0, :, :, :, 0:width].reshape(total, width).astype(F32)
            now = start + STEP_SIZE * start * (state_ref[rows, 0:width] + driving)
            start_ref[rows, 0:width] = start
            state_ref[rows, 0:width] = now
            x_ref[1, :, :, :, 0:width] = now.astype(BF16).reshape(ncomp * groups, 2, 16, width)

        def advance(step, carry):
            field = x_ref[lax.rem(step, 2), :, :, :, 0:width].reshape(total, width)
            driving = jnp.dot(w_ref[...], field, preferred_element_type=F32)
            now = state_ref[:, 0:width]
            now = now + STEP_SIZE * now * driving
            state_ref[:, 0:width] = now
            x_ref[lax.rem(step + 1, 2), :, :, :, 0:width] = now.astype(BF16).reshape(
                ncomp * groups, 2, 16, width)
            return carry

        def last(m, start):
            rows = pl.ds(pl.multiple_of(m * bins + start, 16), piece)
            field = x_ref[(SRC_STEPS - 1) % 2, :, :, :, 0:width].reshape(total, width)
            driving = jnp.dot(w_ref[rows, :], field, preferred_element_type=F32)
            now = state_ref[rows, 0:width]
            now = now + STEP_SIZE * now * driving
            return (now - start_ref[rows, 0:width]).astype(BF16)

        def finish(n, carry):
            m = outward(lax.div(n, PIECES))
            start = lax.rem(n, PIECES) * piece
            span = pl.ds(pl.multiple_of(start, 16), piece)
            gain = last(m, start)

            @pl.when(m == me)
            def _():
                home_ref[me, span] = gain

            @pl.when(m != me)
            def _():
                inc_ref[m, span] = gain
                home_copy(m, me, m, start, piece).start()
            return carry

        def finish_wide(n, carry):
            m = target(lax.div(n, PIECES))
            start = lax.rem(n, PIECES) * piece
            span = pl.ds(pl.multiple_of(start, 16), piece)
            gain = last(m, start)
            blocks = ((me, gain[:, 0:lanes]), (3 - me, gain[:, lanes:2 * lanes]))

            @pl.when(m == me)
            def _():
                for block, part in blocks:
                    home_ref[block, span] = part

            @pl.when(m != me)
            def _():
                for source, (block, part) in enumerate(blocks):
                    inc_ref[source, span] = part
                    home_copy(source, block, m, start, piece).start()
            return carry

        both = width > lanes
        whole_wait(me, 1 - sub)
        for s in range(2):
            whole_wait(target(2), s)
        if both:
            twin_local(3 - me).wait()
            twin_wait(me, 0)
            for s in range(2):
                twin_wait(target(2), s)
        partial(side * late, early, begin)
        for i in (1, 0):
            for s in range(2):
                whole_wait(target(i), s)
                if both:
                    twin_wait(target(i), s)
        partial((1 - side) * early, late, first_step)
        lax.fori_loop(1, SRC_STEPS - 1, advance, 0)
        if both:
            lax.fori_loop((ncomp - 2) * PIECES, ncomp * PIECES, finish_wide, 0)
        else:
            lax.fori_loop(0, ncomp * PIECES, finish, 0)

    sea_wide = [jnp.broadcast_to(sea[:, r * NLON:(r + 1) * NLON], (16, NLON)) for r in range(2)]

    def restore(g, carry):
        js = [g * BACK + n for n in range(BACK)]
        parts = [ref for j in js for ref in (
            pout_ref[j, 2 * sub], pout_ref[j, 2 * sub + 1], pin_ref[j, 0], pin_ref[j, 1])]
        high, low = separate(jnp.concatenate(parts, axis=0))
        plain = (jnp.dot(high, perm_ref[1], preferred_element_type=F32)
                 + jnp.dot(low, perm_ref[1], preferred_element_type=F32))
        for n in range(4 * BACK):
            p = sub if n % 4 < 2 else 1 - sub
            rows = pl.ds(pl.multiple_of((2 * js[n // 4] + p) * 16, 16), 16)
            r = n % 2
            out_ref[rows, r * NLON:(r + 1) * NLON] = sea_wide[r] * plain[n * 16:(n + 1) * 16, :]
        return carry

    def restore_all():
        prop_copy().wait_recv()
        lax.fori_loop(0, groups // BACK, restore, 0)

    pl.when(sub == 1)(restore_all)
    load_w.wait()
    take_w().wait_recv()
    own_copy.wait()
    @pl.when(wide)
    def _():
        integrate(2 * lanes)

    @pl.when(jnp.logical_not(wide))
    def _():
        integrate(lanes)

    pl.when(sub == 0)(restore_all)
    for i in (3, 0, 2, 1):
        z = target(i)

        def land():
            pltpu.make_async_remote_copy(
                src_ref=inc_ref.at[z], dst_ref=home_ref.at[z],
                send_sem=b_send.at[z], recv_sem=b_recv.at[z],
                device_id={"comp": z}, device_id_type=MESH).wait_recv()

        if i < 3:
            pl.when(jnp.logical_not(wide & (z == 3 - me)))(land)
        r = lax.div(z, 2)
        half = lax.rem(z, 2)
        cols = pl.ds(pl.multiple_of(r * NLON, NLON), NLON)
        spread = perm_ref[1, pl.ds(pl.multiple_of(half * lanes, lanes), lanes), :]
        sea_row = jnp.where(r == 0, sea_wide[0][0:8], sea_wide[1][0:8])
        back = jnp.dot(home_ref[z], spread, preferred_element_type=F32)
        back = back.reshape(bins // 8, 8, NLON) * sea_row[None]
        out_ref[:, cols] = out_ref[:, cols] + back.reshape(bins, NLON)

    for n in range(3):
        for copy in point_copies(n):
            copy.wait_send()
    for copy in raw_copies():
        copy.wait_send()

    def halo_left(k, carry):
        @pl.when(n0 + 2 * k < groups)
        def _():
            for p in range(2):
                halo_copy(k, p).wait_send()
        return carry

    lax.fori_loop(0, kmax, halo_left, 0)
    prop_copy().wait_send()
    cross_copy().wait_send()
    give_w().wait_send()
    for i in range(ncomp - 1):
        for h in range(2):
            whole_copy(h, target(i)).wait_send()

        @pl.when(jnp.logical_not(wide))
        def _():
            m = target(i)
            home_copy(m, me, m, 0, bins).wait_send()

    @pl.when(wide)
    def _():
        for source, block in enumerate((me, 3 - me)):
            home_copy(source, block, target(2), 0, bins).wait_send()

    for block, to in ((1, 2), (2, 1)):
        @pl.when(jnp.logical_not(twin_here(to)))
        def _():
            twin_copy(block, to).wait_send()


def write_kernel(src_ref, dst_ref, sems):
    pieces = sems.shape[0]
    rows = src_ref.shape[0] // pieces
    copies = [pltpu.make_async_copy(
        src_ref.at[pl.ds(i * rows, rows)], dst_ref.at[pl.ds(i * rows, rows)], sems.at[i])
        for i in range(pieces)]
    for copy in copies:
        copy.start()
    for copy in copies:
        copy.wait()


def fast_device(ncomp, spectrum, sea_mask, neighbours, substeps, courant, source_operator):
    bins, points = spectrum.shape
    groups = bins // 32
    kmax = (groups + 1) // 2
    lanes = NLON // 2
    total = bins * ncomp
    vmem = pl.BlockSpec(memory_space=pltpu.VMEM)
    hbm = pl.BlockSpec(memory_space=pltpu.HBM)
    dma = pltpu.SemaphoreType.DMA
    result = pl.pallas_call(
        functools.partial(fast_kernel, ncomp),
        out_shape=pltpu.VMEM((bins, points), F32),
        in_specs=[hbm] * 6,
        out_specs=vmem,
        scratch_shapes=[
            pltpu.VMEM((2, 2, 1, points), jnp.int32),
            pltpu.VMEM((2, 2, 4, points), jnp.int32),
            pltpu.SMEM(substeps.shape, jnp.int32),
            pltpu.SMEM(courant.shape, F32),
            pltpu.VMEM((total, total), BF16),
            pltpu.VMEM((2 * kmax, 4, 16, NLON), F32),
            pltpu.VMEM((2 * kmax, 2, 16, NLON), F32),
            pltpu.VMEM((kmax, 2, 2, 16, NLON), BF16),
            pltpu.VMEM((kmax, 4, 16, NLON), BF16),
            pltpu.VMEM((2, 4, 5, 8, NLON), F32),
            pltpu.VMEM((2, 2, 16, lanes), F32),
            pltpu.VMEM((2, NLON, NLON), BF16),
            pltpu.VMEM((2 * kmax, 4, 16, NLON), F32),
            pltpu.VMEM((groups, 2, 16, NLON), F32),
            pltpu.VMEM((2, ncomp, 2 * kmax, 16, lanes), BF16),
            pltpu.VMEM((2, ncomp * groups, 2, 16, 2 * lanes), BF16),
            pltpu.VMEM((total, 2 * lanes), F32),
            pltpu.VMEM((total, 2 * lanes), F32),
            pltpu.VMEM((ncomp, bins, lanes), BF16),
            pltpu.VMEM((ncomp, bins, lanes), BF16),
            dma((4,)), dma((4,)), dma, dma((3, 2)), dma((3, 2)), dma((2,)), dma((2,)), dma, dma,
            dma((kmax, 2)), dma((kmax, 2)), dma((2, ncomp)), dma((ncomp, 2)), dma((ncomp,)), dma((ncomp, 2)),
            dma((2,)), dma, dma,
            dma((ncomp,)), dma((ncomp,)),
        ],
        compiler_params=pltpu.CompilerParams(
            collective_id=1, has_side_effects=True, vmem_limit_bytes=60 * 1024 * 1024),
    )(spectrum.reshape(groups, 2, 16, points), sea_mask.reshape(1, points), neighbours, substeps, courant,
      source_operator)
    return pl.pallas_call(
        write_kernel,
        out_shape=jax.ShapeDtypeStruct((bins, points), F32),
        in_specs=[vmem],
        out_specs=hbm,
        scratch_shapes=[dma((4,))],
        compiler_params=pltpu.CompilerParams(vmem_limit_bytes=4 * 1024 * 1024),
    )(result)


def solution(mesh):
    nlat, ncomp = mesh.shape["lat"], mesh.shape["comp"]

    def per_device(spectrum, sea_mask, neighbours, substeps, courant, source_operator):
        bins, points = spectrum.shape
        even = bins % 32 == 0 and (bins // 32 + 1) // 2 % NEAR == 0 and bins // 32 % BACK == 0
        if nlat == 2 and ncomp == 4 and points == 2 * NLON and even:
            return fast_device(ncomp, spectrum, sea_mask, neighbours, substeps, courant, source_operator)
        size = 16 if bins % 16 == 0 else 8
        chunks = bins // size
        group = 5 if chunks % 5 == 0 else 1
        share = points // ncomp
        total = bins * ncomp
        angles = (np.arange(ND, dtype=np.float32) + np.float32(0.5)) * np.float32(2.0 * math.pi / ND)
        spread = lambda v: jnp.asarray(
            np.broadcast_to(np.abs(v).astype(np.float32)[:, None], (ND, NLON)).reshape(ND // 8, 8, NLON))
        vmem = pl.BlockSpec(memory_space=pltpu.VMEM)
        smem = pl.BlockSpec(memory_space=pltpu.SMEM)
        kinds = 3 if nlat == 2 else 4
        return pl.pallas_call(
            functools.partial(kernel, nlat, ncomp, group),
            out_shape=jax.ShapeDtypeStruct((bins, points), F32),
            in_specs=[vmem, vmem, vmem, smem, smem, vmem, vmem, pl.BlockSpec(memory_space=pl.ANY)],
            out_specs=vmem,
            scratch_shapes=[
                pltpu.VMEM((total, total), BF16),
                pltpu.VMEM((chunks + 2, size, points), BF16),
                pltpu.VMEM((3, chunks + 2, size, points), BF16),
                pltpu.VMEM((2, SLOTS, 4, 8, NLON), F32),
                pltpu.VMEM((chunks, size, points), F32),
                pltpu.VMEM((ncomp, chunks, size, share), BF16),
                pltpu.VMEM((ncomp, chunks, size, share), BF16),
                pltpu.VMEM((total, share), F32),
                pltpu.VMEM((total, share), F32),
                pltpu.VMEM((2, total, share), BF16),
                pltpu.VMEM((ncomp, bins, share), BF16),
                pltpu.VMEM((ncomp, bins, share), BF16),
                pltpu.SemaphoreType.DMA((kinds, chunks + 2)),
                pltpu.SemaphoreType.DMA((kinds, chunks + 2)),
                pltpu.SemaphoreType.DMA,
                pltpu.SemaphoreType.DMA,
                pltpu.SemaphoreType.DMA,
                pltpu.SemaphoreType.DMA((ncomp,)),
                pltpu.SemaphoreType.DMA((ncomp,)),
                pltpu.SemaphoreType.DMA((ncomp,)),
                pltpu.SemaphoreType.DMA((ncomp,)),
            ],
            compiler_params=pltpu.CompilerParams(
                collective_id=0, has_side_effects=True, vmem_limit_bytes=56 * 1024 * 1024),
        )(spectrum, sea_mask.reshape(1, points), neighbours, substeps, courant,
          spread(np.cos(angles)), spread(np.sin(angles)), source_operator)

    placed = (
        P("comp", ("members", "lat", "sub")),
        P(("members", "lat", "sub")),
        P(None, ("members", "lat", "sub")),
        P(),
        P(),
        P("sub", None),
    )
    return jax.shard_map(
        per_device,
        mesh=mesh,
        in_specs=placed,
        out_specs=P("comp", ("members", "lat", "sub")),
        check_vma=False,
    )
```

```python
import functools
import math

import jax
import jax.numpy as jnp
import numpy as np
from jax import lax
from jax.experimental import pallas as pl
from jax.experimental.pallas import tpu as pltpu
from jax.sharding import PartitionSpec as P

NF = 30
ND = 64
NLON = 256
MAXSTEPS = 6
SRC_STEPS = 4
STEP_SIZE = 0.1
MESH = pl.DeviceIdType.MESH
HALF = ND // 2
TILES = 4
SLOTS = 8
NEAR = 2
FAR = 2
BACK = 5
AHEAD = 2
PIECES = 2
F32 = jnp.float32
BF16 = jnp.bfloat16


def kernel(
    nlat, ncomp, group, spec_ref, mask_ref, nb_ref, steps_ref, cour_ref, cos_ref, sin_ref, op_ref,
    out_ref, w_ref, own_ref, halo_ref, code_ref, prop_ref, away_ref, got_ref, start_ref, state_ref,
    low_ref, inc_ref, home_ref,
    h_send, h_recv, w_send, w_recv, w_local, a_send, a_recv, b_send, b_recv,
):
    lat = lax.axis_index("lat")
    sub = lax.axis_index("sub")
    me = lax.axis_index("comp")
    bins, points = spec_ref.shape
    chunks, size = prop_ref.shape[0], prop_ref.shape[1]
    planes = size // 8
    share = points // ncomp
    total = bins * ncomp
    half_rows = total // 2
    first = me * bins
    last_lat = nlat - 1
    partner = {"sub": 1 - sub}

    barrier = pltpu.get_barrier_semaphore()
    peers = [partner]
    if nlat == 2:
        peers.append({"lat": 1 - lat})
    else:
        for move in (1, -1):
            peers.append({"lat": lax.rem(lat + move + nlat, nlat)})
            peers.append({"lat": lax.rem(lat + 2 * move + nlat, nlat), "sub": 1 - sub})
    for j in range(1, ncomp):
        peers.append({"comp": lax.rem(me + j, ncomp)})
    for peer in peers:
        pl.semaphore_signal(barrier, inc=1, device_id=peer, device_id_type=MESH)

    own_half = pl.ds(pl.multiple_of(sub * half_rows, 16), half_rows)
    load_w = pltpu.make_async_copy(op_ref, w_ref.at[own_half], w_local)
    load_w.start()

    lane = lax.broadcasted_iota(jnp.int32, (1, points), 1)
    column = lane & (NLON - 1)
    position = (lat * 2 + sub) * points + lane
    sea = mask_ref[...].astype(F32)
    west = (column - nb_ref[0:1, :]) & (NLON - 1)
    east = (nb_ref[1:2, :] - column) & (NLON - 1)

    def vertical(index_row):
        moved = ((index_row - column + 1) & (NLON - 1)) - 1
        return jnp.where(index_row == position, 2, moved)

    rows = lax.broadcasted_iota(jnp.int32, (size, points), 0)
    codes = jnp.zeros((size, points), F32)
    entries = [west, east, vertical(nb_ref[2:3, :]), vertical(nb_ref[3:4, :])]
    for k, entry in enumerate([e.astype(F32) for e in entries] + [sea]):
        codes = jnp.where(rows == k, jnp.broadcast_to(entry, (size, points)), codes)
    own_ref[0] = codes.astype(BF16)
    own_ref[1] = codes.astype(BF16)

    pl.semaphore_wait(barrier, len(peers))

    def kind(q):
        return lax.rem(lax.div(first + (q - 2) * size, HALF), 2)

    def has_from(ty, far):
        return jnp.where(ty == 0, lat >= far, lat <= last_lat - far)

    def has_to(ty, far):
        return jnp.where(ty == 0, lat <= last_lat - far, lat >= far)

    def pair_copy(q):
        return pltpu.make_async_remote_copy(
            src_ref=own_ref.at[q], dst_ref=halo_ref.at[0, q], send_sem=h_send.at[0, q],
            recv_sem=h_recv.at[0, q], device_id=partner, device_id_type=MESH)

    def side_copy(q, ty):
        to = jnp.clip(lat + 1 - 2 * ty, 0, last_lat)
        return pltpu.make_async_remote_copy(
            src_ref=own_ref.at[q], dst_ref=halo_ref.at[1, q], send_sem=h_send.at[1, q],
            recv_sem=h_recv.at[1, q], device_id={"lat": to}, device_id_type=MESH)

    def hand_copy(q, ty):
        slot = jnp.where(sub == ty, 2, 0)
        return pltpu.make_async_remote_copy(
            src_ref=halo_ref.at[1, q], dst_ref=halo_ref.at[slot, q], send_sem=h_send.at[2, q],
            recv_sem=h_recv.at[2, q], device_id=partner, device_id_type=MESH)

    def far_copy(q, ty):
        to = jnp.clip(lat + 2 - 4 * ty, 0, last_lat)
        return pltpu.make_async_remote_copy(
            src_ref=own_ref.at[q], dst_ref=halo_ref.at[2, q], send_sem=h_send.at[3, q],
            recv_sem=h_recv.at[3, q], device_id={"lat": to, "sub": 1 - sub}, device_id_type=MESH)

    def send_own(q, ty):
        @pl.when(has_to(ty, 1))
        def _():
            side_copy(q, ty).start()

        @pl.when(sub == ty)
        def _():
            pair_copy(q).start()

        if nlat > 2:
            @pl.when((sub != ty) & has_to(ty, 2))
            def _():
                far_copy(q, ty).start()

    def hand_on(q, ty):
        @pl.when(has_from(ty, 1))
        def _():
            side_copy(q, ty).wait_recv()
            hand_copy(q, ty).start()

    def arrive(q, ty):
        @pl.when(has_from(ty, 1))
        def _():
            hand_copy(q, ty).wait_recv()

        @pl.when(sub != ty)
        def _():
            pair_copy(q).wait_recv()

        if nlat > 2:
            @pl.when((sub == ty) & has_from(ty, 2))
            def _():
                far_copy(q, ty).wait_recv()

    def sent(q, ty):
        @pl.when(has_to(ty, 1))
        def _():
            side_copy(q, ty).wait_send()

        @pl.when(sub == ty)
        def _():
            pair_copy(q).wait_send()

        if nlat > 2:
            @pl.when((sub != ty) & has_to(ty, 2))
            def _():
                far_copy(q, ty).wait_send()

        @pl.when(has_from(ty, 1))
        def _():
            hand_copy(q, ty).wait_send()

    send_own(0, 0)
    send_own(1, 1)

    def prepare(i, carry):
        chunk = sea * spec_ref[pl.ds(pl.multiple_of(i * size, size), size), :]
        own_ref[i + 2] = chunk.astype(BF16)
        send_own(i + 2, kind(i + 2))
        return carry

    lax.fori_loop(0, chunks, prepare, 0)

    give_w = pltpu.make_async_remote_copy(
        src_ref=op_ref, dst_ref=w_ref.at[own_half], send_sem=w_send, recv_sem=w_recv,
        device_id=partner, device_id_type=MESH)
    give_w.start()

    for q in (0, 1):
        hand_on(q, q)
    ahead = min(6, chunks)
    for q in range(2, 2 + ahead):
        hand_on(q, kind(q))

    for ty in (0, 1):
        arrive(ty, ty)
        for slot in range(SLOTS):
            row = slot % 2 if ty == 0 else 1 - slot % 2
            cols = slice(row * NLON, (row + 1) * NLON)
            if slot < 6:
                part = halo_ref[2 - slot // 2, ty, :, cols].astype(F32)
            else:
                part = own_ref[ty, :, cols].astype(F32)
            for k, source in enumerate((0, 1, 2 + ty, 4)):
                code_ref[ty, slot, k] = jnp.broadcast_to(part[source:source + 1, :], (8, NLON))

    def propagate(i):
        q = i + 2
        ty = kind(q)

        @pl.when(i + ahead < chunks)
        def _():
            hand_on(q + ahead, kind(q + ahead))

        arrive(q, ty)
        bin0 = first + i * size
        freq = lax.div(bin0, ND)
        direction = lax.rem(bin0, ND)
        to_east = jnp.where((direction < ND // 4) | (direction >= 3 * ND // 4), 1, 0)
        steps = steps_ref[freq]
        speed = cour_ref[freq]
        sign = jnp.where(to_east == 1, 1.0, -1.0)
        shift1 = jnp.where(to_east == 1, 1, NLON - 1)
        shift2 = jnp.where(to_east == 1, 2, NLON - 2)
        back1 = NLON - shift1
        d8 = lax.div(direction, 8)
        abs_cos = cos_ref[pl.ds(d8, planes)]
        abs_sin = sin_ref[pl.ds(d8, planes)]

        def lanes(slot):
            row = jnp.where(ty == 0, slot % 2, 1 - slot % 2)
            return pl.ds(pl.multiple_of(row * NLON, NLON), NLON)

        values = []
        for slot in range(SLOTS):
            if slot < 6:
                part = halo_ref[2 - slot // 2, q, :, lanes(slot)].astype(F32)
            else:
                part = spec_ref[pl.ds(pl.multiple_of(i * size, size), size), lanes(slot)]
            part = part.reshape(planes, 8, NLON)
            if slot >= 6:
                part = part * code_ref[ty, slot, 3][None]
            values.append(part)
        for t in range(MAXSTEPS):
            live = jnp.where(t < steps, speed, 0.0)
            wx = live * abs_cos
            wy = live * abs_sin
            keep = 1.0 - wx - wy
            fresh = list(values)
            for slot in range(t + 1, SLOTS):
                x = values[slot]
                below = values[slot - 1]
                near = code_ref[ty, slot, 1 - to_east][None] == 1.0
                vert = code_ref[ty, slot, 2][None] * sign
                lon = jnp.where(near, pltpu.roll(x, shift1, 2), pltpu.roll(x, shift2, 2))
                up = jnp.where(vert == -1.0, pltpu.roll(below, shift1, 2),
                               jnp.where(vert == 1.0, pltpu.roll(below, back1, 2), below))
                up = jnp.where(jnp.abs(vert) == 2.0, x, up)
                fresh[slot] = code_ref[ty, slot, 3][None] * (keep * x + wx * lon + wy * up)
            values = fresh
        for slot in (6, 7):
            prop_ref[i, :, lanes(slot)] = values[slot].reshape(size, NLON)
        whole = prop_ref[i]
        for c in range(ncomp):
            away_ref[c, i] = whole[:, c * share:(c + 1) * share].astype(BF16)

    groups = chunks // group

    def out_copy(j, g):
        to = lax.rem(me + j, ncomp)
        span = pl.ds(g * group, group)
        return pltpu.make_async_remote_copy(
            src_ref=away_ref.at[to, span], dst_ref=got_ref.at[me, span],
            send_sem=a_send.at[j], recv_sem=a_recv.at[j],
            device_id={"comp": to}, device_id_type=MESH)

    def whole_copy(j):
        to = lax.rem(me + j, ncomp)
        return pltpu.make_async_remote_copy(
            src_ref=away_ref.at[to], dst_ref=got_ref.at[me],
            send_sem=a_send.at[j], recv_sem=a_recv.at[j],
            device_id={"comp": to}, device_id_type=MESH)

    def run_group(g, carry):
        def one(i, inner):
            propagate(g * group + i)
            return inner

        lax.fori_loop(0, group, one, 0)
        for j in range(1, ncomp):
            out_copy(j, g).start()
        return carry

    lax.fori_loop(0, groups, run_group, 0)

    for q in (0, 1):
        sent(q, q)

    def drain(q, carry):
        sent(q, kind(q))
        return carry

    lax.fori_loop(2, chunks + 2, drain, 0)
    got_ref[me] = away_ref[me]
    load_w.wait()
    give_w.wait()

    for j in range(1, ncomp):
        whole_copy(j).wait()
    for c in range(ncomp):
        start_ref[c * bins:(c + 1) * bins, :] = got_ref[c].astype(F32).reshape(bins, share)
    tile = total // TILES
    per_tile = bins // tile if bins >= tile else tile // bins
    for m in range(TILES):
        span = slice(m * tile, (m + 1) * tile)
        low_ref[0, span, :] = start_ref[span, :].astype(BF16)

    def tile_rows(m):
        return pl.ds(pl.multiple_of(m * tile, 16), tile)

    def advance(step, m):
        span = tile_rows(m)
        driving = jnp.dot(w_ref[span, :], low_ref[step % 2], preferred_element_type=F32)
        now = start_ref[span, :] if step == 0 else state_ref[span, :]
        return span, now + STEP_SIZE * now * driving

    for step in range(SRC_STEPS - 1):
        def one_tile(m, carry, step=step):
            span, now = advance(step, m)
            state_ref[span, :] = now
            low_ref[(step + 1) % 2, span, :] = now.astype(BF16)
            return carry

        lax.fori_loop(0, TILES, one_tile, 0)

    def home_copy(j, to):
        return pltpu.make_async_remote_copy(
            src_ref=inc_ref.at[to], dst_ref=home_ref.at[me],
            send_sem=b_send.at[j], recv_sem=b_recv.at[j],
            device_id={"comp": to}, device_id_type=MESH)

    mine = lax.div(me * TILES, ncomp)

    def last_tile(i, carry):
        m = lax.rem(mine + 1 + i, TILES)
        span, now = advance(SRC_STEPS - 1, m)
        gain = now - start_ref[span, :]
        for k in range(per_tile):
            to = m * per_tile + k
            inc_ref[to] = gain[k * bins:(k + 1) * bins, :].astype(BF16)
            j = lax.rem(to - me + ncomp, ncomp)

            @pl.when(to != me)
            def _():
                home_copy(j, to).start()

        return carry

    lax.fori_loop(0, TILES, last_tile, 0)
    home_ref[me] = inc_ref[me]
    for c in range(ncomp):
        j = lax.rem(me - c + ncomp, ncomp)

        @pl.when(me != c)
        def _():
            home_copy(j, lax.rem(me + j, ncomp)).wait()

        cols = slice(c * share, (c + 1) * share)
        before = prop_ref[:, :, cols].reshape(bins, share)
        out_ref[:, cols] = sea[:, cols] * (before + home_ref[c].astype(F32))


def fast_kernel(
    ncomp, spec_ref, mask_hbm, nb_hbm, steps_hbm, cour_hbm, op_ref,
    out_ref, mask_ref, nb_ref, steps_ref, cour_ref, w_ref, full_ref, oth_ref, hsend_ref, halo_ref, code_ref, ang_ref, perm_ref,
    pout_ref, pin_ref, away_ref, x_ref, start_ref, state_ref, inc_ref, home_ref,
    l_sem, i_sem, w_sem, c_send, c_recv, r_send, r_recv, g_send, g_recv, h_send, h_recv,
    a_send, a_recv, t_send, t_recv, o_sem, p_send, p_recv, b_send, b_recv,
):
    lat = lax.axis_index("lat")
    sub = lax.axis_index("sub")
    me = lax.axis_index("comp")
    groups = spec_ref.shape[0]
    bins = groups * 2 * 16
    kmax = halo_ref.shape[0]
    lanes = NLON // 2
    total = bins * ncomp
    partner = {"sub": 1 - sub}
    others = [partner, {"lat": 1 - lat}, {"lat": 1 - lat, "sub": 1 - sub}]

    small = [pltpu.make_async_copy(src, dst, i_sem.at[n]) for n, (src, dst) in enumerate((
        (mask_hbm, mask_ref.at[lat, sub]), (nb_hbm, nb_ref.at[lat, sub]),
        (steps_hbm, steps_ref), (cour_hbm, cour_ref)))]
    loads = []
    for r in range(2):
        cols = slice(r * NLON, (r + 1) * NLON)
        loads.append(pltpu.make_async_copy(
            spec_ref.at[:, 1 - sub, :, cols], oth_ref.at[pl.ds(0, groups), r], l_sem.at[r]))
        loads.append(pltpu.make_async_copy(
            spec_ref.at[:, sub, :, cols], full_ref.at[pl.ds(0, groups), 2 * sub + r], l_sem.at[2 + r]))
    for load in (small[0], *loads, *small[1:]):
        load.start()
    own_half = pl.ds(pl.multiple_of(sub * (total // 2), 16), total // 2)
    load_w = pltpu.make_async_copy(op_ref, w_ref.at[own_half], w_sem)

    barrier = pltpu.get_barrier_semaphore()
    peers = list(others)
    for d in range(1, ncomp):
        z = lax.rem(me + d, ncomp)
        peers += [{"comp": z}, {"comp": z, "sub": 1 - sub}]
    for peer in peers:
        pl.semaphore_signal(barrier, inc=1, device_id=peer, device_id_type=MESH)

    a = lax.broadcasted_iota(jnp.int32, (NLON, NLON), 0)
    b = lax.broadcasted_iota(jnp.int32, (NLON, NLON), 1)
    split = lambda c: jnp.where(c < lanes, 2 * c, 2 * (c - lanes) + 1)
    perm_ref[0] = (a == split(b)).astype(F32).astype(BF16)
    perm_ref[1] = (b == split(a)).astype(F32).astype(BF16)

    near_ty = lat
    far_ty = 1 - lat
    n0 = lax.rem(lat + me * groups, 2)
    f0 = 1 - n0
    for q, ty in enumerate((near_ty, far_ty)):
        d = lax.broadcasted_iota(jnp.int32, (16, lanes), 0) + 16 * (2 * ty + sub)
        angle = (d.astype(F32) + 0.5) * np.float32(2.0 * math.pi / ND)
        ang_ref[q, 0] = jnp.abs(jnp.cos(angle))
        ang_ref[q, 1] = jnp.abs(jnp.sin(angle))

    def point_copies(n):
        return [pltpu.make_async_remote_copy(
            src_ref=ref.at[lat, sub], dst_ref=ref.at[lat, sub], send_sem=c_send.at[n, m],
            recv_sem=c_recv.at[n, m], device_id=others[n], device_id_type=MESH)
            for m, ref in enumerate((mask_ref, nb_ref))]

    cut = 4 * NEAR

    def raw_copies(core):
        return [pltpu.make_async_remote_copy(
            src_ref=oth_ref.at[pl.ds(a, n)], dst_ref=full_ref.at[pl.ds(a, n), pl.ds(2 * core, 2)],
            send_sem=r_send.at[part], recv_sem=r_recv.at[part], device_id=partner, device_id_type=MESH)
            for part, (a, n) in enumerate(((0, cut), (cut, groups - cut)))]

    small[0].wait()
    small[1].wait()
    sea = mask_ref[lat, sub].astype(F32)
    for load in loads:
        load.wait()
    sea_rows = [jnp.broadcast_to(sea[:, r * NLON:(r + 1) * NLON], (16, NLON)) for r in range(2)]

    def convert(k, carry):
        j = n0 + 2 * k
        for r in range(2):
            mine = full_ref[j, 2 * sub + r] * sea_rows[r]
            other = oth_ref[j, r] * sea_rows[r]
            hsend_ref[k, sub, r] = mine.astype(BF16)
            hsend_ref[k, 1 - sub, r] = other.astype(BF16)
        return carry

    lax.fori_loop(0, kmax, convert, 0)
    pl.semaphore_wait(barrier, len(peers))
    def halo_copy(k, p):
        return pltpu.make_async_remote_copy(
            src_ref=hsend_ref.at[k, p], dst_ref=halo_ref.at[k, pl.ds(2 * sub, 2)],
            send_sem=h_send.at[k, p], recv_sem=h_recv.at[k, sub],
            device_id={"lat": 1 - lat, "sub": p}, device_id_type=MESH)

    def halo_wait(k, s):
        pltpu.make_async_remote_copy(
            src_ref=hsend_ref.at[k, s], dst_ref=halo_ref.at[k, pl.ds(2 * s, 2)],
            send_sem=h_send.at[k, s], recv_sem=h_recv.at[k, s],
            device_id={"lat": 1 - lat, "sub": s}, device_id_type=MESH).wait_recv()

    def give_w():
        return pltpu.make_async_remote_copy(
            src_ref=op_ref, dst_ref=w_ref.at[own_half], send_sem=g_send, recv_sem=g_recv,
            device_id=partner, device_id_type=MESH)

    def take_w():
        other_half = pl.ds(pl.multiple_of((1 - sub) * (total // 2), 16), total // 2)
        return pltpu.make_async_remote_copy(
            src_ref=op_ref, dst_ref=w_ref.at[other_half], send_sem=g_send, recv_sem=g_recv,
            device_id=partner, device_id_type=MESH)

    def send_halo(k, carry):
        @pl.when(n0 + 2 * k < groups)
        def _():
            for p in range(2):
                halo_copy(k, p).start()
        return carry

    for copy in point_copies(0):
        copy.start()
    lax.fori_loop(0, AHEAD, send_halo, 0)
    for copy in (*raw_copies(sub), *point_copies(1), *point_copies(2)):
        copy.start()
    lax.fori_loop(AHEAD, kmax, send_halo, 0)
    load_w.start()
    give_w().start()
    for load in small[2:]:
        load.wait()

    points = mask_ref.shape[-1]
    lane = lax.broadcasted_iota(jnp.int32, (1, points), 1)
    column = lane & (NLON - 1)
    index = lax.broadcasted_iota(jnp.int32, (8, points), 0)

    def decode(chip):
        for s in range(2):
            nb = nb_ref[chip, s]
            west = (column - nb[0:1, :]) & (NLON - 1)
            east = (nb[1:2, :] - column) & (NLON - 1)
            moves = [((nb[k:k + 1, :] - column + 1) & (NLON - 1)) - 1 for k in (2, 3)]
            codes = jnp.zeros((8, points), F32)
            for k, entry in enumerate((west, east, *moves, mask_ref[chip, s])):
                codes = jnp.where(index == k, jnp.broadcast_to(entry.astype(F32), (8, points)), codes)
            for r in range(2):
                part = codes[:, r * NLON:(r + 1) * NLON].astype(BF16)
                both = jnp.dot(part, perm_ref[0], preferred_element_type=F32)
                for k in range(5):
                    code_ref[chip, 2 * s + r, k] = jnp.broadcast_to(both[k:k + 1, :], (8, NLON))

    side = lax.div(me, 2)

    def target(i):
        near = me + 1 - 2 * lax.rem(me, 2)
        return jnp.where(i == 0, 3 - 3 * side, jnp.where(i == 1, 2 - side, jnp.where(i == 2, near, me)))

    def outward(i):
        k = lax.rem(i + 2, 3)
        return target(jnp.where((side == 0) & (sub == 0) & (i < 3), k, i))

    def chunk_copy(h, j, to):
        return pltpu.make_async_remote_copy(
            src_ref=away_ref.at[h, to, j], dst_ref=x_ref.at[0, me * groups + j, sub, :, 0:lanes],
            send_sem=a_send.at[h, to], recv_sem=a_recv.at[me, sub],
            device_id={"comp": to, "sub": h}, device_id_type=MESH)

    def whole_copy(h, to):
        return pltpu.make_async_remote_copy(
            src_ref=away_ref.at[h, to, pl.ds(0, groups)],
            dst_ref=x_ref.at[0, pl.ds(me * groups, groups), sub, :, 0:lanes],
            send_sem=a_send.at[h, to], recv_sem=a_recv.at[me, sub],
            device_id={"comp": to, "sub": h}, device_id_type=MESH)

    def whole_wait(z, s):
        pltpu.make_async_remote_copy(
            src_ref=away_ref.at[0, z, pl.ds(0, groups)],
            dst_ref=x_ref.at[0, pl.ds(z * groups, groups), s, :, 0:lanes],
            send_sem=a_send.at[0, 0], recv_sem=a_recv.at[z, s],
            device_id={"comp": z, "sub": s}, device_id_type=MESH).wait_recv()

    def pick(ty, i):
        return ty * 3 + (1 - 2 * ty) * i

    def separate(x):
        high = x.astype(BF16)
        low = (x - high.astype(F32)).astype(BF16)
        return high, low

    def propagate(ks, far, to_east):
        ty = far_ty if far else near_ty
        js = [(f0 if far else n0) + 2 * k for k in ks]
        vert = 2 + ty
        lowest = 0 if far else 4

        def code(q, k, half):
            chip = lat if q >= 4 else 1 - lat
            part = code_ref[chip, pick(ty, q % 4), k, :, half * lanes:(half + 1) * lanes]
            return jnp.concatenate([part, part], axis=0)

        raw = jnp.concatenate([full_ref[j, pick(ty, i)] for j in js for i in range(4)], axis=0)
        high, low = separate(raw)
        mixed = (jnp.dot(high, perm_ref[0], preferred_element_type=F32)
                 + jnp.dot(low, perm_ref[0], preferred_element_type=F32))
        if far:
            edge = jnp.concatenate([halo_ref[k, pick(ty, i)] for k in ks for i in range(4)], axis=0)
            edge = jnp.dot(edge, perm_ref[0], preferred_element_type=F32)
        cells = []
        weights = []
        for n, j in enumerate(js):
            values = [None] * 8
            for i in range(4):
                rows = slice((n * 4 + i) * 16, (n * 4 + i + 1) * 16)
                values[4 + i] = tuple(
                    mixed[rows, half * lanes:(half + 1) * lanes] * code(4 + i, 4, half)
                    for half in range(2))
                if far:
                    values[i] = tuple(edge[rows, half * lanes:(half + 1) * lanes] for half in range(2))
            cells.append(values)
            freq = jnp.minimum(lax.div(me * bins + j * 32, ND), steps_ref.shape[0] - 1)
            weights.append((steps_ref[freq], cour_ref[freq]))
        abs_cos, abs_sin = ang_ref[int(far), 0], ang_ref[int(far), 1]
        ahead, behind = (1, lanes - 1)
        for t in range(MAXSTEPS):
            slots = [q for q in range(7, lowest - 1, -1) if q >= 4 or t <= q + 1]
            for n, (steps, speed) in enumerate(weights):
                live = jnp.where(t < steps, speed, 0.0)
                wx = live * abs_cos
                wy = live * abs_sin
                keep = 1.0 - wx - wy
                values = cells[n]
                fresh = list(values)
                turned = {}

                def turn(q, half, shift):
                    key = (q, half, shift)
                    if key not in turned:
                        turned[key] = pltpu.roll(values[q][half], shift, 1)
                    return turned[key]

                def left(q):
                    return turn(q, 1, ahead), values[q][0]

                def right(q):
                    return values[q][1], turn(q, 0, behind)

                for q in slots:
                    shift = ahead if to_east else behind
                    one = left(q) if to_east else right(q)
                    lon_code = 0 if to_east else 1
                    new = []
                    for half in range(2):
                        x = values[q][half]
                        lon = jnp.where(code(q, lon_code, half) == 1.0, one[half], turn(q, half, shift))
                        if q == lowest:
                            up = x
                        else:
                            move = code(q, vert, half)
                            up = jnp.where(move == -1.0, left(q - 1)[half],
                                           jnp.where(move == 1.0, right(q - 1)[half], values[q - 1][half]))
                        new.append(code(q, 4, half) * (keep * x + wx * lon + wy * up))
                    fresh[q] = tuple(new)
                cells[n] = fresh
        for n, j in enumerate(js):
            for i in range(4):
                r = pick(ty, i)
                for half in range(2):
                    value = cells[n][4 + i][half]
                    pout_ref[j, r, :, half * lanes:(half + 1) * lanes] = value
                    away_ref[lax.div(r, 2), 2 * lax.rem(r, 2) + half, j] = value.astype(BF16)
        for n, j in enumerate(js):
            @pl.when(j < groups)
            def _():
                for i in range(ncomp - 1):
                    chunk_copy(0, j, target(i)).start()

    straight = sub == lat
    for copy in point_copies(0):
        copy.wait_recv()
    decode(lat)
    raw_copies(1 - sub)[0].wait_recv()

    def near_body(g, carry):
        @pl.when(g == 2)
        def _():
            raw_copies(1 - sub)[1].wait_recv()

        ks = [g * NEAR + n for n in range(NEAR)]

        @pl.when(straight)
        def _():
            propagate(ks, False, True)

        @pl.when(jnp.logical_not(straight))
        def _():
            propagate(ks, False, False)
        return carry

    lax.fori_loop(0, kmax // NEAR, near_body, 0)
    for n in (1, 2):
        for copy in point_copies(n):
            copy.wait_recv()
    decode(1 - lat)

    eager = 3 - 2 * side
    patient = 2 - 2 * side

    def far_body(g, carry):
        ks = [g * FAR + n for n in range(FAR)]
        for k in ks:
            @pl.when(f0 + 2 * k < groups)
            def _():
                for s in range(2):
                    halo_wait(k, s)

        @pl.when(straight)
        def _():
            propagate(ks, True, False)

        @pl.when(jnp.logical_not(straight))
        def _():
            propagate(ks, True, True)

        for k in ks:
            @pl.when(n0 + 2 * k < groups)
            def _():
                chunk_copy(1, n0 + 2 * k, eager).start()
        return carry

    lax.fori_loop(0, kmax // FAR, far_body, 0)

    own_copy = pltpu.make_async_copy(
        away_ref.at[sub, me, pl.ds(0, groups)], x_ref.at[0, pl.ds(me * groups, groups), sub, :, 0:lanes], o_sem.at[0])

    def cross_copy():
        return pltpu.make_async_remote_copy(
            src_ref=away_ref.at[1 - sub, me, pl.ds(0, groups)],
            dst_ref=x_ref.at[0, pl.ds(me * groups, groups), sub, :, 0:lanes],
            send_sem=a_send.at[0, me], recv_sem=a_recv.at[me, sub],
            device_id=partner, device_id_type=MESH)

    def prop_copy():
        return pltpu.make_async_remote_copy(
            src_ref=pout_ref.at[pl.ds(0, groups), pl.ds(2 * (1 - sub), 2)],
            dst_ref=pin_ref, send_sem=p_send, recv_sem=p_recv,
            device_id=partner, device_id_type=MESH)

    own_copy.start()
    cross_copy().start()

    def send_rest(k, carry):
        @pl.when(f0 + 2 * k < groups)
        def _():
            chunk_copy(1, f0 + 2 * k, eager).start()
        return carry

    lax.fori_loop(0, kmax, send_rest, 0)

    wide = (sub == 1) & (lax.div(me + 1, 2) == 1)

    def twin_copy(block, to):
        return pltpu.make_async_remote_copy(
            src_ref=away_ref.at[1, block, pl.ds(0, groups)],
            dst_ref=x_ref.at[0, pl.ds(me * groups, groups), sub, :, lanes:2 * lanes],
            send_sem=t_send.at[block], recv_sem=t_recv.at[me, sub],
            device_id={"comp": to, "sub": 1}, device_id_type=MESH)

    def twin_local(block):
        return pltpu.make_async_copy(
            away_ref.at[1, block, pl.ds(0, groups)],
            x_ref.at[0, pl.ds(me * groups, groups), sub, :, lanes:2 * lanes], o_sem.at[1])

    def twin_wait(z, s):
        pltpu.make_async_remote_copy(
            src_ref=away_ref.at[1, 0, pl.ds(0, groups)],
            dst_ref=x_ref.at[0, pl.ds(z * groups, groups), s, :, lanes:2 * lanes],
            send_sem=t_send.at[0], recv_sem=t_recv.at[z, s],
            device_id={"comp": z, "sub": s}, device_id_type=MESH).wait_recv()

    def twin_here(to):
        return (me == to) & (sub == 1)

    def send_twin(block, to):
        @pl.when(jnp.logical_not(twin_here(to)))
        def _():
            twin_copy(block, to).start()

        @pl.when(twin_here(to))
        def _():
            twin_local(block).start()

    send_twin(2, 1)
    whole_copy(1, target(2)).start()
    whole_copy(1, patient).start()
    send_twin(1, 2)
    prop_copy().start()

    piece = bins // PIECES

    def home_copy(source, block, to, start, size):
        span = pl.ds(pl.multiple_of(start, 16), size)
        return pltpu.make_async_remote_copy(
            src_ref=inc_ref.at[source, span], dst_ref=home_ref.at[block, span],
            send_sem=b_send.at[source], recv_sem=b_recv.at[block],
            device_id={"comp": to}, device_id_type=MESH)

    early = (2 * bins) // 128 * 128
    late = total - early

    once = 1 + lax.div(me, ncomp)

    def integrate(width):
        def partial(start, span, use):
            def one(i, carry):
                rows = pl.ds(pl.multiple_of(i * total, 16), total)
                field = x_ref[0, pl.ds(lax.div(start, 32), span // 32), :, :, 0:width].reshape(span, width)
                cols = pl.ds(pl.multiple_of(start, 128), span)
                use(rows, jnp.dot(w_ref[rows, cols], field, preferred_element_type=F32))
                return carry

            lax.fori_loop(0, once, one, 0)

        def begin(rows, driving):
            state_ref[rows, 0:width] = driving

        def first_step(rows, driving):
            start = x_ref[0, :, :, :, 0:width].reshape(total, width).astype(F32)
            now = start + STEP_SIZE * start * (state_ref[rows, 0:width] + driving)
            start_ref[rows, 0:width] = start
            state_ref[rows, 0:width] = now
            x_ref[1, :, :, :, 0:width] = now.astype(BF16).reshape(ncomp * groups, 2, 16, width)

        def advance(step, carry):
            field = x_ref[lax.rem(step, 2), :, :, :, 0:width].reshape(total, width)
            driving = jnp.dot(w_ref[...], field, preferred_element_type=F32)
            now = state_ref[:, 0:width]
            now = now + STEP_SIZE * now * driving
            state_ref[:, 0:width] = now
            x_ref[lax.rem(step + 1, 2), :, :, :, 0:width] = now.astype(BF16).reshape(
                ncomp * groups, 2, 16, width)
            return carry

        def last(m, start):
            rows = pl.ds(pl.multiple_of(m * bins + start, 16), piece)
            field = x_ref[(SRC_STEPS - 1) % 2, :, :, :, 0:width].reshape(total, width)
            driving = jnp.dot(w_ref[rows, :], field, preferred_element_type=F32)
            now = state_ref[rows, 0:width]
            now = now + STEP_SIZE * now * driving
            return (now - start_ref[rows, 0:width]).astype(BF16)

        def finish(n, carry):
            m = outward(lax.div(n, PIECES))
            start = lax.rem(n, PIECES) * piece
            span = pl.ds(pl.multiple_of(start, 16), piece)
            gain = last(m, start)

            @pl.when(m == me)
            def _():
                home_ref[me, span] = gain

            @pl.when(m != me)
            def _():
                inc_ref[m, span] = gain
                home_copy(m, me, m, start, piece).start()
            return carry

        def finish_wide(n, carry):
            m = target(lax.div(n, PIECES))
            start = lax.rem(n, PIECES) * piece
            span = pl.ds(pl.multiple_of(start, 16), piece)
            gain = last(m, start)
            blocks = ((me, gain[:, 0:lanes]), (3 - me, gain[:, lanes:2 * lanes]))

            @pl.when(m == me)
            def _():
                for block, part in blocks:
                    home_ref[block, span] = part

            @pl.when(m != me)
            def _():
                for source, (block, part) in enumerate(blocks):
                    inc_ref[source, span] = part
                    home_copy(source, block, m, start, piece).start()
            return carry

        both = width > lanes
        whole_wait(me, 1 - sub)
        for s in range(2):
            whole_wait(target(2), s)
        if both:
            twin_local(3 - me).wait()
            twin_wait(me, 0)
            for s in range(2):
                twin_wait(target(2), s)
        partial(side * late, early, begin)
        for i in (1, 0):
            for s in range(2):
                whole_wait(target(i), s)
                if both:
                    twin_wait(target(i), s)
        partial((1 - side) * early, late, first_step)
        lax.fori_loop(1, SRC_STEPS - 1, advance, 0)
        if both:
            lax.fori_loop((ncomp - 2) * PIECES, ncomp * PIECES, finish_wide, 0)
        else:
            lax.fori_loop(0, ncomp * PIECES, finish, 0)

    sea_wide = [jnp.broadcast_to(sea[:, r * NLON:(r + 1) * NLON], (16, NLON)) for r in range(2)]

    def restore(g, carry):
        js = [g * BACK + n for n in range(BACK)]
        parts = [ref for j in js for ref in (
            pout_ref[j, 2 * sub], pout_ref[j, 2 * sub + 1], pin_ref[j, 0], pin_ref[j, 1])]
        high, low = separate(jnp.concatenate(parts, axis=0))
        plain = (jnp.dot(high, perm_ref[1], preferred_element_type=F32)
                 + jnp.dot(low, perm_ref[1], preferred_element_type=F32))
        for n in range(4 * BACK):
            p = sub if n % 4 < 2 else 1 - sub
            rows = pl.ds(pl.multiple_of((2 * js[n // 4] + p) * 16, 16), 16)
            r = n % 2
            out_ref[rows, r * NLON:(r + 1) * NLON] = sea_wide[r] * plain[n * 16:(n + 1) * 16, :]
        return carry

    def restore_all():
        prop_copy().wait_recv()
        lax.fori_loop(0, groups // BACK, restore, 0)

    pl.when(sub == 1)(restore_all)
    load_w.wait()
    take_w().wait_recv()
    own_copy.wait()
    @pl.when(wide)
    def _():
        integrate(2 * lanes)

    @pl.when(jnp.logical_not(wide))
    def _():
        integrate(lanes)

    pl.when(sub == 0)(restore_all)
    for i in (3, 0, 2, 1):
        z = target(i)

        def land():
            pltpu.make_async_remote_copy(
                src_ref=inc_ref.at[z], dst_ref=home_ref.at[z],
                send_sem=b_send.at[z], recv_sem=b_recv.at[z],
                device_id={"comp": z}, device_id_type=MESH).wait_recv()

        if i < 3:
            pl.when(jnp.logical_not(wide & (z == 3 - me)))(land)
        r = lax.div(z, 2)
        half = lax.rem(z, 2)
        cols = pl.ds(pl.multiple_of(r * NLON, NLON), NLON)
        spread = perm_ref[1, pl.ds(pl.multiple_of(half * lanes, lanes), lanes), :]
        sea_row = jnp.where(r == 0, sea_wide[0][0:8], sea_wide[1][0:8])
        back = jnp.dot(home_ref[z], spread, preferred_element_type=F32)
        back = back.reshape(bins // 8, 8, NLON) * sea_row[None]
        out_ref[:, cols] = out_ref[:, cols] + back.reshape(bins, NLON)

    for n in range(3):
        for copy in point_copies(n):
            copy.wait_send()
    for copy in raw_copies(sub):
        copy.wait_send()

    def halo_left(k, carry):
        @pl.when(n0 + 2 * k < groups)
        def _():
            for p in range(2):
                halo_copy(k, p).wait_send()
        return carry

    lax.fori_loop(0, kmax, halo_left, 0)
    prop_copy().wait_send()
    cross_copy().wait_send()
    give_w().wait_send()
    for i in range(ncomp - 1):
        for h in range(2):
            whole_copy(h, target(i)).wait_send()

        @pl.when(jnp.logical_not(wide))
        def _():
            m = target(i)
            home_copy(m, me, m, 0, bins).wait_send()

    @pl.when(wide)
    def _():
        for source, block in enumerate((me, 3 - me)):
            home_copy(source, block, target(2), 0, bins).wait_send()

    for block, to in ((1, 2), (2, 1)):
        @pl.when(jnp.logical_not(twin_here(to)))
        def _():
            twin_copy(block, to).wait_send()


def write_kernel(src_ref, dst_ref, sems):
    pieces = sems.shape[0]
    rows = src_ref.shape[0] // pieces
    copies = [pltpu.make_async_copy(
        src_ref.at[pl.ds(i * rows, rows)], dst_ref.at[pl.ds(i * rows, rows)], sems.at[i])
        for i in range(pieces)]
    for copy in copies:
        copy.start()
    for copy in copies:
        copy.wait()


def fast_device(ncomp, spectrum, sea_mask, neighbours, substeps, courant, source_operator):
    bins, points = spectrum.shape
    groups = bins // 32
    kmax = (groups + 1) // 2
    lanes = NLON // 2
    total = bins * ncomp
    vmem = pl.BlockSpec(memory_space=pltpu.VMEM)
    hbm = pl.BlockSpec(memory_space=pltpu.HBM)
    dma = pltpu.SemaphoreType.DMA
    result = pl.pallas_call(
        functools.partial(fast_kernel, ncomp),
        out_shape=pltpu.VMEM((bins, points), F32),
        in_specs=[hbm] * 6,
        out_specs=vmem,
        scratch_shapes=[
            pltpu.VMEM((2, 2, 1, points), jnp.int32),
            pltpu.VMEM((2, 2, 4, points), jnp.int32),
            pltpu.SMEM(substeps.shape, jnp.int32),
            pltpu.SMEM(courant.shape, F32),
            pltpu.VMEM((total, total), BF16),
            pltpu.VMEM((2 * kmax, 4, 16, NLON), F32),
            pltpu.VMEM((2 * kmax, 2, 16, NLON), F32),
            pltpu.VMEM((kmax, 2, 2, 16, NLON), BF16),
            pltpu.VMEM((kmax, 4, 16, NLON), BF16),
            pltpu.VMEM((2, 4, 5, 8, NLON), F32),
            pltpu.VMEM((2, 2, 16, lanes), F32),
            pltpu.VMEM((2, NLON, NLON), BF16),
            pltpu.VMEM((2 * kmax, 4, 16, NLON), F32),
            pltpu.VMEM((groups, 2, 16, NLON), F32),
            pltpu.VMEM((2, ncomp, 2 * kmax, 16, lanes), BF16),
            pltpu.VMEM((2, ncomp * groups, 2, 16, 2 * lanes), BF16),
            pltpu.VMEM((total, 2 * lanes), F32),
            pltpu.VMEM((total, 2 * lanes), F32),
            pltpu.VMEM((ncomp, bins, lanes), BF16),
            pltpu.VMEM((ncomp, bins, lanes), BF16),
            dma((4,)), dma((4,)), dma, dma((3, 2)), dma((3, 2)), dma((2,)), dma((2,)), dma, dma,
            dma((kmax, 2)), dma((kmax, 2)), dma((2, ncomp)), dma((ncomp, 2)), dma((ncomp,)), dma((ncomp, 2)),
            dma((2,)), dma, dma,
            dma((ncomp,)), dma((ncomp,)),
        ],
        compiler_params=pltpu.CompilerParams(
            collective_id=1, has_side_effects=True, vmem_limit_bytes=60 * 1024 * 1024),
    )(spectrum.reshape(groups, 2, 16, points), sea_mask.reshape(1, points), neighbours, substeps, courant,
      source_operator)
    return pl.pallas_call(
        write_kernel,
        out_shape=jax.ShapeDtypeStruct((bins, points), F32),
        in_specs=[vmem],
        out_specs=hbm,
        scratch_shapes=[dma((4,))],
        compiler_params=pltpu.CompilerParams(vmem_limit_bytes=4 * 1024 * 1024),
    )(result)


def solution(mesh):
    nlat, ncomp = mesh.shape["lat"], mesh.shape["comp"]

    def per_device(spectrum, sea_mask, neighbours, substeps, courant, source_operator):
        bins, points = spectrum.shape
        even = bins % 32 == 0 and (bins // 32 + 1) // 2 % NEAR == 0 and bins // 32 % BACK == 0
        if nlat == 2 and ncomp == 4 and points == 2 * NLON and even:
            return fast_device(ncomp, spectrum, sea_mask, neighbours, substeps, courant, source_operator)
        size = 16 if bins % 16 == 0 else 8
        chunks = bins // size
        group = 5 if chunks % 5 == 0 else 1
        share = points // ncomp
        total = bins * ncomp
        angles = (np.arange(ND, dtype=np.float32) + np.float32(0.5)) * np.float32(2.0 * math.pi / ND)
        spread = lambda v: jnp.asarray(
            np.broadcast_to(np.abs(v).astype(np.float32)[:, None], (ND, NLON)).reshape(ND // 8, 8, NLON))
        vmem = pl.BlockSpec(memory_space=pltpu.VMEM)
        smem = pl.BlockSpec(memory_space=pltpu.SMEM)
        kinds = 3 if nlat == 2 else 4
        return pl.pallas_call(
            functools.partial(kernel, nlat, ncomp, group),
            out_shape=jax.ShapeDtypeStruct((bins, points), F32),
            in_specs=[vmem, vmem, vmem, smem, smem, vmem, vmem, pl.BlockSpec(memory_space=pl.ANY)],
            out_specs=vmem,
            scratch_shapes=[
                pltpu.VMEM((total, total), BF16),
                pltpu.VMEM((chunks + 2, size, points), BF16),
                pltpu.VMEM((3, chunks + 2, size, points), BF16),
                pltpu.VMEM((2, SLOTS, 4, 8, NLON), F32),
                pltpu.VMEM((chunks, size, points), F32),
                pltpu.VMEM((ncomp, chunks, size, share), BF16),
                pltpu.VMEM((ncomp, chunks, size, share), BF16),
                pltpu.VMEM((total, share), F32),
                pltpu.VMEM((total, share), F32),
                pltpu.VMEM((2, total, share), BF16),
                pltpu.VMEM((ncomp, bins, share), BF16),
                pltpu.VMEM((ncomp, bins, share), BF16),
                pltpu.SemaphoreType.DMA((kinds, chunks + 2)),
                pltpu.SemaphoreType.DMA((kinds, chunks + 2)),
                pltpu.SemaphoreType.DMA,
                pltpu.SemaphoreType.DMA,
                pltpu.SemaphoreType.DMA,
                pltpu.SemaphoreType.DMA((ncomp,)),
                pltpu.SemaphoreType.DMA((ncomp,)),
                pltpu.SemaphoreType.DMA((ncomp,)),
                pltpu.SemaphoreType.DMA((ncomp,)),
            ],
            compiler_params=pltpu.CompilerParams(
                collective_id=0, has_side_effects=True, vmem_limit_bytes=56 * 1024 * 1024),
        )(spectrum, sea_mask.reshape(1, points), neighbours, substeps, courant,
          spread(np.cos(angles)), spread(np.sin(angles)), source_operator)

    placed = (
        P("comp", ("members", "lat", "sub")),
        P(("members", "lat", "sub")),
        P(None, ("members", "lat", "sub")),
        P(),
        P(),
        P("sub", None),
    )
    return jax.shard_map(
        per_device,
        mesh=mesh,
        in_specs=placed,
        out_specs=P("comp", ("members", "lat", "sub")),
        check_vma=False,
    )
```

```python
import functools
import math

import jax
import jax.numpy as jnp
import numpy as np
from jax import lax
from jax.experimental import pallas as pl
from jax.experimental.pallas import tpu as pltpu
from jax.sharding import PartitionSpec as P

NF = 30
ND = 64
NLON = 256
MAXSTEPS = 6
SRC_STEPS = 4
STEP_SIZE = 0.1
MESH = pl.DeviceIdType.MESH
HALF = ND // 2
TILES = 4
SLOTS = 8
NEAR = 2
FAR = 2
BACK = 5
AHEAD = 2
PIECES = 2
F32 = jnp.float32
BF16 = jnp.bfloat16


def kernel(
    nlat, ncomp, group, spec_ref, mask_ref, nb_ref, steps_ref, cour_ref, cos_ref, sin_ref, op_ref,
    out_ref, w_ref, own_ref, halo_ref, code_ref, prop_ref, away_ref, got_ref, start_ref, state_ref,
    low_ref, inc_ref, home_ref,
    h_send, h_recv, w_send, w_recv, w_local, a_send, a_recv, b_send, b_recv,
):
    lat = lax.axis_index("lat")
    sub = lax.axis_index("sub")
    me = lax.axis_index("comp")
    bins, points = spec_ref.shape
    chunks, size = prop_ref.shape[0], prop_ref.shape[1]
    planes = size // 8
    share = points // ncomp
    total = bins * ncomp
    half_rows = total // 2
    first = me * bins
    last_lat = nlat - 1
    partner = {"sub": 1 - sub}

    barrier = pltpu.get_barrier_semaphore()
    peers = [partner]
    if nlat == 2:
        peers.append({"lat": 1 - lat})
    else:
        for move in (1, -1):
            peers.append({"lat": lax.rem(lat + move + nlat, nlat)})
            peers.append({"lat": lax.rem(lat + 2 * move + nlat, nlat), "sub": 1 - sub})
    for j in range(1, ncomp):
        peers.append({"comp": lax.rem(me + j, ncomp)})
    for peer in peers:
        pl.semaphore_signal(barrier, inc=1, device_id=peer, device_id_type=MESH)

    own_half = pl.ds(pl.multiple_of(sub * half_rows, 16), half_rows)
    load_w = pltpu.make_async_copy(op_ref, w_ref.at[own_half], w_local)
    load_w.start()

    lane = lax.broadcasted_iota(jnp.int32, (1, points), 1)
    column = lane & (NLON - 1)
    position = (lat * 2 + sub) * points + lane
    sea = mask_ref[...].astype(F32)
    west = (column - nb_ref[0:1, :]) & (NLON - 1)
    east = (nb_ref[1:2, :] - column) & (NLON - 1)

    def vertical(index_row):
        moved = ((index_row - column + 1) & (NLON - 1)) - 1
        return jnp.where(index_row == position, 2, moved)

    rows = lax.broadcasted_iota(jnp.int32, (size, points), 0)
    codes = jnp.zeros((size, points), F32)
    entries = [west, east, vertical(nb_ref[2:3, :]), vertical(nb_ref[3:4, :])]
    for k, entry in enumerate([e.astype(F32) for e in entries] + [sea]):
        codes = jnp.where(rows == k, jnp.broadcast_to(entry, (size, points)), codes)
    own_ref[0] = codes.astype(BF16)
    own_ref[1] = codes.astype(BF16)

    pl.semaphore_wait(barrier, len(peers))

    def kind(q):
        return lax.rem(lax.div(first + (q - 2) * size, HALF), 2)

    def has_from(ty, far):
        return jnp.where(ty == 0, lat >= far, lat <= last_lat - far)

    def has_to(ty, far):
        return jnp.where(ty == 0, lat <= last_lat - far, lat >= far)

    def pair_copy(q):
        return pltpu.make_async_remote_copy(
            src_ref=own_ref.at[q], dst_ref=halo_ref.at[0, q], send_sem=h_send.at[0, q],
            recv_sem=h_recv.at[0, q], device_id=partner, device_id_type=MESH)

    def side_copy(q, ty):
        to = jnp.clip(lat + 1 - 2 * ty, 0, last_lat)
        return pltpu.make_async_remote_copy(
            src_ref=own_ref.at[q], dst_ref=halo_ref.at[1, q], send_sem=h_send.at[1, q],
            recv_sem=h_recv.at[1, q], device_id={"lat": to}, device_id_type=MESH)

    def hand_copy(q, ty):
        slot = jnp.where(sub == ty, 2, 0)
        return pltpu.make_async_remote_copy(
            src_ref=halo_ref.at[1, q], dst_ref=halo_ref.at[slot, q], send_sem=h_send.at[2, q],
            recv_sem=h_recv.at[2, q], device_id=partner, device_id_type=MESH)

    def far_copy(q, ty):
        to = jnp.clip(lat + 2 - 4 * ty, 0, last_lat)
        return pltpu.make_async_remote_copy(
            src_ref=own_ref.at[q], dst_ref=halo_ref.at[2, q], send_sem=h_send.at[3, q],
            recv_sem=h_recv.at[3, q], device_id={"lat": to, "sub": 1 - sub}, device_id_type=MESH)

    def send_own(q, ty):
        @pl.when(has_to(ty, 1))
        def _():
            side_copy(q, ty).start()

        @pl.when(sub == ty)
        def _():
            pair_copy(q).start()

        if nlat > 2:
            @pl.when((sub != ty) & has_to(ty, 2))
            def _():
                far_copy(q, ty).start()

    def hand_on(q, ty):
        @pl.when(has_from(ty, 1))
        def _():
            side_copy(q, ty).wait_recv()
            hand_copy(q, ty).start()

    def arrive(q, ty):
        @pl.when(has_from(ty, 1))
        def _():
            hand_copy(q, ty).wait_recv()

        @pl.when(sub != ty)
        def _():
            pair_copy(q).wait_recv()

        if nlat > 2:
            @pl.when((sub == ty) & has_from(ty, 2))
            def _():
                far_copy(q, ty).wait_recv()

    def sent(q, ty):
        @pl.when(has_to(ty, 1))
        def _():
            side_copy(q, ty).wait_send()

        @pl.when(sub == ty)
        def _():
            pair_copy(q).wait_send()

        if nlat > 2:
            @pl.when((sub != ty) & has_to(ty, 2))
            def _():
                far_copy(q, ty).wait_send()

        @pl.when(has_from(ty, 1))
        def _():
            hand_copy(q, ty).wait_send()

    send_own(0, 0)
    send_own(1, 1)

    def prepare(i, carry):
        chunk = sea * spec_ref[pl.ds(pl.multiple_of(i * size, size), size), :]
        own_ref[i + 2] = chunk.astype(BF16)
        send_own(i + 2, kind(i + 2))
        return carry

    lax.fori_loop(0, chunks, prepare, 0)

    give_w = pltpu.make_async_remote_copy(
        src_ref=op_ref, dst_ref=w_ref.at[own_half], send_sem=w_send, recv_sem=w_recv,
        device_id=partner, device_id_type=MESH)
    give_w.start()

    for q in (0, 1):
        hand_on(q, q)
    ahead = min(6, chunks)
    for q in range(2, 2 + ahead):
        hand_on(q, kind(q))

    for ty in (0, 1):
        arrive(ty, ty)
        for slot in range(SLOTS):
            row = slot % 2 if ty == 0 else 1 - slot % 2
            cols = slice(row * NLON, (row + 1) * NLON)
            if slot < 6:
                part = halo_ref[2 - slot // 2, ty, :, cols].astype(F32)
            else:
                part = own_ref[ty, :, cols].astype(F32)
            for k, source in enumerate((0, 1, 2 + ty, 4)):
                code_ref[ty, slot, k] = jnp.broadcast_to(part[source:source + 1, :], (8, NLON))

    def propagate(i):
        q = i + 2
        ty = kind(q)

        @pl.when(i + ahead < chunks)
        def _():
            hand_on(q + ahead, kind(q + ahead))

        arrive(q, ty)
        bin0 = first + i * size
        freq = lax.div(bin0, ND)
        direction = lax.rem(bin0, ND)
        to_east = jnp.where((direction < ND // 4) | (direction >= 3 * ND // 4), 1, 0)
        steps = steps_ref[freq]
        speed = cour_ref[freq]
        sign = jnp.where(to_east == 1, 1.0, -1.0)
        shift1 = jnp.where(to_east == 1, 1, NLON - 1)
        shift2 = jnp.where(to_east == 1, 2, NLON - 2)
        back1 = NLON - shift1
        d8 = lax.div(direction, 8)
        abs_cos = cos_ref[pl.ds(d8, planes)]
        abs_sin = sin_ref[pl.ds(d8, planes)]

        def lanes(slot):
            row = jnp.where(ty == 0, slot % 2, 1 - slot % 2)
            return pl.ds(pl.multiple_of(row * NLON, NLON), NLON)

        values = []
        for slot in range(SLOTS):
            if slot < 6:
                part = halo_ref[2 - slot // 2, q, :, lanes(slot)].astype(F32)
            else:
                part = spec_ref[pl.ds(pl.multiple_of(i * size, size), size), lanes(slot)]
            part = part.reshape(planes, 8, NLON)
            if slot >= 6:
                part = part * code_ref[ty, slot, 3][None]
            values.append(part)
        for t in range(MAXSTEPS):
            live = jnp.where(t < steps, speed, 0.0)
            wx = live * abs_cos
            wy = live * abs_sin
            keep = 1.0 - wx - wy
            fresh = list(values)
            for slot in range(t + 1, SLOTS):
                x = values[slot]
                below = values[slot - 1]
                near = code_ref[ty, slot, 1 - to_east][None] == 1.0
                vert = code_ref[ty, slot, 2][None] * sign
                lon = jnp.where(near, pltpu.roll(x, shift1, 2), pltpu.roll(x, shift2, 2))
                up = jnp.where(vert == -1.0, pltpu.roll(below, shift1, 2),
                               jnp.where(vert == 1.0, pltpu.roll(below, back1, 2), below))
                up = jnp.where(jnp.abs(vert) == 2.0, x, up)
                fresh[slot] = code_ref[ty, slot, 3][None] * (keep * x + wx * lon + wy * up)
            values = fresh
        for slot in (6, 7):
            prop_ref[i, :, lanes(slot)] = values[slot].reshape(size, NLON)
        whole = prop_ref[i]
        for c in range(ncomp):
            away_ref[c, i] = whole[:, c * share:(c + 1) * share].astype(BF16)

    groups = chunks // group

    def out_copy(j, g):
        to = lax.rem(me + j, ncomp)
        span = pl.ds(g * group, group)
        return pltpu.make_async_remote_copy(
            src_ref=away_ref.at[to, span], dst_ref=got_ref.at[me, span],
            send_sem=a_send.at[j], recv_sem=a_recv.at[j],
            device_id={"comp": to}, device_id_type=MESH)

    def whole_copy(j):
        to = lax.rem(me + j, ncomp)
        return pltpu.make_async_remote_copy(
            src_ref=away_ref.at[to], dst_ref=got_ref.at[me],
            send_sem=a_send.at[j], recv_sem=a_recv.at[j],
            device_id={"comp": to}, device_id_type=MESH)

    def run_group(g, carry):
        def one(i, inner):
            propagate(g * group + i)
            return inner

        lax.fori_loop(0, group, one, 0)
        for j in range(1, ncomp):
            out_copy(j, g).start()
        return carry

    lax.fori_loop(0, groups, run_group, 0)

    for q in (0, 1):
        sent(q, q)

    def drain(q, carry):
        sent(q, kind(q))
        return carry

    lax.fori_loop(2, chunks + 2, drain, 0)
    got_ref[me] = away_ref[me]
    load_w.wait()
    give_w.wait()

    for j in range(1, ncomp):
        whole_copy(j).wait()
    for c in range(ncomp):
        start_ref[c * bins:(c + 1) * bins, :] = got_ref[c].astype(F32).reshape(bins, share)
    tile = total // TILES
    per_tile = bins // tile if bins >= tile else tile // bins
    for m in range(TILES):
        span = slice(m * tile, (m + 1) * tile)
        low_ref[0, span, :] = start_ref[span, :].astype(BF16)

    def tile_rows(m):
        return pl.ds(pl.multiple_of(m * tile, 16), tile)

    def advance(step, m):
        span = tile_rows(m)
        driving = jnp.dot(w_ref[span, :], low_ref[step % 2], preferred_element_type=F32)
        now = start_ref[span, :] if step == 0 else state_ref[span, :]
        return span, now + STEP_SIZE * now * driving

    for step in range(SRC_STEPS - 1):
        def one_tile(m, carry, step=step):
            span, now = advance(step, m)
            state_ref[span, :] = now
            low_ref[(step + 1) % 2, span, :] = now.astype(BF16)
            return carry

        lax.fori_loop(0, TILES, one_tile, 0)

    def home_copy(j, to):
        return pltpu.make_async_remote_copy(
            src_ref=inc_ref.at[to], dst_ref=home_ref.at[me],
            send_sem=b_send.at[j], recv_sem=b_recv.at[j],
            device_id={"comp": to}, device_id_type=MESH)

    mine = lax.div(me * TILES, ncomp)

    def last_tile(i, carry):
        m = lax.rem(mine + 1 + i, TILES)
        span, now = advance(SRC_STEPS - 1, m)
        gain = now - start_ref[span, :]
        for k in range(per_tile):
            to = m * per_tile + k
            inc_ref[to] = gain[k * bins:(k + 1) * bins, :].astype(BF16)
            j = lax.rem(to - me + ncomp, ncomp)

            @pl.when(to != me)
            def _():
                home_copy(j, to).start()

        return carry

    lax.fori_loop(0, TILES, last_tile, 0)
    home_ref[me] = inc_ref[me]
    for c in range(ncomp):
        j = lax.rem(me - c + ncomp, ncomp)

        @pl.when(me != c)
        def _():
            home_copy(j, lax.rem(me + j, ncomp)).wait()

        cols = slice(c * share, (c + 1) * share)
        before = prop_ref[:, :, cols].reshape(bins, share)
        out_ref[:, cols] = sea[:, cols] * (before + home_ref[c].astype(F32))


def fast_kernel(
    ncomp, spec_ref, mask_hbm, nb_hbm, steps_hbm, cour_hbm, op_ref,
    out_ref, mask_ref, nb_ref, steps_ref, cour_ref, w_ref, full_ref, oth_ref, hsend_ref, halo_ref, code_ref, ang_ref, perm_ref,
    pout_ref, pin_ref, away_ref, x_ref, start_ref, state_ref, inc_ref, home_ref,
    l_sem, i_sem, w_sem, c_send, c_recv, r_send, r_recv, g_send, g_recv, h_send, h_recv,
    a_send, a_recv, t_send, t_recv, o_sem, p_send, p_recv, b_send, b_recv,
):
    lat = lax.axis_index("lat")
    sub = lax.axis_index("sub")
    me = lax.axis_index("comp")
    groups = spec_ref.shape[0]
    bins = groups * 2 * 16
    kmax = halo_ref.shape[0]
    lanes = NLON // 2
    total = bins * ncomp
    partner = {"sub": 1 - sub}
    others = [partner, {"lat": 1 - lat}, {"lat": 1 - lat, "sub": 1 - sub}]

    small = [pltpu.make_async_copy(src, dst, i_sem.at[n]) for n, (src, dst) in enumerate((
        (mask_hbm, mask_ref.at[lat, sub]), (nb_hbm, nb_ref.at[lat, sub]),
        (steps_hbm, steps_ref), (cour_hbm, cour_ref)))]
    loads = []
    for r in range(2):
        cols = slice(r * NLON, (r + 1) * NLON)
        loads.append(pltpu.make_async_copy(
            spec_ref.at[:, 1 - sub, :, cols], oth_ref.at[pl.ds(0, groups), r], l_sem.at[r]))
        loads.append(pltpu.make_async_copy(
            spec_ref.at[:, sub, :, cols], full_ref.at[pl.ds(0, groups), 2 * sub + r], l_sem.at[2 + r]))
    for load in (small[0], *loads, *small[1:]):
        load.start()
    own_half = pl.ds(pl.multiple_of(sub * (total // 2), 16), total // 2)
    load_w = pltpu.make_async_copy(op_ref, w_ref.at[own_half], w_sem)

    barrier = pltpu.get_barrier_semaphore()
    peers = list(others)
    for d in range(1, ncomp):
        z = lax.rem(me + d, ncomp)
        peers += [{"comp": z}, {"comp": z, "sub": 1 - sub}]
    for peer in peers:
        pl.semaphore_signal(barrier, inc=1, device_id=peer, device_id_type=MESH)

    a = lax.broadcasted_iota(jnp.int32, (NLON, NLON), 0)
    b = lax.broadcasted_iota(jnp.int32, (NLON, NLON), 1)
    split = lambda c: jnp.where(c < lanes, 2 * c, 2 * (c - lanes) + 1)
    perm_ref[0] = (a == split(b)).astype(F32).astype(BF16)
    perm_ref[1] = (b == split(a)).astype(F32).astype(BF16)

    near_ty = lat
    far_ty = 1 - lat
    n0 = lax.rem(lat + me * groups, 2)
    f0 = 1 - n0
    for q, ty in enumerate((near_ty, far_ty)):
        d = lax.broadcasted_iota(jnp.int32, (16, lanes), 0) + 16 * (2 * ty + sub)
        angle = (d.astype(F32) + 0.5) * np.float32(2.0 * math.pi / ND)
        ang_ref[q, 0] = jnp.abs(jnp.cos(angle))
        ang_ref[q, 1] = jnp.abs(jnp.sin(angle))

    def point_copies(n):
        return [pltpu.make_async_remote_copy(
            src_ref=ref.at[lat, sub], dst_ref=ref.at[lat, sub], send_sem=c_send.at[n, m],
            recv_sem=c_recv.at[n, m], device_id=others[n], device_id_type=MESH)
            for m, ref in enumerate((mask_ref, nb_ref))]

    cut = 4 * NEAR

    def raw_copies(core):
        return [pltpu.make_async_remote_copy(
            src_ref=oth_ref.at[pl.ds(a, n)], dst_ref=full_ref.at[pl.ds(a, n), pl.ds(2 * core, 2)],
            send_sem=r_send.at[part], recv_sem=r_recv.at[part], device_id=partner, device_id_type=MESH)
            for part, (a, n) in enumerate(((0, cut), (cut, groups - cut)))]

    small[0].wait()
    small[1].wait()
    sea = mask_ref[lat, sub].astype(F32)
    for load in loads:
        load.wait()
    sea_rows = [jnp.broadcast_to(sea[:, r * NLON:(r + 1) * NLON], (16, NLON)) for r in range(2)]

    def convert(k, carry):
        j = n0 + 2 * k
        for r in range(2):
            mine = full_ref[j, 2 * sub + r] * sea_rows[r]
            other = oth_ref[j, r] * sea_rows[r]
            hsend_ref[k, sub, r] = mine.astype(BF16)
            hsend_ref[k, 1 - sub, r] = other.astype(BF16)
        return carry

    lax.fori_loop(0, kmax, convert, 0)
    pl.semaphore_wait(barrier, len(peers))
    def halo_copy(k, p):
        return pltpu.make_async_remote_copy(
            src_ref=hsend_ref.at[k, p], dst_ref=halo_ref.at[k, pl.ds(2 * sub, 2)],
            send_sem=h_send.at[k, p], recv_sem=h_recv.at[k, sub],
            device_id={"lat": 1 - lat, "sub": p}, device_id_type=MESH)

    def halo_wait(k, s):
        pltpu.make_async_remote_copy(
            src_ref=hsend_ref.at[k, s], dst_ref=halo_ref.at[k, pl.ds(2 * s, 2)],
            send_sem=h_send.at[k, s], recv_sem=h_recv.at[k, s],
            device_id={"lat": 1 - lat, "sub": s}, device_id_type=MESH).wait_recv()

    def give_w():
        return pltpu.make_async_remote_copy(
            src_ref=op_ref, dst_ref=w_ref.at[own_half], send_sem=g_send, recv_sem=g_recv,
            device_id=partner, device_id_type=MESH)

    def take_w():
        other_half = pl.ds(pl.multiple_of((1 - sub) * (total // 2), 16), total // 2)
        return pltpu.make_async_remote_copy(
            src_ref=op_ref, dst_ref=w_ref.at[other_half], send_sem=g_send, recv_sem=g_recv,
            device_id=partner, device_id_type=MESH)

    def send_halo(k, carry):
        @pl.when(n0 + 2 * k < groups)
        def _():
            for p in range(2):
                halo_copy(k, p).start()
        return carry

    for copy in point_copies(0):
        copy.start()
    lax.fori_loop(0, AHEAD, send_halo, 0)
    for copy in (*raw_copies(sub), *point_copies(1), *point_copies(2)):
        copy.start()
    lax.fori_loop(AHEAD, kmax, send_halo, 0)
    load_w.start()
    give_w().start()
    for load in small[2:]:
        load.wait()

    points = mask_ref.shape[-1]
    lane = lax.broadcasted_iota(jnp.int32, (1, points), 1)
    column = lane & (NLON - 1)
    index = lax.broadcasted_iota(jnp.int32, (8, points), 0)

    def decode(chip):
        for s in range(2):
            nb = nb_ref[chip, s]
            west = (column - nb[0:1, :]) & (NLON - 1)
            east = (nb[1:2, :] - column) & (NLON - 1)
            moves = [((nb[k:k + 1, :] - column + 1) & (NLON - 1)) - 1 for k in (2, 3)]
            codes = jnp.zeros((8, points), F32)
            for k, entry in enumerate((west, east, *moves, mask_ref[chip, s])):
                codes = jnp.where(index == k, jnp.broadcast_to(entry.astype(F32), (8, points)), codes)
            for r in range(2):
                part = codes[:, r * NLON:(r + 1) * NLON].astype(BF16)
                both = jnp.dot(part, perm_ref[0], preferred_element_type=F32)
                for k in range(5):
                    code_ref[chip, 2 * s + r, k] = jnp.broadcast_to(both[k:k + 1, :], (8, NLON))

    side = lax.div(me, 2)

    def target(i):
        near = me + 1 - 2 * lax.rem(me, 2)
        return jnp.where(i == 0, 3 - 3 * side, jnp.where(i == 1, 2 - side, jnp.where(i == 2, near, me)))

    def outward(i):
        k = lax.rem(i + 2, 3)
        return target(jnp.where((side == 0) & (sub == 0) & (i < 3), k, i))

    def chunk_copy(h, j, to):
        return pltpu.make_async_remote_copy(
            src_ref=away_ref.at[h, to, j], dst_ref=x_ref.at[0, me * groups + j, sub, :, 0:lanes],
            send_sem=a_send.at[h, to], recv_sem=a_recv.at[me, sub],
            device_id={"comp": to, "sub": h}, device_id_type=MESH)

    def whole_copy(h, to):
        return pltpu.make_async_remote_copy(
            src_ref=away_ref.at[h, to, pl.ds(0, groups)],
            dst_ref=x_ref.at[0, pl.ds(me * groups, groups), sub, :, 0:lanes],
            send_sem=a_send.at[h, to], recv_sem=a_recv.at[me, sub],
            device_id={"comp": to, "sub": h}, device_id_type=MESH)

    def whole_wait(z, s):
        pltpu.make_async_remote_copy(
            src_ref=away_ref.at[0, z, pl.ds(0, groups)],
            dst_ref=x_ref.at[0, pl.ds(z * groups, groups), s, :, 0:lanes],
            send_sem=a_send.at[0, 0], recv_sem=a_recv.at[z, s],
            device_id={"comp": z, "sub": s}, device_id_type=MESH).wait_recv()

    def pick(ty, i):
        return ty * 3 + (1 - 2 * ty) * i

    def separate(x):
        high = x.astype(BF16)
        low = (x - high.astype(F32)).astype(BF16)
        return high, low

    def propagate(ks, far, to_east):
        ty = far_ty if far else near_ty
        js = [(f0 if far else n0) + 2 * k for k in ks]
        vert = 2 + ty
        lowest = 0 if far else 4

        def code(q, k, half):
            chip = lat if q >= 4 else 1 - lat
            part = code_ref[chip, pick(ty, q % 4), k, :, half * lanes:(half + 1) * lanes]
            return jnp.concatenate([part, part], axis=0)

        raw = jnp.concatenate([full_ref[j, pick(ty, i)] for j in js for i in range(4)], axis=0)
        high, low = separate(raw)
        mixed = (jnp.dot(high, perm_ref[0], preferred_element_type=F32)
                 + jnp.dot(low, perm_ref[0], preferred_element_type=F32))
        if far:
            edge = jnp.concatenate([halo_ref[k, pick(ty, i)] for k in ks for i in range(4)], axis=0)
            edge = jnp.dot(edge, perm_ref[0], preferred_element_type=F32)
        cells = []
        weights = []
        for n, j in enumerate(js):
            values = [None] * 8
            for i in range(4):
                rows = slice((n * 4 + i) * 16, (n * 4 + i + 1) * 16)
                values[4 + i] = tuple(
                    mixed[rows, half * lanes:(half + 1) * lanes] * code(4 + i, 4, half)
                    for half in range(2))
                if far:
                    values[i] = tuple(edge[rows, half * lanes:(half + 1) * lanes] for half in range(2))
            cells.append(values)
            freq = jnp.minimum(lax.div(me * bins + j * 32, ND), steps_ref.shape[0] - 1)
            weights.append((steps_ref[freq], cour_ref[freq]))
        abs_cos, abs_sin = ang_ref[int(far), 0], ang_ref[int(far), 1]
        ahead, behind = (1, lanes - 1)
        for t in range(MAXSTEPS):
            slots = [q for q in range(7, lowest - 1, -1) if q >= 4 or t <= q + 1]
            for n, (steps, speed) in enumerate(weights):
                live = jnp.where(t < steps, speed, 0.0)
                wx = live * abs_cos
                wy = live * abs_sin
                keep = 1.0 - wx - wy
                values = cells[n]
                fresh = list(values)
                turned = {}

                def turn(q, half, shift):
                    key = (q, half, shift)
                    if key not in turned:
                        turned[key] = pltpu.roll(values[q][half], shift, 1)
                    return turned[key]

                def left(q):
                    return turn(q, 1, ahead), values[q][0]

                def right(q):
                    return values[q][1], turn(q, 0, behind)

                for q in slots:
                    shift = ahead if to_east else behind
                    one = left(q) if to_east else right(q)
                    lon_code = 0 if to_east else 1
                    new = []
                    for half in range(2):
                        x = values[q][half]
                        lon = jnp.where(code(q, lon_code, half) == 1.0, one[half], turn(q, half, shift))
                        if q == lowest:
                            up = x
                        else:
                            move = code(q, vert, half)
                            up = jnp.where(move == -1.0, left(q - 1)[half],
                                           jnp.where(move == 1.0, right(q - 1)[half], values[q - 1][half]))
                        new.append(code(q, 4, half) * (keep * x + wx * lon + wy * up))
                    fresh[q] = tuple(new)
                cells[n] = fresh
        for n, j in enumerate(js):
            for i in range(4):
                r = pick(ty, i)
                for half in range(2):
                    value = cells[n][4 + i][half]
                    pout_ref[j, r, :, half * lanes:(half + 1) * lanes] = value
                    away_ref[lax.div(r, 2), 2 * lax.rem(r, 2) + half, j] = value.astype(BF16)
        for n, j in enumerate(js):
            @pl.when(j < groups)
            def _():
                for i in range(ncomp - 1):
                    chunk_copy(0, j, target(i)).start()

    straight = sub == lat
    for copy in point_copies(0):
        copy.wait_recv()
    decode(lat)
    raw_copies(1 - sub)[0].wait_recv()

    def near_body(g, carry):
        @pl.when(g == 2)
        def _():
            raw_copies(1 - sub)[1].wait_recv()

        ks = [g * NEAR + n for n in range(NEAR)]

        @pl.when(straight)
        def _():
            propagate(ks, False, True)

        @pl.when(jnp.logical_not(straight))
        def _():
            propagate(ks, False, False)
        return carry

    lax.fori_loop(0, kmax // NEAR, near_body, 0)
    for n in (1, 2):
        for copy in point_copies(n):
            copy.wait_recv()
    decode(1 - lat)

    eager = 3 - 2 * side
    patient = 2 - 2 * side

    def far_body(g, carry):
        ks = [g * FAR + n for n in range(FAR)]
        for k in ks:
            @pl.when(f0 + 2 * k < groups)
            def _():
                for s in range(2):
                    halo_wait(k, s)

        @pl.when(straight)
        def _():
            propagate(ks, True, False)

        @pl.when(jnp.logical_not(straight))
        def _():
            propagate(ks, True, True)

        for k in ks:
            @pl.when(n0 + 2 * k < groups)
            def _():
                chunk_copy(1, n0 + 2 * k, eager).start()
        return carry

    lax.fori_loop(0, kmax // FAR, far_body, 0)

    own_copy = pltpu.make_async_copy(
        away_ref.at[sub, me, pl.ds(0, groups)], x_ref.at[0, pl.ds(me * groups, groups), sub, :, 0:lanes], o_sem.at[0])

    def cross_copy():
        return pltpu.make_async_remote_copy(
            src_ref=away_ref.at[1 - sub, me, pl.ds(0, groups)],
            dst_ref=x_ref.at[0, pl.ds(me * groups, groups), sub, :, 0:lanes],
            send_sem=a_send.at[0, me], recv_sem=a_recv.at[me, sub],
            device_id=partner, device_id_type=MESH)

    def prop_copy():
        return pltpu.make_async_remote_copy(
            src_ref=pout_ref.at[pl.ds(0, groups), pl.ds(2 * (1 - sub), 2)],
            dst_ref=pin_ref, send_sem=p_send, recv_sem=p_recv,
            device_id=partner, device_id_type=MESH)

    own_copy.start()
    cross_copy().start()

    def send_rest(k, carry):
        @pl.when(f0 + 2 * k < groups)
        def _():
            chunk_copy(1, f0 + 2 * k, eager).start()
        return carry

    lax.fori_loop(0, kmax, send_rest, 0)

    wide = (sub == 1) & (lax.div(me + 1, 2) == 1)

    def twin_copy(block, to):
        return pltpu.make_async_remote_copy(
            src_ref=away_ref.at[1, block, pl.ds(0, groups)],
            dst_ref=x_ref.at[0, pl.ds(me * groups, groups), sub, :, lanes:2 * lanes],
            send_sem=t_send.at[block], recv_sem=t_recv.at[me, sub],
            device_id={"comp": to, "sub": 1}, device_id_type=MESH)

    def twin_local(block):
        return pltpu.make_async_copy(
            away_ref.at[1, block, pl.ds(0, groups)],
            x_ref.at[0, pl.ds(me * groups, groups), sub, :, lanes:2 * lanes], o_sem.at[1])

    def twin_wait(z, s):
        pltpu.make_async_remote_copy(
            src_ref=away_ref.at[1, 0, pl.ds(0, groups)],
            dst_ref=x_ref.at[0, pl.ds(z * groups, groups), s, :, lanes:2 * lanes],
            send_sem=t_send.at[0], recv_sem=t_recv.at[z, s],
            device_id={"comp": z, "sub": s}, device_id_type=MESH).wait_recv()

    def twin_here(to):
        return (me == to) & (sub == 1)

    def send_twin(block, to):
        @pl.when(jnp.logical_not(twin_here(to)))
        def _():
            twin_copy(block, to).start()

        @pl.when(twin_here(to))
        def _():
            twin_local(block).start()

    send_twin(2, 1)
    whole_copy(1, jnp.where(side == 0, target(2), patient)).start()
    whole_copy(1, jnp.where(side == 0, patient, target(2))).start()
    send_twin(1, 2)
    prop_copy().start()

    piece = bins // PIECES

    def home_copy(source, block, to, start, size):
        span = pl.ds(pl.multiple_of(start, 16), size)
        return pltpu.make_async_remote_copy(
            src_ref=inc_ref.at[source, span], dst_ref=home_ref.at[block, span],
            send_sem=b_send.at[source], recv_sem=b_recv.at[block],
            device_id={"comp": to}, device_id_type=MESH)

    early = (2 * bins) // 128 * 128
    late = total - early

    once = 1 + lax.div(me, ncomp)

    def integrate(width):
        def partial(start, span, use):
            def one(i, carry):
                rows = pl.ds(pl.multiple_of(i * total, 16), total)
                field = x_ref[0, pl.ds(lax.div(start, 32), span // 32), :, :, 0:width].reshape(span, width)
                cols = pl.ds(pl.multiple_of(start, 128), span)
                use(rows, jnp.dot(w_ref[rows, cols], field, preferred_element_type=F32))
                return carry

            lax.fori_loop(0, once, one, 0)

        def begin(rows, driving):
            state_ref[rows, 0:width] = driving

        def first_step(rows, driving):
            start = x_ref[0, :, :, :, 0:width].reshape(total, width).astype(F32)
            now = start + STEP_SIZE * start * (state_ref[rows, 0:width] + driving)
            start_ref[rows, 0:width] = start
            state_ref[rows, 0:width] = now
            x_ref[1, :, :, :, 0:width] = now.astype(BF16).reshape(ncomp * groups, 2, 16, width)

        def advance(step, carry):
            field = x_ref[lax.rem(step, 2), :, :, :, 0:width].reshape(total, width)
            driving = jnp.dot(w_ref[...], field, preferred_element_type=F32)
            now = state_ref[:, 0:width]
            now = now + STEP_SIZE * now * driving
            state_ref[:, 0:width] = now
            x_ref[lax.rem(step + 1, 2), :, :, :, 0:width] = now.astype(BF16).reshape(
                ncomp * groups, 2, 16, width)
            return carry

        def last(m, start):
            rows = pl.ds(pl.multiple_of(m * bins + start, 16), piece)
            field = x_ref[(SRC_STEPS - 1) % 2, :, :, :, 0:width].reshape(total, width)
            driving = jnp.dot(w_ref[rows, :], field, preferred_element_type=F32)
            now = state_ref[rows, 0:width]
            now = now + STEP_SIZE * now * driving
            return (now - start_ref[rows, 0:width]).astype(BF16)

        def finish(n, carry):
            m = outward(lax.div(n, PIECES))
            start = lax.rem(n, PIECES) * piece
            span = pl.ds(pl.multiple_of(start, 16), piece)
            gain = last(m, start)

            @pl.when(m == me)
            def _():
                home_ref[me, span] = gain

            @pl.when(m != me)
            def _():
                inc_ref[m, span] = gain
                home_copy(m, me, m, start, piece).start()
            return carry

        def finish_wide(n, carry):
            m = target(lax.div(n, PIECES))
            start = lax.rem(n, PIECES) * piece
            span = pl.ds(pl.multiple_of(start, 16), piece)
            gain = last(m, start)
            blocks = ((me, gain[:, 0:lanes]), (3 - me, gain[:, lanes:2 * lanes]))

            @pl.when(m == me)
            def _():
                for block, part in blocks:
                    home_ref[block, span] = part

            @pl.when(m != me)
            def _():
                for source, (block, part) in enumerate(blocks):
                    inc_ref[source, span] = part
                    home_copy(source, block, m, start, piece).start()
            return carry

        both = width > lanes
        whole_wait(me, 1 - sub)
        for s in range(2):
            whole_wait(target(2), s)
        if both:
            twin_local(3 - me).wait()
            twin_wait(me, 0)
            for s in range(2):
                twin_wait(target(2), s)
        partial(side * late, early, begin)
        for i in (1, 0):
            for s in range(2):
                whole_wait(target(i), s)
                if both:
                    twin_wait(target(i), s)
        partial((1 - side) * early, late, first_step)
        lax.fori_loop(1, SRC_STEPS - 1, advance, 0)
        if both:
            lax.fori_loop((ncomp - 2) * PIECES, ncomp * PIECES, finish_wide, 0)
        else:
            lax.fori_loop(0, ncomp * PIECES, finish, 0)

    sea_wide = [jnp.broadcast_to(sea[:, r * NLON:(r + 1) * NLON], (16, NLON)) for r in range(2)]

    def restore(g, carry):
        js = [g * BACK + n for n in range(BACK)]
        parts = [ref for j in js for ref in (
            pout_ref[j, 2 * sub], pout_ref[j, 2 * sub + 1], pin_ref[j, 0], pin_ref[j, 1])]
        high, low = separate(jnp.concatenate(parts, axis=0))
        plain = (jnp.dot(high, perm_ref[1], preferred_element_type=F32)
                 + jnp.dot(low, perm_ref[1], preferred_element_type=F32))
        for n in range(4 * BACK):
            p = sub if n % 4 < 2 else 1 - sub
            rows = pl.ds(pl.multiple_of((2 * js[n // 4] + p) * 16, 16), 16)
            r = n % 2
            out_ref[rows, r * NLON:(r + 1) * NLON] = sea_wide[r] * plain[n * 16:(n + 1) * 16, :]
        return carry

    def restore_all():
        prop_copy().wait_recv()
        lax.fori_loop(0, groups // BACK, restore, 0)

    pl.when(sub == 1)(restore_all)
    load_w.wait()
    take_w().wait_recv()
    own_copy.wait()
    @pl.when(wide)
    def _():
        integrate(2 * lanes)

    @pl.when(jnp.logical_not(wide))
    def _():
        integrate(lanes)

    pl.when(sub == 0)(restore_all)
    for i in (3, 0, 2, 1):
        z = target(i)

        def land():
            pltpu.make_async_remote_copy(
                src_ref=inc_ref.at[z], dst_ref=home_ref.at[z],
                send_sem=b_send.at[z], recv_sem=b_recv.at[z],
                device_id={"comp": z}, device_id_type=MESH).wait_recv()

        if i < 3:
            pl.when(jnp.logical_not(wide & (z == 3 - me)))(land)
        r = lax.div(z, 2)
        half = lax.rem(z, 2)
        cols = pl.ds(pl.multiple_of(r * NLON, NLON), NLON)
        spread = perm_ref[1, pl.ds(pl.multiple_of(half * lanes, lanes), lanes), :]
        sea_row = jnp.where(r == 0, sea_wide[0][0:8], sea_wide[1][0:8])
        back = jnp.dot(home_ref[z], spread, preferred_element_type=F32)
        back = back.reshape(bins // 8, 8, NLON) * sea_row[None]
        out_ref[:, cols] = out_ref[:, cols] + back.reshape(bins, NLON)

    for n in range(3):
        for copy in point_copies(n):
            copy.wait_send()
    for copy in raw_copies(sub):
        copy.wait_send()

    def halo_left(k, carry):
        @pl.when(n0 + 2 * k < groups)
        def _():
            for p in range(2):
                halo_copy(k, p).wait_send()
        return carry

    lax.fori_loop(0, kmax, halo_left, 0)
    prop_copy().wait_send()
    cross_copy().wait_send()
    give_w().wait_send()
    for i in range(ncomp - 1):
        for h in range(2):
            whole_copy(h, target(i)).wait_send()

        @pl.when(jnp.logical_not(wide))
        def _():
            m = target(i)
            home_copy(m, me, m, 0, bins).wait_send()

    @pl.when(wide)
    def _():
        for source, block in enumerate((me, 3 - me)):
            home_copy(source, block, target(2), 0, bins).wait_send()

    for block, to in ((1, 2), (2, 1)):
        @pl.when(jnp.logical_not(twin_here(to)))
        def _():
            twin_copy(block, to).wait_send()


def write_kernel(src_ref, dst_ref, sems):
    pieces = sems.shape[0]
    rows = src_ref.shape[0] // pieces
    copies = [pltpu.make_async_copy(
        src_ref.at[pl.ds(i * rows, rows)], dst_ref.at[pl.ds(i * rows, rows)], sems.at[i])
        for i in range(pieces)]
    for copy in copies:
        copy.start()
    for copy in copies:
        copy.wait()


def fast_device(ncomp, spectrum, sea_mask, neighbours, substeps, courant, source_operator):
    bins, points = spectrum.shape
    groups = bins // 32
    kmax = (groups + 1) // 2
    lanes = NLON // 2
    total = bins * ncomp
    vmem = pl.BlockSpec(memory_space=pltpu.VMEM)
    hbm = pl.BlockSpec(memory_space=pltpu.HBM)
    dma = pltpu.SemaphoreType.DMA
    result = pl.pallas_call(
        functools.partial(fast_kernel, ncomp),
        out_shape=pltpu.VMEM((bins, points), F32),
        in_specs=[hbm] * 6,
        out_specs=vmem,
        scratch_shapes=[
            pltpu.VMEM((2, 2, 1, points), jnp.int32),
            pltpu.VMEM((2, 2, 4, points), jnp.int32),
            pltpu.SMEM(substeps.shape, jnp.int32),
            pltpu.SMEM(courant.shape, F32),
            pltpu.VMEM((total, total), BF16),
            pltpu.VMEM((2 * kmax, 4, 16, NLON), F32),
            pltpu.VMEM((2 * kmax, 2, 16, NLON), F32),
            pltpu.VMEM((kmax, 2, 2, 16, NLON), BF16),
            pltpu.VMEM((kmax, 4, 16, NLON), BF16),
            pltpu.VMEM((2, 4, 5, 8, NLON), F32),
            pltpu.VMEM((2, 2, 16, lanes), F32),
            pltpu.VMEM((2, NLON, NLON), BF16),
            pltpu.VMEM((2 * kmax, 4, 16, NLON), F32),
            pltpu.VMEM((groups, 2, 16, NLON), F32),
            pltpu.VMEM((2, ncomp, 2 * kmax, 16, lanes), BF16),
            pltpu.VMEM((2, ncomp * groups, 2, 16, 2 * lanes), BF16),
            pltpu.VMEM((total, 2 * lanes), F32),
            pltpu.VMEM((total, 2 * lanes), F32),
            pltpu.VMEM((ncomp, bins, lanes), BF16),
            pltpu.VMEM((ncomp, bins, lanes), BF16),
            dma((4,)), dma((4,)), dma, dma((3, 2)), dma((3, 2)), dma((2,)), dma((2,)), dma, dma,
            dma((kmax, 2)), dma((kmax, 2)), dma((2, ncomp)), dma((ncomp, 2)), dma((ncomp,)), dma((ncomp, 2)),
            dma((2,)), dma, dma,
            dma((ncomp,)), dma((ncomp,)),
        ],
        compiler_params=pltpu.CompilerParams(
            collective_id=1, has_side_effects=True, vmem_limit_bytes=60 * 1024 * 1024),
    )(spectrum.reshape(groups, 2, 16, points), sea_mask.reshape(1, points), neighbours, substeps, courant,
      source_operator)
    return pl.pallas_call(
        write_kernel,
        out_shape=jax.ShapeDtypeStruct((bins, points), F32),
        in_specs=[vmem],
        out_specs=hbm,
        scratch_shapes=[dma((4,))],
        compiler_params=pltpu.CompilerParams(vmem_limit_bytes=4 * 1024 * 1024),
    )(result)


def solution(mesh):
    nlat, ncomp = mesh.shape["lat"], mesh.shape["comp"]

    def per_device(spectrum, sea_mask, neighbours, substeps, courant, source_operator):
        bins, points = spectrum.shape
        even = bins % 32 == 0 and (bins // 32 + 1) // 2 % NEAR == 0 and bins // 32 % BACK == 0
        if nlat == 2 and ncomp == 4 and points == 2 * NLON and even:
            return fast_device(ncomp, spectrum, sea_mask, neighbours, substeps, courant, source_operator)
        size = 16 if bins % 16 == 0 else 8
        chunks = bins // size
        group = 5 if chunks % 5 == 0 else 1
        share = points // ncomp
        total = bins * ncomp
        angles = (np.arange(ND, dtype=np.float32) + np.float32(0.5)) * np.float32(2.0 * math.pi / ND)
        spread = lambda v: jnp.asarray(
            np.broadcast_to(np.abs(v).astype(np.float32)[:, None], (ND, NLON)).reshape(ND // 8, 8, NLON))
        vmem = pl.BlockSpec(memory_space=pltpu.VMEM)
        smem = pl.BlockSpec(memory_space=pltpu.SMEM)
        kinds = 3 if nlat == 2 else 4
        return pl.pallas_call(
            functools.partial(kernel, nlat, ncomp, group),
            out_shape=jax.ShapeDtypeStruct((bins, points), F32),
            in_specs=[vmem, vmem, vmem, smem, smem, vmem, vmem, pl.BlockSpec(memory_space=pl.ANY)],
            out_specs=vmem,
            scratch_shapes=[
                pltpu.VMEM((total, total), BF16),
                pltpu.VMEM((chunks + 2, size, points), BF16),
                pltpu.VMEM((3, chunks + 2, size, points), BF16),
                pltpu.VMEM((2, SLOTS, 4, 8, NLON), F32),
                pltpu.VMEM((chunks, size, points), F32),
                pltpu.VMEM((ncomp, chunks, size, share), BF16),
                pltpu.VMEM((ncomp, chunks, size, share), BF16),
                pltpu.VMEM((total, share), F32),
                pltpu.VMEM((total, share), F32),
                pltpu.VMEM((2, total, share), BF16),
                pltpu.VMEM((ncomp, bins, share), BF16),
                pltpu.VMEM((ncomp, bins, share), BF16),
                pltpu.SemaphoreType.DMA((kinds, chunks + 2)),
                pltpu.SemaphoreType.DMA((kinds, chunks + 2)),
                pltpu.SemaphoreType.DMA,
                pltpu.SemaphoreType.DMA,
                pltpu.SemaphoreType.DMA,
                pltpu.SemaphoreType.DMA((ncomp,)),
                pltpu.SemaphoreType.DMA((ncomp,)),
                pltpu.SemaphoreType.DMA((ncomp,)),
                pltpu.SemaphoreType.DMA((ncomp,)),
            ],
            compiler_params=pltpu.CompilerParams(
                collective_id=0, has_side_effects=True, vmem_limit_bytes=56 * 1024 * 1024),
        )(spectrum, sea_mask.reshape(1, points), neighbours, substeps, courant,
          spread(np.cos(angles)), spread(np.sin(angles)), source_operator)

    placed = (
        P("comp", ("members", "lat", "sub")),
        P(("members", "lat", "sub")),
        P(None, ("members", "lat", "sub")),
        P(),
        P(),
        P("sub", None),
    )
    return jax.shard_map(
        per_device,
        mesh=mesh,
        in_specs=placed,
        out_specs=P("comp", ("members", "lat", "sub")),
        check_vma=False,
    )
```
